32 devices in a mesh: outer: 4 (over y, x), rep: 4 (over z), shard: 2 (over core).
Axes of the slice: x: 2, y: 2, z: 4, core: 2. Of those that a mesh axis runs over, the one named last changes fastest.
Arguments:
- deltas: bfloat16 [4, 4, 1024, 5120], P('outer', 'rep', 'shard'), may hold values from -1400 to 1400, as said below
- owners: int32 [2, 4, 1], P('shard'), may hold values from 0 to 3; in each aligned block of 4 rows (0 to 3, 4 to 7, ..., all dimensions but the last counted through in order) at most 2 rows name the same one
- master: float32 [4, 2, 2, 128, 5120], P('outer', 'shard', None, 'rep'), may hold values from -6 to 6
- momentum: float32 [4, 2, 2, 128, 5120], P('outer', 'shard', None, 'rep'), may hold values from -3 to 3
Outputs:
- new_params: bfloat16 [1024, 5120], P('shard')
- new_momentum: float32 [4, 2, 2, 128, 5120], P('outer', 'shard', None, 'rep')
- new_master: float32 [4, 2, 2, 128, 5120], P('outer', 'shard', None, 'rep')
The draws below stay inside these ranges and needn't reach their ends.
Inputs may be any that keep to these rules, and one draw needn't show every extreme that they name: `owners`: within each shard, no pod owns more than 2 blocks, and in some shards one pod owns exactly 2. `deltas`: finite values.
All inputs are finite; a program needn't handle non-finite values.
Results may differ from the reference program's by a relative error of at most 0.0075.
Values may be sent and summed in bfloat16 or wider, within the bound.
A program may use at most 128 MiB of HBM per device.

```python
import math
import jax
import jax.numpy as jnp
import numpy as np
from jax import lax

D = 5120
BLOCK_ROWS = 128
BLOCKS = 4
MOST = 2
N_OUTER = 4
N_REP = 4
N_SHARD = 2


def draw_deltas(key, part):
    total_rows = N_SHARD * BLOCKS * BLOCK_ROWS
    noise_key, row_key, col_key = jax.random.split(key, 3)
    position = jnp.arange(total_rows, dtype=jnp.float32) / (total_rows - 1.0)
    noise = jnp.clip(jax.random.normal(noise_key, (N_OUTER, N_REP, total_rows, D), jnp.float32), -5.0, 5.0)
    ramp = 1.0 + 2.0 * position
    row_scale = jnp.exp(jax.random.uniform(row_key, (N_OUTER, N_REP, total_rows, 1), jnp.float32, 0.0, 2.302585))
    col_scale = jnp.exp(jax.random.uniform(col_key, (1, 1, 1, D), jnp.float32, 0.0, 1.098612))
    values = noise * row_scale * col_scale * ramp[None, None, :, None]
    return values.astype(jnp.bfloat16)


def shard_levels(key, extent, cuts, least, high):
    def one(dim, shards_of):
        draws = jax.random.uniform(jax.random.fold_in(jax.random.fold_in(key, 6), dim), (shards_of,), jnp.float32, least / len(cuts), high / len(cuts))
        return jnp.repeat(jnp.exp(draws), extent[dim] // shards_of).reshape((-1,) + (1,) * (len(extent) - dim - 1))

    factor_of = one(*cuts[0])
    for cut in cuts[1:]:
        factor_of = factor_of * one(*cut)
    return factor_of


def routed_block(stream_key, own, number, rows, count, top, bound, lean):
    ranking = jax.random.permutation(stream_key, count)
    crowded, usual = shares(count, rows * top, bound, lean, True), shares(count, rows * top, bound, lean, False)
    places = jnp.arange(count)

    def named(tallies, offset_by):
        used = int((tallies > 0).sum())
        fixed = max(1, used // 4)
        moved = fixed + (places - fixed + offset_by * (used - fixed)) % max(1, count - fixed)
        return jnp.zeros((count,), jnp.int32).at[ranking[jnp.where(places < fixed, places, moved)]].set(jnp.asarray(tallies, jnp.int32))

    tallies = jnp.where(number % 4 == 0, named(crowded, number // 4), named(usual, number - number // 4 - 1))
    mixed = jax.random.permutation(jax.random.fold_in(own, 3), count)
    giver, taker = mixed[0:count // 2 * 2:2], mixed[1:count // 2 * 2:2]
    room = jnp.minimum(tallies[giver] - 1, bound - tallies[taker]) // 2
    room = jnp.where((giver == ranking[0]) | (taker == ranking[0]) | (tallies[taker] == 0), 0, jnp.maximum(room, 0))
    moved = jax.random.randint(jax.random.fold_in(own, 4), (count // 2,), 0, 1 << 20) % (room + 1)
    tallies = tallies.at[giver].add(-moved).at[taker].add(moved)
    labels = jnp.searchsorted(jnp.cumsum(tallies), jnp.arange(rows * top), side="right").astype(jnp.int32)
    grid = labels.reshape(top, rows).T
    grid = grid[jax.random.permutation(jax.random.fold_in(own, 1), rows)]
    offset_by = jax.random.randint(jax.random.fold_in(own, 2), (rows, 1), 0, top)
    return jnp.take_along_axis(grid, (jnp.arange(top)[None, :] + offset_by) % top, axis=1)


def shares(amount, total, limit, lean, full):
    weights = [(1 << 20) // math.isqrt(grade ** lean) + 1 for grade in range(1, amount + 1)]
    largest = limit if full else min(limit, max(-(-total // amount), total * weights[0] // sum(weights)))
    least = 1 if total - largest >= amount - 1 else 0
    holding, rest = [largest] + [least] * (amount - 1), total - largest - least * (amount - 1)
    while rest > 0:
        candidates = [i for i in range(1, amount) if holding[i] < largest] or [i for i in range(1, amount) if holding[i] < limit]
        pool, budget = sum([weights[i] for i in candidates]), rest
        for i in candidates:
            extra = min(limit - holding[i], max(1, budget * weights[i] // pool), rest)
            holding[i] = holding[i] + extra
            rest = rest - extra
    return np.array(holding)


def bell_draw(key, extent, spread, bound, shards=(), held_as=jnp.bfloat16):
    values = jax.random.normal(key, extent, jnp.float32) * spread
    if len(shards) > 0:
        values = shard_levels(key, extent, shards, -0.22, 0.18) * values
    return jnp.clip(values, min=-bound, max=bound).astype(held_as)


def setup_inputs(seed: int = 0) -> dict:
    arg_keys = jax.random.split(jax.random.key(seed), 5)
    deltas = draw_deltas(jax.random.fold_in(arg_keys[4], 71), 0)
    owners_keys = jax.random.split(jax.random.fold_in(arg_keys[1], 1), N_SHARD * BLOCKS // BLOCKS)
    owners_turns = jax.random.permutation(jax.random.fold_in(arg_keys[1], 3), N_SHARD * BLOCKS // BLOCKS)
    owners = jax.vmap(lambda own, number: routed_block(jax.random.fold_in(arg_keys[1], 2), own, number, BLOCKS, N_OUTER, 1, MOST, 2))(owners_keys, owners_turns).reshape((N_SHARD, BLOCKS, 1))
    master = bell_draw(arg_keys[2], (N_OUTER, N_SHARD, MOST, BLOCK_ROWS, D), 1.0, 6.0, ((0, 4), (1, 2), (3, 4)), jnp.float32)
    momentum = bell_draw(arg_keys[3], (N_OUTER, N_SHARD, MOST, BLOCK_ROWS, D), 0.5, 3.0, ((0, 4), (1, 2), (3, 4)), jnp.float32)
    return dict(deltas=deltas, owners=owners, master=master, momentum=momentum)


def reference(deltas, owners, master, momentum):
    total_reps = N_OUTER * N_REP
    pod_sums = lax.optimization_barrier(jnp.sum(deltas.astype(jnp.float32), axis=1)).astype(jnp.bfloat16)
    mean_delta = lax.optimization_barrier(jnp.sum(pod_sums.astype(jnp.float32), axis=0)) / total_reps
    owned_blocks = owners[:, :, 0].astype(jnp.int32)
    pod_ids = jnp.arange(N_OUTER, dtype=jnp.int32)
    onehot = (owned_blocks[:, :, None] == pod_ids[None, None, :]).astype(jnp.int32)
    rank_all = jnp.cumsum(onehot, axis=1) - onehot
    rank_own = lax.optimization_barrier(jnp.sum(rank_all * onehot, axis=2))
    slot_ids = jnp.arange(MOST, dtype=jnp.int32)
    selector = ((owned_blocks[None, :, None, :] == pod_ids[:, None, None, None]) & (rank_own[None, :, None, :] == slot_ids[None, None, :, None])).astype(jnp.float32)
    blocks = mean_delta.reshape(N_SHARD, BLOCKS, BLOCK_ROWS, D)
    slotted = jnp.einsum('osjb,sbrw->osjrw', selector, blocks, precision=lax.Precision.HIGHEST)
    sum_squares = jnp.sum(mean_delta * mean_delta)
    clip_limit = 0.5 * math.sqrt(N_SHARD * BLOCKS * BLOCK_ROWS * D)
    factor = jnp.minimum(1.0, clip_limit / jnp.sqrt(sum_squares + 1e-06))
    new_momentum = 0.9 * momentum + factor * slotted
    new_master = master - 0.7 * (factor * slotted + 0.9 * new_momentum)
    restored = jnp.einsum('osjb,osjrw->sbrw', selector, new_master, precision=lax.Precision.HIGHEST)
    new_params = restored.reshape(N_SHARD * BLOCKS * BLOCK_ROWS, D).astype(jnp.bfloat16)
    return (new_params, new_momentum, new_master)
```

```python
import functools
import math

import jax
import jax.numpy as jnp
from jax import lax
from jax.experimental import pallas as pl
from jax.experimental.pallas import tpu as pltpu
from jax.sharding import PartitionSpec as P

HALVES = 1
DEEP = 0.3
TILE = 16
SIDE = 2
LINE = 4


def kernel(
    plan, axis_sizes, clip_limit,
    owners, deltas, master, momentum,
    out, new_momentum, new_master,
    first, passed, second, zin, zrecv,
    near, far, last, onward, ztotal, cross,
    apack, arecv, mean, packed, slotted, squares, others,
    send_sem, recv_sem,
):
    halves, widths = plan
    pod_count, rep_count, shard_count = axis_sizes
    blocks, sub_rows, slots = deltas.shape[0], master.shape[1], master.shape[0]
    rows_here = sub_rows // halves
    w1, w2, w3 = widths
    pair_width = w1 + w2
    base = (0, pod_count * w1, pod_count * pair_width)
    offset = (0, w1, pair_width)
    chunks = blocks * halves
    o, q, s = lax.axis_index("outer"), lax.axis_index("rep"), lax.axis_index("shard")
    y, x = o // SIDE, o % SIDE
    neighbour = {"x": y * SIDE + 1 - x, "y": (1 - y) * SIDE + x}
    is_low = q < rep_count // 2
    tip = jnp.where(is_low, 0, rep_count - 1)
    is_tip = q == tip

    def place(k):
        return jnp.where(is_low, k, rep_count - 1 - k)

    def pod(d):
        return ((y + d // SIDE) % SIDE) * SIDE + (x + d % SIDE) % SIDE

    barrier = pltpu.get_barrier_semaphore()
    peers = []
    for d in range(pod_count):
        for e in range(rep_count):
            if d or e:
                peers.append({"outer": pod(d), "rep": (q + e) % rep_count})
    peers += [{"shard": (s + d) % shard_count} for d in range(1, shard_count)]
    for peer in peers:
        pl.semaphore_signal(barrier, inc=1, device_id=peer, device_id_type=pl.DeviceIdType.MESH)
    pl.semaphore_wait(barrier, len(peers))

    numbers, drains = {}, []

    def copy(key, src, dst, **to):
        number = numbers.setdefault(key, len(numbers))
        return pltpu.make_async_remote_copy(
            src_ref=src, dst_ref=dst, send_sem=send_sem.at[number], recv_sem=recv_sem.at[number],
            device_id=to, device_id_type=pl.DeviceIdType.MESH,
        )

    flight = {}

    def send(key, src, dst, **to):
        made = copy(key, src, dst, **to)
        made.start()
        flight[key] = made
        drains.append((None, made))

    def send_if(role, key, src, dst, **to):
        made = copy(key, src, dst, **to)
        drains.append((role, made))
        pl.when(role)(made.start)

    def arrive(key):
        flight[key].wait_recv()

    def arrive_at(key, src, dst):
        copy(key, src, dst, rep=q).wait_recv()

    def loop(count, body):
        def step(i, carry):
            body(i)
            return carry

        lax.fori_loop(0, count, step, 0)

    def up(value):
        return value.astype(jnp.float32)

    def down(value):
        return value.astype(jnp.bfloat16)

    def where(c):
        return c // halves, pl.ds((c % halves) * rows_here, rows_here)

    def cols(region, k):
        width = widths[region]
        return pl.ds(pl.multiple_of(base[region] + k * width, 128), width)

    def local_cols(region):
        return pl.ds(offset[region], widths[region])

    def order(region, c):
        return ("x", "y") if (region + c // halves) % 2 == 0 else ("y", "x")

    whole = pl.ds(base[2], pod_count * w3)

    def quarter(axis, j, away):
        if axis == "x":
            return j * SIDE + (1 - x if away else x)
        return (1 - y if away else y) * SIDE + j

    def stay(axis):
        return y if axis == "x" else x

    def send_first(c):
        b, rows = where(c)
        for r in range(2):
            axis = order(r, c)[0]
            for j in range(SIDE):
                send(
                    ("first", c, r, j), deltas.at[b, :, rows, cols(r, quarter(axis, j, True))],
                    first[r].at[j, b, :, rows, :], outer=neighbour[axis],
                )

    def send_second(c):
        b, rows = where(c)
        for r in range(2):
            axis, other = order(r, c)
            for j in range(SIDE):
                arrive(("first", c, r, j))
            go = 1 - stay(axis)
            at = cols(r, quarter(axis, go, False))

            def body(i):
                passed[r][b, i, rows, :] = down(up(deltas[b, i, rows, at]) + up(first[r][go, b, i, rows, :]))

            loop(rep_count, body)
            send(
                ("second", c, r), passed[r].at[b, :, rows, :], second[r].at[b, :, rows, :],
                outer=neighbour[other],
            )

    def send_third(c):
        b, rows = where(c)
        for r in range(2):
            axis, other = order(r, c)
            arrive(("second", c, r))
            keep = stay(axis)
            at = cols(r, o)

            def body(i):
                total = up(deltas[b, i, rows, at]) + up(first[r][keep, b, i, rows, :])
                zin[b, i, rows, local_cols(r)] = down(total + up(second[r][b, i, rows, :]))

            loop(rep_count, body)
        for d in range(1, rep_count):
            there = (q + d) % rep_count
            send(
                ("third", c, d), zin.at[b, there, rows, :], zrecv.at[d - 1, b, rows, :], rep=there
            )

    def start_tips(c):
        b, rows = where(c)
        for k in (3, 2, 1):
            send_if(
                is_tip, ("near", c, k), deltas.at[b, place(k), rows, whole], near.at[k - 1, b, rows, :],
                rep=place(1),
            )

    def relay_near(c):
        b, rows = where(c)

        @pl.when(jnp.logical_not(is_tip))
        def _():
            for k in (3, 2):
                arrive_at(("near", c, k), deltas.at[b, place(k), rows, whole], near.at[k - 1, b, rows, :])
                onward[k - 1, b, rows, :] = down(up(deltas[b, place(k), rows, whole]) + up(near[k - 1, b, rows, :]))
                copy(
                    ("far", c, 3 - k), onward.at[k - 1, b, rows, :], far.at[3 - k, b, rows, :], rep=place(2)
                ).start()

        for k in (3, 2):
            drains.append((jnp.logical_not(is_tip), copy(
                ("far", c, 3 - k), onward.at[k - 1, b, rows, :], far.at[3 - k, b, rows, :], rep=place(2)
            )))

    def relay_far(c):
        b, rows = where(c)

        @pl.when(jnp.logical_not(is_tip))
        def _():
            arrive_at(("far", c, 0), onward.at[2, b, rows, :], far.at[0, b, rows, :])
            onward[0, b, rows, :] = down(up(deltas[b, place(0), rows, whole]) + up(far[0, b, rows, :]))
            copy(("last", c), onward.at[0, b, rows, :], last.at[b, rows, :], rep=place(0)).start()

        drains.append((jnp.logical_not(is_tip), copy(
            ("last", c), onward.at[0, b, rows, :], last.at[b, rows, :], rep=place(0)
        )))

    def send_cross(c):
        b, rows = where(c)

        @pl.when(is_tip)
        def _():
            arrive_at(("last", c), onward.at[0, b, rows, :], last.at[b, rows, :])
            ztotal[b, rows, :] = down(up(deltas[b, q, rows, whole]) + up(last[b, rows, :]))

        @pl.when(jnp.logical_not(is_tip))
        def _():
            arrive_at(("near", c, 1), deltas.at[b, q, rows, whole], near.at[0, b, rows, :])
            arrive_at(("far", c, 1), onward.at[1, b, rows, :], far.at[1, b, rows, :])
            total = up(deltas[b, q, rows, whole]) + up(near[0, b, rows, :])
            ztotal[b, rows, :] = down(total + up(far[1, b, rows, :]))

        for d in range(1, pod_count):
            at = pl.ds(pl.multiple_of(pod(d) * w3, 128), w3)
            send(("cross", c, d), ztotal.at[b, rows, at], cross.at[d - 1, b, rows, :], outer=pod(d))

    scale = 1.0 / (pod_count * rep_count)

    def put_mean(b, rows, at, total):
        value = total * scale
        mean[b, rows, at] = down(value)
        square = value * value
        part = squares[0]
        height, width = square.shape
        for k in range(height // 8):
            for i in range(width // 128):
                part = part + square[k * 8:(k + 1) * 8, i * 128:(i + 1) * 128]
        squares[0] = part

    def finish_pair(c):
        b, rows = where(c)
        for d in range(1, rep_count):
            arrive(("third", c, d))
        total = up(zin[b, q, rows, :])
        for d in range(rep_count - 1):
            total = total + up(zrecv[d, b, rows, :])
        put_mean(b, rows, pl.ds(0, pair_width), total)

    def finish_cross(c):
        b, rows = where(c)
        for d in range(1, pod_count):
            arrive(("cross", c, d))
        total = up(ztotal[b, rows, pl.ds(pl.multiple_of(o * w3, 128), w3)])
        for d in range(pod_count - 1):
            total = total + up(cross[d, b, rows, :])
        put_mean(b, rows, pl.ds(pair_width, w3), total)

    owner = [owners[b] for b in range(blocks)]
    rank = []
    for b in range(blocks):
        count = jnp.int32(0)
        for before in range(b):
            count = count + (owner[before] == owner[b]).astype(jnp.int32)
        rank.append(count)

    def block_of(k, j):
        index, found = jnp.int32(0), jnp.int32(0)
        for b in range(blocks):
            match = ((owner[b] == k) & (rank[b] == j)).astype(jnp.int32)
            index, found = index + b * match, found + match
        return index, found

    def pack_early():
        for k in range(pod_count):
            for r in range(3):
                at = pl.ds(base[r] + k * widths[r], widths[r])

                def body(i):
                    value = master[i, :, at] - 0.567 * momentum[i, :, at]
                    apack[k, i, :, local_cols(r)] = down(value)

                loop(slots, body)
        arecv[o] = apack[o]

    def send_early():
        for d in range(1, pod_count):
            send(("early", d), apack.at[pod(d)], arecv.at[o], outer=pod(d))

    squares[0] = jnp.zeros(squares.shape[1:], jnp.float32)
    send_first(0)
    send_first(1)
    for c in range(chunks):
        start_tips(c)
    pack_early()
    for t in range(chunks + 3):
        if t < chunks:
            relay_near(t)
            send_second(t)
        if t + 2 < chunks:
            send_first(t + 2)
        if t == chunks - 1:
            send_early()
        if 0 <= t - 1 < chunks:
            relay_far(t - 1)
            send_third(t - 1)
        if 0 <= t - 2 < chunks:
            send_cross(t - 2)
            finish_pair(t - 2)
        if 0 <= t - 3 < chunks:
            finish_cross(t - 3)

    others[0] = jnp.sum(squares[0], axis=0, keepdims=True)
    group = pod_count * rep_count
    for d in range(pod_count):
        for e in range(rep_count):
            if d or e:
                send(
                    ("norm", d, e), others.at[0], others.at[d * rep_count + e],
                    outer=pod(d), rep=(q + e) % rep_count,
                )
    for d in range(pod_count):
        for j in range(slots):
            index = block_of(pod(d), j)[0]
            packed[d, j] = mean[index]
        if d == 0:
            slotted[o] = packed[0]
        else:
            send(("slot", d), packed.at[d], slotted.at[o], outer=pod(d))
    for d in range(pod_count):
        for e in range(rep_count):
            if d or e:
                arrive(("norm", d, e))
    total = others[0]
    for d in range(1, group):
        total = total + others[d]
    others[group] = total
    for d in range(1, shard_count):
        send(("shard", d), others.at[group], others.at[group + d], shard=(s + d) % shard_count)
    for d in range(1, pod_count):
        arrive(("early", d))
    for d in range(1, shard_count):
        arrive(("shard", d))
    for d in range(1, shard_count):
        total = total + others[group + d]
    total = jnp.sum(total, keepdims=True)
    factor = jnp.minimum(1.0, clip_limit / jnp.sqrt(total + 1e-06))

    def spread(c):
        b, rows = where(c)
        for r in range(3):
            at = local_cols(r)
            value = up(arecv[owner[b], jnp.minimum(rank[b], slots - 1), rows, at]) - (1.33 * factor) * up(mean[b, rows, at])
            out[b, q, rows, cols(r, o)] = down(value)
        for d in range(1, pod_count):
            at = out.at[b, q, rows, cols(2, o)]
            send(("wide", c, d), at, at, outer=pod(d))
        for d in range(1, rep_count):
            for r in range(2):
                at = out.at[b, q, rows, cols(r, o)]
                send(("line", c, d, r), at, at, rep=(q + d) % rep_count)

    def line(c):
        b, rows = where(c)
        for d in range(1, pod_count):
            arrive(("wide", c, d))
        mine = out.at[b, q, rows, whole]
        send_if(is_tip, ("outward", c, 0), mine, mine, rep=place(1))
        middle = jnp.logical_not(is_tip)
        send_if(middle, ("across", c, 1), mine, mine, rep=place(2))
        send_if(middle, ("inward", c, 1), mine, mine, rep=place(0))

    def line_across(c):
        b, rows = where(c)
        middle = jnp.logical_not(is_tip)
        at = out.at[b, place(0), rows, whole]
        pl.when(middle)(lambda: arrive_at(("outward", c, 0), at, at))
        send_if(middle, ("across", c, 0), at, at, rep=place(2))
        at = out.at[b, place(2), rows, whole]
        pl.when(middle)(lambda: arrive_at(("across", c, 1), at, at))
        send_if(middle, ("inward", c, 2), at, at, rep=place(0))

    def line_inward(c):
        b, rows = where(c)
        middle = jnp.logical_not(is_tip)
        at = out.at[b, place(3), rows, whole]
        pl.when(middle)(lambda: arrive_at(("across", c, 0), at, at))
        send_if(middle, ("inward", c, 3), at, at, rep=place(0))

    def line_end(c):
        b, rows = where(c)
        for k in (1, 2, 3):
            at = out.at[b, place(k), rows, whole]
            pl.when(is_tip)(lambda: arrive_at(("inward", c, k), at, at))

    def send_block(c):
        b, rows = where(c)
        for r in range(2):
            for d in range(1, rep_count):
                arrive(("line", c, d, r))
            other = order(r, c)[1]
            at = out.at[b, :, rows, cols(r, o)]
            send(("block", c, r), at, at, outer=neighbour[other])

    def send_blocks(c):
        b, rows = where(c)
        for r in range(2):
            arrive(("block", c, r))
            axis = order(r, c)[0]
            for j in range(SIDE):
                at = out.at[b, :, rows, cols(r, quarter(axis, j, False))]
                send(("blocks", c, r, j), at, at, outer=neighbour[axis])

    def update():
        for d in range(1, pod_count):
            arrive(("slot", d))
        for j in range(slots):
            found = block_of(o, j)[1].astype(jnp.float32)
            for k in range(pod_count):
                for r in range(3):
                    at = pl.ds(base[r] + k * widths[r], widths[r])
                    step = (factor * found) * up(slotted[k, j, :, local_cols(r)])
                    moved = 0.9 * momentum[j, :, at] + step
                    new_momentum[j, :, at] = moved
                    new_master[j, :, at] = master[j, :, at] - 0.7 * (step + 0.9 * moved)

    for c in range(chunks):
        spread(c)
    for t in range(chunks + 3):
        if t < chunks:
            line(t)
            send_block(t)
        if 0 <= t - 1 < chunks:
            line_across(t - 1)
            send_blocks(t - 1)
        if t == 1:
            update()
        if 0 <= t - 2 < chunks:
            line_inward(t - 2)
        if 0 <= t - 3 < chunks:
            line_end(t - 3)
    for c in range(chunks):
        for r in range(2):
            for j in range(SIDE):
                arrive(("blocks", c, r, j))
    for role, made in drains:
        if role is None:
            made.wait_send()
        else:
            pl.when(role)(made.wait_send)
    assert len(numbers) <= send_sem.shape[0]


def regions(width, pod_count):
    tiles = width // (128 * pod_count)
    third = max(1, round(tiles * DEEP))
    second = (tiles - third) // 2
    return tuple(128 * n for n in (tiles - third - second, second, third))


def fused(deltas, owners, master, momentum):
    blocks = owners.shape[1]
    slots, sub_rows, width = master.shape[2:]
    pod_count, rep_count = lax.axis_size("outer"), lax.axis_size("rep")
    shard_count = lax.axis_size("shard")
    entries = shard_count * blocks * rep_count * sub_rows * width
    clip_limit = 0.5 * math.sqrt(entries)
    widths = regions(width, pod_count)
    w1, w2, w3 = widths
    part, deep = width // pod_count, pod_count * w3
    group = pod_count * rep_count
    copies = blocks * HALVES * 39 + 2 * pod_count + group + shard_count
    vmem = pl.BlockSpec(memory_space=pltpu.VMEM)
    bf16, f32 = jnp.bfloat16, jnp.float32
    V = pltpu.VMEM
    out, new_momentum, new_master = pl.pallas_call(
        functools.partial(kernel, (HALVES, widths), (pod_count, rep_count, shard_count), clip_limit),
        out_shape=(
            V((blocks, rep_count, sub_rows, width), bf16),
            V(master.shape[2:], f32),
            V(master.shape[2:], f32),
        ),
        in_specs=[pl.BlockSpec(memory_space=pltpu.SMEM), vmem, vmem, vmem],
        out_specs=(vmem, vmem, vmem),
        scratch_shapes=[
            [V((SIDE, blocks, rep_count, sub_rows, w), bf16) for w in (w1, w2)],
            [V((blocks, rep_count, sub_rows, w), bf16) for w in (w1, w2)],
            [V((blocks, rep_count, sub_rows, w), bf16) for w in (w1, w2)],
            V((blocks, rep_count, sub_rows, w1 + w2), bf16),
            V((rep_count - 1, blocks, sub_rows, w1 + w2), bf16),
            V((3, blocks, sub_rows, deep), bf16),
            V((2, blocks, sub_rows, deep), bf16),
            V((blocks, sub_rows, deep), bf16),
            V((3, blocks, sub_rows, deep), bf16),
            V((blocks, sub_rows, deep), bf16),
            V((pod_count - 1, blocks, sub_rows, w3), bf16),
            V((pod_count, slots, sub_rows, part), bf16),
            V((pod_count, slots, sub_rows, part), bf16),
            V((blocks, sub_rows, part), bf16),
            V((pod_count, slots, sub_rows, part), bf16),
            V((pod_count, slots, sub_rows, part), bf16),
            V((1, 8, 128), f32),
            V((group + shard_count, 1, 128), f32),
            pltpu.SemaphoreType.DMA((copies,)),
            pltpu.SemaphoreType.DMA((copies,)),
        ],
        compiler_params=pltpu.CompilerParams(
            collective_id=0, has_side_effects=True, vmem_limit_bytes=48 * 1024 * 1024
        ),
    )(
        owners[0, :, 0],
        deltas.reshape(blocks, rep_count, sub_rows, width),
        master.reshape(master.shape[2:]),
        momentum.reshape(momentum.shape[2:]),
    )
    return (
        out.reshape(blocks * rep_count * sub_rows, width),
        new_momentum.reshape(momentum.shape),
        new_master.reshape(master.shape),
    )


def local(deltas, owners, master, momentum):
    blocks_here = owners.shape[1]
    slot_count = master.shape[2]
    sub_rows = master.shape[3]
    row_width = deltas.shape[3]
    block_rows = deltas.shape[2] // blocks_here
    pod_count = lax.axis_size("outer")
    rep_count = lax.axis_size("rep")
    owned_blocks = owners[0, :, 0]
    pod_ids = jnp.arange(pod_count, dtype=jnp.int32)
    onehot = (owned_blocks[:, None] == pod_ids[None, :]).astype(jnp.int32)
    rank_all = jnp.cumsum(onehot, axis=0) - onehot
    rank_own = jnp.sum(rank_all * onehot, axis=1)
    slot_ids = jnp.arange(slot_count, dtype=jnp.int32)
    selector = (
        (owned_blocks[None, None, :] == pod_ids[:, None, None])
        & (rank_own[None, None, :] == slot_ids[None, :, None])
    ).astype(jnp.bfloat16)
    local_rows = deltas[0, 0].reshape(blocks_here, block_rows, row_width)
    block_sums = lax.psum_scatter(
        local_rows.astype(jnp.float32).astype(jnp.bfloat16), "rep", scatter_dimension=1, tiled=True
    ).astype(jnp.float32)
    block_sums = block_sums.astype(jnp.bfloat16)
    pod_part = jnp.einsum(
        "ojb,brw->ojrw", selector, block_sums, preferred_element_type=jnp.float32
    ).astype(jnp.bfloat16)
    arrived = lax.all_to_all(pod_part, "outer", split_axis=0, concat_axis=0, tiled=True)
    mean_share = jnp.sum(arrived.astype(jnp.float32), axis=0) / (pod_count * rep_count)
    local_sq = jnp.sum(mean_share * mean_share)
    total_sq = lax.psum(local_sq, ("outer", "rep", "shard"))
    total_entries = lax.axis_size("shard") * blocks_here * block_rows * row_width
    clip_limit = 0.5 * math.sqrt(total_entries)
    factor = jnp.minimum(1.0, clip_limit / jnp.sqrt(total_sq + 1e-06))
    step_part = factor * mean_share[None, None]
    new_momentum = 0.9 * momentum + step_part
    new_master = master - 0.7 * (step_part + 0.9 * new_momentum)
    params_here = new_master.astype(jnp.bfloat16)
    gathered = lax.all_gather(params_here, ("outer", "rep"), axis=0, tiled=True).reshape(
        pod_count, rep_count, slot_count, sub_rows, row_width
    )
    unpacked = jnp.einsum("ojb,oqjrw->bqrw", selector, gathered, preferred_element_type=jnp.float32)
    new_params = unpacked.astype(jnp.bfloat16).reshape(blocks_here * block_rows, row_width)
    return (new_params, new_momentum, new_master)


def solution(mesh):
    fits = mesh.shape["outer"] == SIDE * SIDE and mesh.shape["rep"] == LINE

    def body(deltas, owners, master, momentum):
        blocks = owners.shape[1]
        width, sub_rows = master.shape[4], master.shape[3]
        tiled = width % (SIDE * SIDE * 128) == 0 and width >= 3 * SIDE * SIDE * 128
        tiled = tiled and sub_rows % (TILE * HALVES) == 0
        tiled = tiled and deltas.shape[2] == blocks * LINE * sub_rows
        return (fused if fits and tiled else local)(deltas, owners, master, momentum)

    return jax.shard_map(
        body,
        mesh=mesh,
        in_specs=(
            P("outer", "rep", "shard", None),
            P("shard", None, None),
            P("outer", "shard", None, "rep", None),
            P("outer", "shard", None, "rep", None),
        ),
        out_specs=(
            P("shard", None),
            P("outer", "shard", None, "rep", None),
            P("outer", "shard", None, "rep", None),
        ),
        check_vma=False,
    )
```

```python
import functools
import math

import jax
import jax.numpy as jnp
from jax import lax
from jax.experimental import pallas as pl
from jax.experimental.pallas import tpu as pltpu
from jax.sharding import PartitionSpec as P

DEEP_IN = 0.3
DEEP_OUT = 0.2
TILE = 16
SIDE = 2
LATE = 2
KINDS = 18
LINE = 4


def kernel(
    plan, axis_sizes, clip_limit,
    owners_far, deltas_far, master_far, momentum_far,
    out, new_momentum, new_master,
    owners, deltas, master, momentum, load_sem, first, passed, second, zin, zrecv,
    staged, near, far, last, onward, ztotal, cross,
    apack, arecv, mean, packed, slotted, squares, others,
    send_sem, recv_sem,
):
    wa, wb, wc, ws = plan
    pod_count, rep_count, shard_count = axis_sizes
    blocks, sub_rows, slots = deltas.shape[0], master.shape[1], master.shape[0]
    widths = (wa, wb, wc)
    base = (0, pod_count * wa, pod_count * (wa + wb))
    offset = (0, wa, wa + wb)
    pair = (wa, ws)
    pair_width, deep_width = wa + ws, wb - ws + wc
    o, q, s = lax.axis_index("outer"), lax.axis_index("rep"), lax.axis_index("shard")
    y, x = o // SIDE, o % SIDE
    neighbour = {"x": y * SIDE + 1 - x, "y": (1 - y) * SIDE + x}
    is_low = q < rep_count // 2
    tip = jnp.where(is_low, 0, rep_count - 1)
    is_tip = q == tip

    def place(k):
        return jnp.where(is_low, k, rep_count - 1 - k)

    def pod(d):
        return ((y + d // SIDE) % SIDE) * SIDE + (x + d % SIDE) % SIDE

    barrier = pltpu.get_barrier_semaphore()
    peers = []
    for d in range(pod_count):
        for e in range(rep_count):
            if d or e:
                peers.append({"outer": pod(d), "rep": (q + e) % rep_count})
    peers += [{"shard": (s + d) % shard_count} for d in range(1, shard_count)]
    for peer in peers:
        pl.semaphore_signal(barrier, inc=1, device_id=peer, device_id_type=pl.DeviceIdType.MESH)
    loads = [
        pltpu.make_async_copy(deltas_far.at[b], deltas.at[b], load_sem.at[b]) for b in range(blocks)
    ]
    loads.append(pltpu.make_async_copy(master_far, master, load_sem.at[blocks]))
    loads.append(pltpu.make_async_copy(momentum_far, momentum, load_sem.at[blocks + 1]))
    loads.append(pltpu.make_async_copy(owners_far, owners, load_sem.at[blocks + 2]))
    for load in loads:
        load.start()
    pl.semaphore_wait(barrier, len(peers))

    numbers, sent, roles = {}, {}, {}

    def copy(group, src, dst, **to):
        kind = group[0]
        number = numbers.setdefault(group, len(numbers))
        sent.setdefault(kind, len(sent))
        return pltpu.make_async_remote_copy(
            src_ref=src, dst_ref=dst, send_sem=send_sem.at[sent[kind]], recv_sem=recv_sem.at[number],
            device_id=to, device_id_type=pl.DeviceIdType.MESH,
        )

    def send(group, src, dst, **to):
        roles[group[0]] = None
        copy(group, src, dst, **to).start()

    def send_if(role, group, src, dst, **to):
        roles[group[0]] = role
        pl.when(role)(copy(group, src, dst, **to).start)

    def arrive(group, like):
        copy(group, like, like, rep=q).wait_recv()

    def leave(kind, like):
        made = pltpu.make_async_remote_copy(
            src_ref=like, dst_ref=like, send_sem=send_sem.at[sent[kind]], recv_sem=recv_sem.at[0],
            device_id={"rep": q}, device_id_type=pl.DeviceIdType.MESH,
        )
        if roles[kind] is None:
            made.wait_send()
        else:
            pl.when(roles[kind])(made.wait_send)

    def loop(count, body):
        def step(i, carry):
            body(i)
            return carry

        lax.fori_loop(0, count, step, 0)

    def up(value):
        return value.astype(jnp.float32)

    def down(value):
        return value.astype(jnp.bfloat16)

    def cols(region, k):
        width = widths[region]
        return pl.ds(pl.multiple_of(base[region] + k * width, 128), width)

    def pair_cols(r, k):
        return pl.ds(pl.multiple_of(base[r] + k * widths[r], 128), pair[r])

    def local_cols(region):
        return pl.ds(offset[region], widths[region])

    def pair_local(r):
        return pl.ds(offset[r], pair[r])

    def deep_cols(k):
        return pl.ds(pl.multiple_of(k * deep_width, 128), deep_width)

    def order(region, b):
        return ("x", "y") if (region + b) % 2 == 0 else ("y", "x")

    def at_rows(g):
        return slice(None) if g is None else (q + g) % rep_count

    def each(g, body):
        if g is None:
            loop(rep_count, body)
        else:
            body((q + g) % rep_count)

    tail = (None,)
    others_of = tuple(range(1, rep_count))

    def late(b):
        return b >= blocks - LATE

    whole = pl.ds(base[2], pod_count * wc)

    def quarter(axis, j, away):
        if axis == "x":
            return j * SIDE + (1 - x if away else x)
        return (1 - y if away else y) * SIDE + j

    def stay(axis):
        return y if axis == "x" else x

    def send_first(b, g):
        i = at_rows(g)
        for r in range(2):
            axis = order(r, b)[0]
            for j in range(SIDE):
                send(
                    ("first", b, g), deltas.at[b, i, :, pair_cols(r, quarter(axis, j, True))],
                    first[r].at[j, b, i], outer=neighbour[axis],
                )

    def send_second(b, g):
        arrive(("first", b, g), deltas.at[b, at_rows(g), :, pl.ds(0, SIDE * pair_width)])
        for r in range(2):
            axis, other = order(r, b)
            go = 1 - stay(axis)
            at = pair_cols(r, quarter(axis, go, False))

            def body(i):
                passed[r][b, i] = down(up(deltas[b, i, :, at]) + up(first[r][go, b, i]))

            each(g, body)
            i = at_rows(g)
            send(("second", b, g), passed[r].at[b, i], second[r].at[b, i], outer=neighbour[other])

    def pair_total(r, b, i):
        total = up(deltas[b, i, :, pair_cols(r, o)]) + up(first[r][stay(order(r, b)[0]), b, i])
        return total + up(second[r][b, i])

    def send_third(b):
        groups = others_of if late(b) else tail
        for g in groups:
            arrive(("second", b, g), deltas.at[b, at_rows(g), :, pl.ds(0, pair_width)])
        for d in others_of:
            there = (q + d) % rep_count
            for r in range(2):
                zin[b, d - 1, :, pair_local(r)] = down(pair_total(r, b, there))
            send(("third", b), zin.at[b, d - 1], zrecv.at[d - 1, b], rep=there)

    def deep_of(b, i):
        parts = []
        for k in range(pod_count):
            parts.append(deltas[b, i, :, pl.ds(base[1] + k * wb + ws, wb - ws)])
            parts.append(deltas[b, i, :, pl.ds(base[2] + k * wc, wc)])
        return jnp.concatenate([p for p in parts if p.shape[-1]], axis=-1)

    def start_tips(b):
        @pl.when(is_tip)
        def _():
            for k in (3, 2, 1):
                staged[k - 1, b] = deep_of(b, place(k))
                copy(("near", b, k), staged.at[k - 1, b], near.at[k - 1, b], rep=place(1)).start()

        roles["near"] = is_tip

    def relay_near(b):
        @pl.when(jnp.logical_not(is_tip))
        def _():
            for k in (3, 2):
                arrive(("near", b, k), near.at[k - 1, b])
                onward[k - 1, b] = down(up(deep_of(b, place(k))) + up(near[k - 1, b]))
                copy(("far", b, 3 - k), onward.at[k - 1, b], far.at[3 - k, b], rep=place(2)).start()

        roles["far"] = jnp.logical_not(is_tip)

    def relay_far(b):
        @pl.when(jnp.logical_not(is_tip))
        def _():
            arrive(("far", b, 0), far.at[0, b])
            onward[0, b] = down(up(deep_of(b, place(0))) + up(far[0, b]))
            copy(("last", b), onward.at[0, b], last.at[b], rep=place(0)).start()

        roles["last"] = jnp.logical_not(is_tip)

    def send_cross(b):
        @pl.when(is_tip)
        def _():
            arrive(("last", b), last.at[b])
            ztotal[b] = down(up(deep_of(b, q)) + up(last[b]))

        @pl.when(jnp.logical_not(is_tip))
        def _():
            arrive(("near", b, 1), near.at[0, b])
            arrive(("far", b, 1), far.at[1, b])
            ztotal[b] = down(up(deep_of(b, q)) + up(near[0, b]) + up(far[1, b]))

        for d in range(1, pod_count):
            send(("cross", b), ztotal.at[b, :, deep_cols(pod(d))], cross.at[d - 1, b], outer=pod(d))

    scale = 1.0 / (pod_count * rep_count)

    def put_mean(b, at, total):
        value = total * scale
        mean[b, :, at] = down(value)
        square = value * value
        part = squares[0]
        height, width = square.shape
        for k in range(height // 8):
            for i in range(width // 128):
                part = part + square[k * 8:(k + 1) * 8, i * 128:(i + 1) * 128]
        squares[0] = part

    def finish_pair(b):
        if late(b):
            arrive(("second", b, 0), deltas.at[b, q, :, pl.ds(0, pair_width)])
        arrive(("third", b), zrecv.at[:, b])
        for r in range(2):
            total = pair_total(r, b, q)
            for d in range(rep_count - 1):
                total = total + up(zrecv[d, b, :, pair_local(r)])
            put_mean(b, pair_local(r), total)

    def finish_cross(b):
        arrive(("cross", b), cross.at[:, b])
        total = up(ztotal[b, :, deep_cols(o)])
        for d in range(pod_count - 1):
            total = total + up(cross[d, b])
        put_mean(b, pl.ds(pair_width, deep_width), total)

    owner, rank = [], []

    def read_owners():
        loads[blocks + 2].wait()
        owner.extend(owners[b] for b in range(blocks))
        for b in range(blocks):
            count = jnp.int32(0)
            for before in range(b):
                count = count + (owner[before] == owner[b]).astype(jnp.int32)
            rank.append(count)

    def block_of(k, j):
        index, found = jnp.int32(0), jnp.int32(0)
        for b in range(blocks):
            match = ((owner[b] == k) & (rank[b] == j)).astype(jnp.int32)
            index, found = index + b * match, found + match
        return index, found

    def load_rows(b):
        loads[b].wait()

    def pack_early():
        loads[blocks].wait()
        loads[blocks + 1].wait()
        for k in range(pod_count):
            for r in range(3):
                at = pl.ds(base[r] + k * widths[r], widths[r])

                def body(i):
                    value = master[i, :, at] - 0.567 * momentum[i, :, at]
                    apack[k, i, :, local_cols(r)] = down(value)

                loop(slots, body)
        arecv[o] = apack[o]

    def send_early():
        for d in range(1, pod_count):
            send(("early",), apack.at[pod(d)], arecv.at[o], outer=pod(d))

    group = pod_count * rep_count

    def norm_send():
        others[0] = jnp.sum(squares[0], axis=0, keepdims=True)
        for d in range(pod_count):
            for e in range(rep_count):
                if d or e:
                    send(
                        ("norm",), others.at[0], others.at[d * rep_count + e],
                        outer=pod(d), rep=(q + e) % rep_count,
                    )

    def mean_send():
        for d in range(pod_count):
            for j in range(slots):
                index = block_of(pod(d), j)[0]
                packed[d, j] = mean[index]
            if d == 0:
                slotted[o] = packed[0]
            else:
                send(("slot",), packed.at[d], slotted.at[o], outer=pod(d))

    def norm_wait():
        arrive(("norm",), others.at[pl.ds(1, group - 1)])
        total = others[0]
        for d in range(1, group):
            total = total + others[d]
        others[group] = total
        for d in range(1, shard_count):
            send(("shard",), others.at[group], others.at[group + d], shard=(s + d) % shard_count)
        arrive(("early",), arecv.at[pl.ds(1, pod_count - 1)])

    def norm_shard():
        arrive(("shard",), others.at[pl.ds(group + 1, shard_count - 1)])
        total = others[group]
        for d in range(1, shard_count):
            total = total + others[group + d]
        total = jnp.sum(total, keepdims=True)
        return jnp.minimum(1.0, clip_limit / jnp.sqrt(total + 1e-06))

    def spread(b, factor):
        for r in range(3):
            at = local_cols(r)
            early = up(arecv[owner[b], jnp.minimum(rank[b], slots - 1), :, at])
            value = early - (1.33 * factor) * up(mean[b, :, at])
            out[b, q, :, cols(r, o)] = down(value)

    def send_wide(b):
        for d in range(1, pod_count):
            at = out.at[b, q, :, cols(2, o)]
            send(("wide", b), at, at, outer=pod(d))

    def send_line(b):
        for d in others_of:
            for r in range(2):
                at = out.at[b, q, :, cols(r, o)]
                send(("line", b, d), at, at, rep=(q + d) % rep_count)

    middle = jnp.logical_not(is_tip)

    def line(b):
        arrive(("wide", b), out.at[b, q, :, pl.ds(0, (pod_count - 1) * wc)])
        mine = out.at[b, q, :, whole]
        send_if(is_tip, ("outward", b, 0), mine, mine, rep=place(1))
        send_if(middle, ("across", b, 1), mine, mine, rep=place(2))
        send_if(middle, ("inward",), mine, mine, rep=place(0))

    def line_across(b):
        at = out.at[b, place(0), :, whole]
        pl.when(middle)(lambda: arrive(("outward", b, 0), at))
        send_if(middle, ("across", b, 0), at, at, rep=place(2))
        at2 = out.at[b, place(2), :, whole]
        pl.when(middle)(lambda: arrive(("across", b, 1), at2))
        send_if(middle, ("inward",), at2, at2, rep=place(0))

    def line_inward(b):
        at = out.at[b, place(3), :, whole]
        pl.when(middle)(lambda: arrive(("across", b, 0), at))
        send_if(middle, ("inward",), at, at, rep=place(0))

    def line_end():
        pl.when(is_tip)(lambda: arrive(("inward",), out.at[:, pl.ds(0, 3), :, whole]))

    def send_block(b, d):
        i = (q + rep_count - d) % rep_count
        if d:
            arrive(("line", b, d), out.at[b, i, :, pl.ds(0, wa + wb)])
        for r in range(2):
            at = out.at[b, i, :, cols(r, o)]
            send(("block", b, d), at, at, outer=neighbour[order(r, b)[1]])

    def send_blocks(b, d):
        i = (q + rep_count - d) % rep_count
        arrive(("block", b, d), out.at[b, i, :, pl.ds(0, wa + wb)])
        for r in range(2):
            axis = order(r, b)[0]
            for j in range(SIDE):
                at = out.at[b, i, :, cols(r, quarter(axis, j, False))]
                send(("blocks",), at, at, outer=neighbour[axis])

    def update(factor):
        arrive(("slot",), slotted.at[pl.ds(1, pod_count - 1)])
        for j in range(slots):
            found = block_of(o, j)[1].astype(jnp.float32)
            for k in range(pod_count):
                for r in range(3):
                    at = pl.ds(base[r] + k * widths[r], widths[r])
                    step = (factor * found) * up(slotted[k, j, :, local_cols(r)])
                    moved = 0.9 * momentum[j, :, at] + step
                    new_momentum[j, :, at] = moved
                    new_master[j, :, at] = master[j, :, at] - 0.7 * (step + 0.9 * moved)

    def finish():
        arrive(("blocks",), out.at[:, :, :, pl.ds(0, SIDE * (wa + wb))])

    def drain():
        leave("first", deltas.at[:, :, :, pl.ds(0, SIDE * pair_width)])
        leave("second", deltas.at[:, :, :, pl.ds(0, pair_width)])
        leave("third", zin)
        leave("near", staged)
        leave("far", far)
        leave("last", last)
        leave("cross", cross)
        leave("early", arecv.at[pl.ds(1, pod_count - 1)])
        leave("norm", others.at[pl.ds(1, group - 1)])
        leave("slot", slotted.at[pl.ds(1, pod_count - 1)])
        leave("shard", others.at[pl.ds(group + 1, shard_count - 1)])
        leave("wide", out.at[:, 0, :, pl.ds(0, (pod_count - 1) * wc)])
        leave("line", out.at[:, pl.ds(0, rep_count - 1), :, pl.ds(0, wa + wb)])
        leave("outward", out.at[:, 0, :, whole])
        leave("across", out.at[:, pl.ds(0, 2), :, whole])
        leave("inward", out.at[:, pl.ds(0, 3), :, whole])
        leave("block", out.at[:, :, :, pl.ds(0, wa + wb)])
        leave("blocks", out.at[:, :, :, pl.ds(0, SIDE * (wa + wb))])

    squares[0] = jnp.zeros(squares.shape[1:], jnp.float32)
    def firsts(b):
        for g in others_of if late(b) else tail:
            send_first(b, g)

    def seconds(b):
        for g in others_of if late(b) else tail:
            send_second(b, g)

    for b in range(blocks):
        load_rows(b)
        if b < 2:
            firsts(b)
        if b > 0:
            start_tips(b - 1)
    start_tips(blocks - 1)
    pack_early()
    read_owners()
    for t in range(blocks + 2):
        if t < blocks:
            relay_near(t)
            seconds(t)
        if t + 2 < blocks:
            firsts(t + 2)
            if t + 3 == blocks:
                for b in range(blocks - LATE, blocks):
                    send_first(b, 0)
        if 0 <= t - 1 < blocks:
            if t == blocks:
                send_early()
                for b in range(blocks - LATE, blocks):
                    send_second(b, 0)
                send_third(t - 1)
                relay_far(t - 1)
            else:
                relay_far(t - 1)
                send_third(t - 1)
        if 0 <= t - 2 < blocks:
            send_cross(t - 2)
    for b in range(blocks):
        finish_pair(b)
        finish_cross(b)
    norm_send()
    mean_send()
    norm_wait()
    factor = norm_shard()
    for b in range(blocks):
        spread(b, factor)
        send_wide(b)
        send_block(b, 0)
        if b == 0:
            send_line(0)
    for b in range(blocks):
        line(b)
        for later in {0: (1,), 1: (2, 3)}.get(b, ()):
            send_line(later)
    for b in range(blocks):
        send_blocks(b, 0)
    for b in range(blocks):
        for d in others_of:
            send_block(b, d)
        line_across(b)
        for d in others_of:
            send_blocks(b, d)
        if b == 1:
            update(factor)
    for b in range(blocks):
        line_inward(b)
    line_end()
    finish()
    drain()
    assert len(numbers) == recv_sem.shape[0] and len(sent) == send_sem.shape[0]


def store(*refs):
    sem = refs[-1]
    copies = [pltpu.make_async_copy(refs[i], refs[i + 3], sem.at[i]) for i in range(3)]
    for copy in copies:
        copy.start()
    for copy in copies:
        copy.wait()


def regions(width, pod_count):
    tiles = width // (128 * pod_count)
    deep = round(tiles * DEEP_IN)
    wc = min(deep, round(tiles * DEEP_OUT))
    wb = (tiles - wc) // 2
    return tuple(128 * n for n in (tiles - wc - wb, wb, wc, wb - (deep - wc)))


def fused(deltas, owners, master, momentum):
    blocks = owners.shape[1]
    slots, sub_rows, width = master.shape[2:]
    pod_count, rep_count = lax.axis_size("outer"), lax.axis_size("rep")
    shard_count = lax.axis_size("shard")
    entries = shard_count * blocks * rep_count * sub_rows * width
    clip_limit = 0.5 * math.sqrt(entries)
    widths = regions(width, pod_count)
    wa, wb, wc, ws = widths
    part, deep_width = width // pod_count, wb - ws + wc
    deep = pod_count * deep_width
    group = pod_count * rep_count
    waits = 2 * (blocks + (rep_count - 1) * LATE) + 8 * blocks + 4 + blocks * (2 * rep_count + 3) + 2
    vmem, hbm = pl.BlockSpec(memory_space=pltpu.VMEM), pl.BlockSpec(memory_space=pltpu.HBM)
    bf16, f32 = jnp.bfloat16, jnp.float32
    V = pltpu.VMEM
    out, new_momentum, new_master = pl.pallas_call(
        functools.partial(kernel, widths, (pod_count, rep_count, shard_count), clip_limit),
        out_shape=(
            V((blocks, rep_count, sub_rows, width), bf16),
            V(master.shape[2:], f32),
            V(master.shape[2:], f32),
        ),
        in_specs=[hbm] * 4,
        out_specs=(vmem, vmem, vmem),
        scratch_shapes=[
            pltpu.SMEM((blocks,), jnp.int32),
            V((blocks, rep_count, sub_rows, width), bf16),
            V(master.shape[2:], f32),
            V(master.shape[2:], f32),
            pltpu.SemaphoreType.DMA((blocks + 3,)),
            [V((SIDE, blocks, rep_count, sub_rows, w), bf16) for w in (wa, ws)],
            [V((blocks, rep_count, sub_rows, w), bf16) for w in (wa, ws)],
            [V((blocks, rep_count, sub_rows, w), bf16) for w in (wa, ws)],
            V((blocks, rep_count - 1, sub_rows, wa + ws), bf16),
            V((rep_count - 1, blocks, sub_rows, wa + ws), bf16),
            V((3, blocks, sub_rows, deep), bf16),
            V((3, blocks, sub_rows, deep), bf16),
            V((2, blocks, sub_rows, deep), bf16),
            V((blocks, sub_rows, deep), bf16),
            V((3, blocks, sub_rows, deep), bf16),
            V((blocks, sub_rows, deep), bf16),
            V((pod_count - 1, blocks, sub_rows, deep_width), bf16),
            V((pod_count, slots, sub_rows, part), bf16),
            V((pod_count, slots, sub_rows, part), bf16),
            V((blocks, sub_rows, part), bf16),
            V((pod_count, slots, sub_rows, part), bf16),
            V((pod_count, slots, sub_rows, part), bf16),
            V((1, 8, 128), f32),
            V((group + shard_count, 1, 128), f32),
            pltpu.SemaphoreType.DMA((KINDS,)),
            pltpu.SemaphoreType.DMA((waits,)),
        ],
        compiler_params=pltpu.CompilerParams(
            collective_id=0, has_side_effects=True, vmem_limit_bytes=48 * 1024 * 1024
        ),
    )(
        owners[0, :, 0],
        deltas.reshape(blocks, rep_count, sub_rows, width),
        master.reshape(master.shape[2:]),
        momentum.reshape(momentum.shape[2:]),
    )
    arrays = (out, new_momentum, new_master)
    out, new_momentum, new_master = pl.pallas_call(
        store,
        out_shape=tuple(jax.ShapeDtypeStruct(a.shape, a.dtype) for a in arrays),
        in_specs=[pl.BlockSpec(memory_space=pl.ANY)] * 3,
        out_specs=(hbm,) * 3,
        scratch_shapes=[pltpu.SemaphoreType.DMA((3,))],
        compiler_params=pltpu.CompilerParams(vmem_limit_bytes=4 * 1024 * 1024),
    )(*(pltpu.with_memory_space_constraint(a, pltpu.VMEM) for a in arrays))
    return (
        out.reshape(blocks * rep_count * sub_rows, width),
        new_momentum.reshape(momentum.shape),
        new_master.reshape(master.shape),
    )


def local(deltas, owners, master, momentum):
    blocks_here = owners.shape[1]
    slot_count = master.shape[2]
    sub_rows = master.shape[3]
    row_width = deltas.shape[3]
    block_rows = deltas.shape[2] // blocks_here
    pod_count = lax.axis_size("outer")
    rep_count = lax.axis_size("rep")
    owned_blocks = owners[0, :, 0]
    pod_ids = jnp.arange(pod_count, dtype=jnp.int32)
    onehot = (owned_blocks[:, None] == pod_ids[None, :]).astype(jnp.int32)
    rank_all = jnp.cumsum(onehot, axis=0) - onehot
    rank_own = jnp.sum(rank_all * onehot, axis=1)
    slot_ids = jnp.arange(slot_count, dtype=jnp.int32)
    selector = (
        (owned_blocks[None, None, :] == pod_ids[:, None, None])
        & (rank_own[None, None, :] == slot_ids[None, :, None])
    ).astype(jnp.bfloat16)
    local_rows = deltas[0, 0].reshape(blocks_here, block_rows, row_width)
    block_sums = lax.psum_scatter(
        local_rows.astype(jnp.float32).astype(jnp.bfloat16), "rep", scatter_dimension=1, tiled=True
    ).astype(jnp.float32)
    block_sums = block_sums.astype(jnp.bfloat16)
    pod_part = jnp.einsum(
        "ojb,brw->ojrw", selector, block_sums, preferred_element_type=jnp.float32
    ).astype(jnp.bfloat16)
    arrived = lax.all_to_all(pod_part, "outer", split_axis=0, concat_axis=0, tiled=True)
    mean_share = jnp.sum(arrived.astype(jnp.float32), axis=0) / (pod_count * rep_count)
    local_sq = jnp.sum(mean_share * mean_share)
    total_sq = lax.psum(local_sq, ("outer", "rep", "shard"))
    total_entries = lax.axis_size("shard") * blocks_here * block_rows * row_width
    clip_limit = 0.5 * math.sqrt(total_entries)
    factor = jnp.minimum(1.0, clip_limit / jnp.sqrt(total_sq + 1e-06))
    step_part = factor * mean_share[None, None]
    new_momentum = 0.9 * momentum + step_part
    new_master = master - 0.7 * (step_part + 0.9 * new_momentum)
    params_here = new_master.astype(jnp.bfloat16)
    gathered = lax.all_gather(params_here, ("outer", "rep"), axis=0, tiled=True).reshape(
        pod_count, rep_count, slot_count, sub_rows, row_width
    )
    unpacked = jnp.einsum("ojb,oqjrw->bqrw", selector, gathered, preferred_element_type=jnp.float32)
    new_params = unpacked.astype(jnp.bfloat16).reshape(blocks_here * block_rows, row_width)
    return (new_params, new_momentum, new_master)


def solution(mesh):
    fits = mesh.shape["outer"] == SIDE * SIDE and mesh.shape["rep"] == LINE

    def body(deltas, owners, master, momentum):
        blocks = owners.shape[1]
        width, sub_rows = master.shape[4], master.shape[3]
        tiled = width % (SIDE * SIDE * 128) == 0 and width >= 3 * SIDE * SIDE * 128
        tiled = tiled and sub_rows % TILE == 0 and blocks == SIDE * SIDE
        tiled = tiled and deltas.shape[2] == blocks * LINE * sub_rows
        return (fused if fits and tiled else local)(deltas, owners, master, momentum)

    return jax.shard_map(
        body,
        mesh=mesh,
        in_specs=(
            P("outer", "rep", "shard", None),
            P("shard", None, None),
            P("outer", "shard", None, "rep", None),
            P("outer", "shard", None, "rep", None),
        ),
        out_specs=(
            P("shard", None),
            P("outer", "shard", None, "rep", None),
            P("outer", "shard", None, "rep", None),
        ),
        check_vma=False,
    )
```

```python
import functools
import math

import jax
import jax.numpy as jnp
from jax import lax
from jax.experimental import pallas as pl
from jax.experimental.pallas import tpu as pltpu
from jax.sharding import PartitionSpec as P

DEEP = 0.2
EXTRA = 1
TILE = 16
SIDE = 2
LATE = 2
KINDS = 20
LINE = 4


def kernel(
    plan, axis_sizes, clip_limit,
    owners_far, deltas_far, master_far, momentum_far,
    out, new_momentum, new_master,
    owners, deltas, master, momentum, load_sem, first, passed, second, zin, zrecv,
    staged, near, far, last, onward, ztotal, cross,
    apack, arecv, mean, packed, slotted, squares, others,
    send_sem, recv_sem, ready,
):
    wa, wb, wc, extra = plan
    pod_count, rep_count, shard_count = axis_sizes
    blocks, sub_rows, slots = deltas.shape[0], master.shape[1], master.shape[0]
    widths = (wa, wb, wc)
    base = (0, pod_count * wa, pod_count * (wa + wb))
    offset = (0, wa, wa + wb)

    def pair(b):
        return (wa, wb - extra if b < blocks // 2 else wb)

    def pair_width(b):
        return sum(pair(b))

    def deep_width(b):
        return wa + wb + wc - pair_width(b)

    def part(r, b):
        return pl.ds(0, pair(b)[r])

    def deep(b):
        return pl.ds(0, pod_count * deep_width(b))

    o, q, s = lax.axis_index("outer"), lax.axis_index("rep"), lax.axis_index("shard")
    y, x = o // SIDE, o % SIDE
    neighbour = {"x": y * SIDE + 1 - x, "y": (1 - y) * SIDE + x}
    is_low = q < rep_count // 2
    tip = jnp.where(is_low, 0, rep_count - 1)
    is_tip = q == tip

    def place(k):
        return jnp.where(is_low, k, rep_count - 1 - k)

    def pod(d):
        return ((y + d // SIDE) % SIDE) * SIDE + (x + d % SIDE) % SIDE

    barrier = pltpu.get_barrier_semaphore()

    def greet(sem, **to):
        pl.semaphore_signal(sem, inc=1, device_id=to, device_id_type=pl.DeviceIdType.MESH)

    middle = jnp.logical_not(is_tip)
    greet(barrier, outer=neighbour["x"])
    greet(barrier, outer=neighbour["y"])
    greet(barrier, rep=jnp.where(is_tip, place(1), place(0)))
    pl.when(middle)(lambda: greet(barrier, rep=place(2)))
    for d in range(1, shard_count):
        greet(barrier, shard=(s + d) % shard_count)
    loads = [
        pltpu.make_async_copy(deltas_far.at[b], deltas.at[b], load_sem.at[b]) for b in range(blocks)
    ]
    loads.append(pltpu.make_async_copy(master_far, master, load_sem.at[blocks]))
    loads.append(pltpu.make_async_copy(momentum_far, momentum, load_sem.at[blocks + 1]))
    loads.append(pltpu.make_async_copy(owners_far, owners, load_sem.at[blocks + 2]))
    for load in loads:
        load.start()
    pl.semaphore_wait(barrier, jnp.where(is_tip, 3, 4) + shard_count - 1)
    pl.when(middle)(lambda: greet(ready, rep=place(2)))

    def pass_ready():
        @pl.when(middle)
        def _():
            pl.semaphore_wait(ready, 1)
            greet(ready, rep=place(0))

    def all_ready():
        pl.when(is_tip)(lambda: pl.semaphore_wait(ready, 1))


    sent, roles = {}, {}
    spans, phases = (("slot", 0), ("slot", 1), ("early",), ("norm",), ("shard",)), ({}, {})
    gathers = ("wide", "up", "over", "down", "outward", "across", "inward", "block", "blocks")

    def copy(group, src, dst, **to):
        kind = group[0]
        if group in spans:
            number = spans.index(group)
        else:
            numbers = phases[kind in gathers]
            number = len(spans) + numbers.setdefault(group, len(numbers))
        sent.setdefault(kind, len(sent))
        return pltpu.make_async_remote_copy(
            src_ref=src, dst_ref=dst, send_sem=send_sem.at[sent[kind]], recv_sem=recv_sem.at[number],
            device_id=to, device_id_type=pl.DeviceIdType.MESH,
        )

    def send(group, src, dst, **to):
        roles[group[0]] = None
        copy(group, src, dst, **to).start()

    def send_if(role, group, src, dst, **to):
        roles[group[0]] = role
        pl.when(role)(copy(group, src, dst, **to).start)

    def arrive(group, like):
        copy(group, like, like, rep=q).wait_recv()

    def leave(kind, like):
        made = pltpu.make_async_remote_copy(
            src_ref=like, dst_ref=like, send_sem=send_sem.at[sent[kind]], recv_sem=recv_sem.at[0],
            device_id={"rep": q}, device_id_type=pl.DeviceIdType.MESH,
        )
        if roles[kind] is None:
            made.wait_send()
        else:
            pl.when(roles[kind])(made.wait_send)

    def loop(count, body):
        def step(i, carry):
            body(i)
            return carry

        lax.fori_loop(0, count, step, 0)

    def up(value):
        return value.astype(jnp.float32)

    def down(value):
        return value.astype(jnp.bfloat16)

    def cols(region, k):
        width = widths[region]
        return pl.ds(pl.multiple_of(base[region] + k * width, 128), width)

    def pair_cols(r, b, k):
        return pl.ds(pl.multiple_of(base[r] + k * widths[r], 128), pair(b)[r])

    def local_cols(region):
        return pl.ds(offset[region], widths[region])

    def pair_local(r, b):
        return pl.ds(offset[r], pair(b)[r])

    def deep_cols(b, k):
        return pl.ds(pl.multiple_of(k * deep_width(b), 128), deep_width(b))

    def order(region, b):
        return ("x", "y") if (region + b) % 2 == 0 else ("y", "x")

    def at_rows(g):
        return slice(None) if g is None else (q + g) % rep_count

    def each(g, body):
        if g is None:
            loop(rep_count, body)
        else:
            body((q + g) % rep_count)

    tail = (None,)
    others_of = tuple(range(1, rep_count))

    def late(b):
        return b >= blocks - LATE

    whole = pl.ds(base[2], pod_count * wc)

    def quarter(axis, j, away):
        if axis == "x":
            return j * SIDE + (1 - x if away else x)
        return (1 - y if away else y) * SIDE + j

    def stay(axis):
        return y if axis == "x" else x

    def send_first(b, g):
        i = at_rows(g)
        for r in range(2):
            axis = order(r, b)[0]
            for j in range(SIDE):
                send(
                    ("first", b, g), deltas.at[b, i, :, pair_cols(r, b, quarter(axis, j, True))],
                    first[r].at[j, b, i, :, part(r, b)], outer=neighbour[axis],
                )

    def send_second(b, g):
        arrive(("first", b, g), deltas.at[b, at_rows(g), :, pl.ds(0, SIDE * pair_width(b))])
        for r in range(2):
            axis, other = order(r, b)
            go = 1 - stay(axis)
            at = pair_cols(r, b, quarter(axis, go, False))

            def body(i):
                came = first[r][go, b, i, :, part(r, b)]
                passed[r][b, i, :, part(r, b)] = down(up(deltas[b, i, :, at]) + up(came))

            each(g, body)
            i = at_rows(g)
            send(
                ("second", b, g), passed[r].at[b, i, :, part(r, b)],
                second[r].at[b, i, :, part(r, b)], outer=neighbour[other],
            )

    def pair_total(r, b, i):
        at = part(r, b)
        total = up(deltas[b, i, :, pair_cols(r, b, o)]) + up(first[r][stay(order(r, b)[0]), b, i, :, at])
        return total + up(second[r][b, i, :, at])

    def send_third(b):
        groups = others_of if late(b) else tail
        for g in groups:
            arrive(("second", b, g), deltas.at[b, at_rows(g), :, pl.ds(0, pair_width(b))])
        for d in others_of:
            there = (q + d) % rep_count
            for r in range(2):
                zin[b, d - 1, :, pair_local(r, b)] = down(pair_total(r, b, there))
            at = pl.ds(0, pair_width(b))
            send(("third", b), zin.at[b, d - 1, :, at], zrecv.at[d - 1, b, :, at], rep=there)

    def deep_of(b, i):
        keep = pair(b)[1]
        if keep == wb:
            return deltas[b, i, :, whole]
        parts = []
        for k in range(pod_count):
            parts.append(deltas[b, i, :, pl.ds(base[1] + k * wb + keep, wb - keep)])
            parts.append(deltas[b, i, :, pl.ds(base[2] + k * wc, wc)])
        return jnp.concatenate(parts, axis=-1)

    def start_tips(b):
        @pl.when(is_tip)
        def _():
            for k in (3, 2, 1):
                staged[k - 1, b, :, deep(b)] = deep_of(b, place(k))
                copy(("near", b, k), staged.at[k - 1, b, :, deep(b)], near.at[k - 1, b, :, deep(b)], rep=place(1)).start()

        roles["near"] = is_tip

    def relay_near(b):
        @pl.when(middle)
        def _():
            for k in (3, 2):
                arrive(("near", b, k), near.at[k - 1, b, :, deep(b)])
                onward[k - 1, b, :, deep(b)] = down(up(deep_of(b, place(k))) + up(near[k - 1, b, :, deep(b)]))
                copy(("far", b, 3 - k), onward.at[k - 1, b, :, deep(b)], far.at[3 - k, b, :, deep(b)], rep=place(2)).start()

        roles["far"] = middle

    def relay_far(b):
        @pl.when(middle)
        def _():
            arrive(("far", b, 0), far.at[0, b, :, deep(b)])
            onward[0, b, :, deep(b)] = down(up(deep_of(b, place(0))) + up(far[0, b, :, deep(b)]))
            copy(("last", b), onward.at[0, b, :, deep(b)], last.at[b, :, deep(b)], rep=place(0)).start()

        roles["last"] = middle

    def send_cross(b):
        at = deep(b)

        @pl.when(is_tip)
        def _():
            arrive(("last", b), last.at[b, :, at])
            ztotal[b, :, at] = down(up(deep_of(b, q)) + up(last[b, :, at]))

        @pl.when(middle)
        def _():
            arrive(("near", b, 1), near.at[0, b, :, at])
            arrive(("far", b, 1), far.at[1, b, :, at])
            total = up(deep_of(b, q)) + up(near[0, b, :, at])
            ztotal[b, :, at] = down(total + up(far[1, b, :, at]))

        for d in range(1, pod_count):
            send(
                ("cross", b), ztotal.at[b, :, deep_cols(b, pod(d))],
                cross.at[d - 1, b, :, pl.ds(0, deep_width(b))], outer=pod(d),
            )

    scale = 1.0 / (pod_count * rep_count)

    def put_mean(b, at, total):
        value = total * scale
        mean[b, :, at] = down(value)
        square = value * value
        part = squares[0]
        height, width = square.shape
        for k in range(height // 8):
            for i in range(width // 128):
                part = part + square[k * 8:(k + 1) * 8, i * 128:(i + 1) * 128]
        squares[0] = part

    def finish_pair(b):
        if late(b):
            arrive(("second", b, 0), deltas.at[b, q, :, pl.ds(0, pair_width(b))])
        arrive(("third", b), zrecv.at[:, b, :, pl.ds(0, pair_width(b))])
        for r in range(2):
            total = pair_total(r, b, q)
            for d in range(rep_count - 1):
                total = total + up(zrecv[d, b, :, pair_local(r, b)])
            put_mean(b, pair_local(r, b), total)

    def finish_cross(b):
        at = pl.ds(0, deep_width(b))
        arrive(("cross", b), cross.at[:, b, :, at])
        total = up(ztotal[b, :, deep_cols(b, o)])
        for d in range(pod_count - 1):
            total = total + up(cross[d, b, :, at])
        put_mean(b, pl.ds(pair_width(b), deep_width(b)), total)

    owner, rank = [], []

    def read_owners():
        loads[blocks + 2].wait()
        owner.extend(owners[b] for b in range(blocks))
        for b in range(blocks):
            count = jnp.int32(0)
            for before in range(b):
                count = count + (owner[before] == owner[b]).astype(jnp.int32)
            rank.append(count)

    def block_of(k, j):
        index, found = jnp.int32(0), jnp.int32(0)
        for b in range(blocks):
            match = ((owner[b] == k) & (rank[b] == j)).astype(jnp.int32)
            index, found = index + b * match, found + match
        return index, found

    def load_rows(b):
        loads[b].wait()

    def pack_early():
        loads[blocks].wait()
        loads[blocks + 1].wait()
        for k in range(pod_count):
            for r in range(3):
                at = pl.ds(base[r] + k * widths[r], widths[r])

                def body(i):
                    value = master[i, :, at] - 0.567 * momentum[i, :, at]
                    apack[k, i, :, local_cols(r)] = down(value)

                loop(slots, body)
        arecv[o] = apack[o]

    def send_early():
        for d in range(1, pod_count):
            send(("early",), apack.at[pod(d)], arecv.at[o], outer=pod(d))

    group = pod_count * rep_count

    def norm_send():
        others[0] = jnp.sum(squares[0], axis=0, keepdims=True)
        for d in range(pod_count):
            for e in range(rep_count):
                if d or e:
                    send(
                        ("norm",), others.at[0], others.at[d * rep_count + e],
                        outer=pod(d), rep=(q + e) % rep_count,
                    )

    def mean_send(part):
        at = pl.ds(wa + wb, wc) if part == 0 else pl.ds(0, wa + wb)
        for d in range(pod_count):
            for j in range(slots):
                packed[d, j, :, at] = mean[block_of(pod(d), j)[0], :, at]
            if d == 0:
                slotted[o, :, :, at] = packed[0, :, :, at]
            else:
                send(("slot", part), packed.at[d, :, :, at], slotted.at[o, :, :, at], outer=pod(d))

    def norm_wait():
        arrive(("norm",), others.at[pl.ds(1, group - 1)])
        total = others[0]
        for d in range(1, group):
            total = total + others[d]
        others[group] = total
        for d in range(1, shard_count):
            send(("shard",), others.at[group], others.at[group + d], shard=(s + d) % shard_count)
        arrive(("early",), arecv.at[pl.ds(1, pod_count - 1)])

    def norm_shard():
        arrive(("shard",), others.at[pl.ds(group + 1, shard_count - 1)])
        total = others[group]
        for d in range(1, shard_count):
            total = total + others[group + d]
        total = jnp.sum(total, keepdims=True)
        return jnp.minimum(1.0, clip_limit / jnp.sqrt(total + 1e-06))

    def spread(b, factor):
        for r in range(3):
            at = local_cols(r)
            early = up(arecv[owner[b], jnp.minimum(rank[b], slots - 1), :, at])
            value = early - (1.33 * factor) * up(mean[b, :, at])
            out[b, q, :, cols(r, o)] = down(value)

    def send_wide(b):
        for d in range(1, pod_count):
            at = out.at[b, q, :, cols(2, o)]
            send(("wide", b), at, at, outer=pod(d))

    def pass_line(role, group, b, k, **to):
        for r in range(2):
            at = out.at[b, place(k), :, cols(r, o)]
            send_if(role, group, at, at, **to)

    def line_rows(b, count):
        return out.at[b, pl.ds(0, count), :, pl.ds(0, wa + wb)]

    def send_line(b):
        pass_line(is_tip, ("up", b), b, 0, rep=place(1))
        pass_line(middle, ("down", b), b, 1, rep=place(0))
        pass_line(middle, ("over", b, 1), b, 1, rep=place(2))

    def line_near(b):
        pl.when(middle)(lambda: arrive(("over", b, 1), line_rows(b, 1)))
        pass_line(middle, ("down", b), b, 2, rep=place(0))
        pl.when(middle)(lambda: arrive(("up", b), line_rows(b, 1)))
        pass_line(middle, ("over", b, 0), b, 0, rep=place(2))

    def line_far(b):
        pl.when(middle)(lambda: arrive(("over", b, 0), line_rows(b, 1)))
        pass_line(middle, ("down", b), b, 3, rep=place(0))

    def line(b):
        arrive(("wide", b), out.at[b, q, :, pl.ds(0, (pod_count - 1) * wc)])
        mine = out.at[b, q, :, whole]
        send_if(is_tip, ("outward", b, 0), mine, mine, rep=place(1))
        send_if(middle, ("across", b, 1), mine, mine, rep=place(2))

    def line_across(b):
        at = out.at[b, place(0), :, whole]
        pl.when(middle)(lambda: arrive(("outward", b, 0), at))
        send_if(middle, ("across", b, 0), at, at, rep=place(2))

    def line_inward(b, k):
        at = out.at[b, place(k), :, whole]
        if k > 1:
            pl.when(middle)(lambda: arrive(("across", b, 3 - k), at))
        send_if(middle, ("inward",), at, at, rep=place(0))

    def line_end():
        pl.when(is_tip)(lambda: arrive(("inward",), out.at[:, pl.ds(0, 3), :, whole]))

    def send_block(b, d):
        i = (q + rep_count - d) % rep_count
        for r in range(2):
            at = out.at[b, i, :, cols(r, o)]
            send(("block", b, d), at, at, outer=neighbour[order(r, b)[1]])

    def send_blocks(b, d):
        i = (q + rep_count - d) % rep_count
        arrive(("block", b, d), out.at[b, i, :, pl.ds(0, wa + wb)])
        for r in range(2):
            axis = order(r, b)[0]
            for j in range(SIDE):
                at = out.at[b, i, :, cols(r, quarter(axis, j, False))]
                send(("blocks",), at, at, outer=neighbour[axis])

    def update(factor):
        for part, width in enumerate((wc, wa + wb)):
            arrive(("slot", part), slotted.at[pl.ds(1, pod_count - 1), :, :, pl.ds(0, width)])
        for j in range(slots):
            found = block_of(o, j)[1].astype(jnp.float32)
            for k in range(pod_count):
                for r in range(3):
                    at = pl.ds(base[r] + k * widths[r], widths[r])
                    step = (factor * found) * up(slotted[k, j, :, local_cols(r)])
                    moved = 0.9 * momentum[j, :, at] + step
                    new_momentum[j, :, at] = moved
                    new_master[j, :, at] = master[j, :, at] - 0.7 * (step + 0.9 * moved)

    def finish():
        arrive(("blocks",), out.at[:, :, :, pl.ds(0, SIDE * (wa + wb))])

    def drain():
        pairs = sum(pair_width(b) for b in range(blocks))
        deeps = sum(deep_width(b) for b in range(blocks))
        some = blocks // 2

        def rows(count, width):
            return deltas.at[0, pl.ds(0, count), :, pl.ds(0, width)]

        leave("first", deltas.at[pl.ds(0, some), :, :, pl.ds(0, SIDE * pairs // some)])
        leave("second", deltas.at[pl.ds(0, some), :, :, pl.ds(0, pairs // some)])
        leave("third", rows(rep_count - 1, pairs))
        leave("near", rows(3, pod_count * deeps))
        leave("far", rows(2, pod_count * deeps))
        leave("last", rows(1, pod_count * deeps))
        leave("cross", rows(pod_count - 1, deeps))
        leave("early", arecv.at[pl.ds(1, pod_count - 1)])
        leave("norm", others.at[pl.ds(1, group - 1)])
        leave("slot", slotted.at[pl.ds(1, pod_count - 1)])
        leave("shard", others.at[pl.ds(group + 1, shard_count - 1)])
        leave("wide", out.at[:, 0, :, pl.ds(0, (pod_count - 1) * wc)])
        leave("up", out.at[:, 0, :, pl.ds(0, wa + wb)])
        leave("over", out.at[:, pl.ds(0, 2), :, pl.ds(0, wa + wb)])
        leave("down", out.at[:, pl.ds(0, 3), :, pl.ds(0, wa + wb)])
        leave("outward", out.at[:, 0, :, whole])
        leave("across", out.at[:, pl.ds(0, 2), :, whole])
        leave("inward", out.at[:, pl.ds(0, 3), :, whole])
        leave("block", out.at[:, :, :, pl.ds(0, wa + wb)])
        leave("blocks", out.at[:, :, :, pl.ds(0, SIDE * (wa + wb))])

    def rests(b):
        pl.when(is_tip)(lambda: arrive(("down", b), line_rows(b, 3)))
        for d in others_of:
            send_block(b, d)

    def rests_on(b):
        for d in others_of:
            send_blocks(b, d)

    squares[0] = jnp.zeros(squares.shape[1:], jnp.float32)
    def firsts(b):
        for g in others_of if late(b) else tail:
            send_first(b, g)

    def seconds(b):
        for g in others_of if late(b) else tail:
            send_second(b, g)

    for b in range(blocks):
        load_rows(b)
        if b < 2:
            firsts(b)
        if b > 0:
            start_tips(b - 1)
    start_tips(blocks - 1)
    pack_early()
    read_owners()
    for t in range(blocks + 2):
        if t < blocks:
            relay_near(t)
            if t == 0:
                pass_ready()
            seconds(t)
            if t == 0:
                all_ready()
        if t + 2 < blocks:
            firsts(t + 2)
            if t + 3 == blocks:
                for b in range(blocks - LATE, blocks):
                    send_first(b, 0)
        if 0 <= t - 1 < blocks:
            if t == blocks:
                send_early()
                for b in range(blocks - LATE, blocks):
                    send_second(b, 0)
                send_third(t - 1)
                relay_far(t - 1)
            else:
                relay_far(t - 1)
                send_third(t - 1)
        if 0 <= t - 2 < blocks:
            send_cross(t - 2)
    for b in range(blocks):
        if b < 2:
            finish_pair(b)
        finish_cross(b)
    mean_send(0)
    for b in range(2, blocks):
        finish_pair(b)
    norm_send()
    mean_send(1)
    norm_wait()
    factor = norm_shard()
    for b in range(blocks):
        spread(b, factor)
        send_wide(b)
        send_line(b)
        send_block(b, 0)
    for b in range(blocks):
        line(b)
        send_blocks(b, 0)
        line_near(b)
    line_far(0)
    rests(0)
    line_far(1)
    line_across(0)
    rests(1)
    rests_on(0)
    line_far(2)
    line_across(1)
    rests(2)
    line_far(3)
    rests_on(1)
    rests(3)
    line_across(2)
    line_across(3)
    for b in range(blocks):
        line_inward(b, 1)
        line_inward(b, 2)
    rests_on(2)
    update(factor)
    line_inward(0, 3)
    line_inward(1, 3)
    rests_on(3)
    line_inward(2, 3)
    line_inward(3, 3)
    line_end()
    finish()
    drain()
    assert len(spans) + max(len(p) for p in phases) == recv_sem.shape[0]
    assert len(sent) == send_sem.shape[0]


def store(*refs):
    sem = refs[-1]
    copies = []
    for i in range(3):
        for k in range(refs[i].shape[0]):
            copies.append(pltpu.make_async_copy(refs[i].at[k], refs[i + 3].at[k], sem.at[len(copies)]))
    for copy in copies:
        copy.start()
    for copy in copies:
        copy.wait()


def regions(width, pod_count):
    tiles = width // (128 * pod_count)
    wc = max(1, round(tiles * DEEP))
    wb = (tiles - wc) // 2
    return tuple(128 * n for n in (tiles - wc - wb, wb, wc, EXTRA))


def fused(deltas, owners, master, momentum):
    blocks = owners.shape[1]
    slots, sub_rows, width = master.shape[2:]
    pod_count, rep_count = lax.axis_size("outer"), lax.axis_size("rep")
    shard_count = lax.axis_size("shard")
    entries = shard_count * blocks * rep_count * sub_rows * width
    clip_limit = 0.5 * math.sqrt(entries)
    widths = regions(width, pod_count)
    wa, wb, wc, extra = widths
    part, deep_width = width // pod_count, extra + wc
    deep = pod_count * deep_width
    group = pod_count * rep_count
    reduce_waits = 2 * (blocks + (rep_count - 1) * LATE) + 8 * blocks
    waits = 5 + max(reduce_waits, blocks * (rep_count + 8) + 2)
    vmem, hbm = pl.BlockSpec(memory_space=pltpu.VMEM), pl.BlockSpec(memory_space=pltpu.HBM)
    bf16, f32 = jnp.bfloat16, jnp.float32
    V = pltpu.VMEM
    out, new_momentum, new_master = pl.pallas_call(
        functools.partial(kernel, widths, (pod_count, rep_count, shard_count), clip_limit),
        out_shape=(
            V((blocks, rep_count, sub_rows, width), bf16),
            V(master.shape[2:], f32),
            V(master.shape[2:], f32),
        ),
        in_specs=[hbm] * 4,
        out_specs=(vmem, vmem, vmem),
        scratch_shapes=[
            pltpu.SMEM((blocks,), jnp.int32),
            V((blocks, rep_count, sub_rows, width), bf16),
            V(master.shape[2:], f32),
            V(master.shape[2:], f32),
            pltpu.SemaphoreType.DMA((blocks + 3,)),
            [V((SIDE, blocks, rep_count, sub_rows, w), bf16) for w in (wa, wb)],
            [V((blocks, rep_count, sub_rows, w), bf16) for w in (wa, wb)],
            [V((blocks, rep_count, sub_rows, w), bf16) for w in (wa, wb)],
            V((blocks, rep_count - 1, sub_rows, wa + wb), bf16),
            V((rep_count - 1, blocks, sub_rows, wa + wb), bf16),
            V((3, blocks, sub_rows, deep), bf16),
            V((3, blocks, sub_rows, deep), bf16),
            V((2, blocks, sub_rows, deep), bf16),
            V((blocks, sub_rows, deep), bf16),
            V((3, blocks, sub_rows, deep), bf16),
            V((blocks, sub_rows, deep), bf16),
            V((pod_count - 1, blocks, sub_rows, deep_width), bf16),
            V((pod_count, slots, sub_rows, part), bf16),
            V((pod_count, slots, sub_rows, part), bf16),
            V((blocks, sub_rows, part), bf16),
            V((pod_count, slots, sub_rows, part), bf16),
            V((pod_count, slots, sub_rows, part), bf16),
            V((1, 8, 128), f32),
            V((group + shard_count, 1, 128), f32),
            pltpu.SemaphoreType.DMA((KINDS,)),
            pltpu.SemaphoreType.DMA((waits,)),
            pltpu.SemaphoreType.REGULAR,
        ],
        compiler_params=pltpu.CompilerParams(
            collective_id=0, has_side_effects=True, vmem_limit_bytes=48 * 1024 * 1024
        ),
    )(
        owners[0, :, 0],
        deltas.reshape(blocks, rep_count, sub_rows, width),
        master.reshape(master.shape[2:]),
        momentum.reshape(momentum.shape[2:]),
    )
    arrays = (out, new_momentum, new_master)
    out, new_momentum, new_master = pl.pallas_call(
        store,
        out_shape=tuple(jax.ShapeDtypeStruct(a.shape, a.dtype) for a in arrays),
        in_specs=[pl.BlockSpec(memory_space=pl.ANY)] * 3,
        out_specs=(hbm,) * 3,
        scratch_shapes=[pltpu.SemaphoreType.DMA((blocks + 2 * slots,))],
        compiler_params=pltpu.CompilerParams(vmem_limit_bytes=4 * 1024 * 1024),
    )(*(pltpu.with_memory_space_constraint(a, pltpu.VMEM) for a in arrays))
    return (
        out.reshape(blocks * rep_count * sub_rows, width),
        new_momentum.reshape(momentum.shape),
        new_master.reshape(master.shape),
    )


def local(deltas, owners, master, momentum):
    blocks_here = owners.shape[1]
    slot_count = master.shape[2]
    sub_rows = master.shape[3]
    row_width = deltas.shape[3]
    block_rows = deltas.shape[2] // blocks_here
    pod_count = lax.axis_size("outer")
    rep_count = lax.axis_size("rep")
    owned_blocks = owners[0, :, 0]
    pod_ids = jnp.arange(pod_count, dtype=jnp.int32)
    onehot = (owned_blocks[:, None] == pod_ids[None, :]).astype(jnp.int32)
    rank_all = jnp.cumsum(onehot, axis=0) - onehot
    rank_own = jnp.sum(rank_all * onehot, axis=1)
    slot_ids = jnp.arange(slot_count, dtype=jnp.int32)
    selector = (
        (owned_blocks[None, None, :] == pod_ids[:, None, None])
        & (rank_own[None, None, :] == slot_ids[None, :, None])
    ).astype(jnp.bfloat16)
    local_rows = deltas[0, 0].reshape(blocks_here, block_rows, row_width)
    block_sums = lax.psum_scatter(
        local_rows.astype(jnp.float32).astype(jnp.bfloat16), "rep", scatter_dimension=1, tiled=True
    ).astype(jnp.float32)
    block_sums = block_sums.astype(jnp.bfloat16)
    pod_part = jnp.einsum(
        "ojb,brw->ojrw", selector, block_sums, preferred_element_type=jnp.float32
    ).astype(jnp.bfloat16)
    arrived = lax.all_to_all(pod_part, "outer", split_axis=0, concat_axis=0, tiled=True)
    mean_share = jnp.sum(arrived.astype(jnp.float32), axis=0) / (pod_count * rep_count)
    local_sq = jnp.sum(mean_share * mean_share)
    total_sq = lax.psum(local_sq, ("outer", "rep", "shard"))
    total_entries = lax.axis_size("shard") * blocks_here * block_rows * row_width
    clip_limit = 0.5 * math.sqrt(total_entries)
    factor = jnp.minimum(1.0, clip_limit / jnp.sqrt(total_sq + 1e-06))
    step_part = factor * mean_share[None, None]
    new_momentum = 0.9 * momentum + step_part
    new_master = master - 0.7 * (step_part + 0.9 * new_momentum)
    params_here = new_master.astype(jnp.bfloat16)
    gathered = lax.all_gather(params_here, ("outer", "rep"), axis=0, tiled=True).reshape(
        pod_count, rep_count, slot_count, sub_rows, row_width
    )
    unpacked = jnp.einsum("ojb,oqjrw->bqrw", selector, gathered, preferred_element_type=jnp.float32)
    new_params = unpacked.astype(jnp.bfloat16).reshape(blocks_here * block_rows, row_width)
    return (new_params, new_momentum, new_master)


def solution(mesh):
    fits = mesh.shape["outer"] == SIDE * SIDE and mesh.shape["rep"] == LINE

    def body(deltas, owners, master, momentum):
        blocks = owners.shape[1]
        width, sub_rows = master.shape[4], master.shape[3]
        tiled = width % (SIDE * SIDE * 128) == 0 and width >= 3 * SIDE * SIDE * 128
        tiled = tiled and sub_rows % TILE == 0 and blocks == SIDE * SIDE
        tiled = tiled and deltas.shape[2] == blocks * LINE * sub_rows
        if tiled:
            wa, wb, wc, extra = regions(width, SIDE * SIDE)
            tiled = wb > extra and SIDE * SIDE * blocks * (wc + extra // 2) <= width
        return (fused if fits and tiled else local)(deltas, owners, master, momentum)

    return jax.shard_map(
        body,
        mesh=mesh,
        in_specs=(
            P("outer", "rep", "shard", None),
            P("shard", None, None),
            P("outer", "shard", None, "rep", None),
            P("outer", "shard", None, "rep", None),
        ),
        out_specs=(
            P("shard", None),
            P("outer", "shard", None, "rep", None),
            P("outer", "shard", None, "rep", None),
        ),
        check_vma=False,
    )
```

```python
import functools
import math

import jax
import jax.numpy as jnp
from jax import lax
from jax.experimental import pallas as pl
from jax.experimental.pallas import tpu as pltpu
from jax.sharding import PartitionSpec as P

DEEP = 0.2
EXTRA = 1
THICK = 2
TILE = 16
SIDE = 2
LATE = 2
KINDS = 20
LINE = 4


def kernel(
    plan, axis_sizes, clip_limit,
    owners_far, deltas_far, master_far, momentum_far,
    out, new_momentum, new_master,
    owners, deltas, master, momentum, load_sem, first, passed, second, zin, zrecv,
    staged, near, far, last, onward, ztotal, cross,
    apack, arecv, mean, packed, slotted, squares, others,
    send_sem, recv_sem, ready,
):
    wa, wb, wc, extra = plan
    pod_count, rep_count, shard_count = axis_sizes
    blocks, sub_rows, slots = deltas.shape[0], master.shape[1], master.shape[0]
    widths = (wa, wb, wc)
    base = (0, pod_count * wa, pod_count * (wa + wb))
    offset = (0, wa, wa + wb)

    def pair(b):
        return (wa, wb - extra if b < THICK else wb)

    def pair_width(b):
        return sum(pair(b))

    def deep_width(b):
        return wa + wb + wc - pair_width(b)

    def part(r, b):
        return pl.ds(0, pair(b)[r])

    def deep(b):
        return pl.ds(0, pod_count * deep_width(b))

    o, q, s = lax.axis_index("outer"), lax.axis_index("rep"), lax.axis_index("shard")
    y, x = o // SIDE, o % SIDE
    neighbour = {"x": y * SIDE + 1 - x, "y": (1 - y) * SIDE + x}
    is_low = q < rep_count // 2
    tip = jnp.where(is_low, 0, rep_count - 1)
    is_tip = q == tip

    def place(k):
        return jnp.where(is_low, k, rep_count - 1 - k)

    def pod(d):
        return ((y + d // SIDE) % SIDE) * SIDE + (x + d % SIDE) % SIDE

    barrier = pltpu.get_barrier_semaphore()

    def greet(sem, **to):
        pl.semaphore_signal(sem, inc=1, device_id=to, device_id_type=pl.DeviceIdType.MESH)

    middle = jnp.logical_not(is_tip)
    greet(barrier, outer=neighbour["x"])
    greet(barrier, outer=neighbour["y"])
    greet(barrier, rep=jnp.where(is_tip, place(1), place(0)))
    pl.when(middle)(lambda: greet(barrier, rep=place(2)))
    for d in range(1, shard_count):
        greet(barrier, shard=(s + d) % shard_count)
    loads = [
        pltpu.make_async_copy(deltas_far.at[b], deltas.at[b], load_sem.at[b]) for b in range(blocks)
    ]
    loads.append(pltpu.make_async_copy(master_far, master, load_sem.at[blocks]))
    loads.append(pltpu.make_async_copy(momentum_far, momentum, load_sem.at[blocks + 1]))
    loads.append(pltpu.make_async_copy(owners_far, owners, load_sem.at[blocks + 2]))
    for load in loads:
        load.start()
    pl.semaphore_wait(barrier, jnp.where(is_tip, 3, 4) + shard_count - 1)
    pl.when(middle)(lambda: greet(ready, rep=place(2)))

    def pass_ready():
        @pl.when(middle)
        def _():
            pl.semaphore_wait(ready, 1)
            greet(ready, rep=place(0))

    def all_ready():
        pl.when(is_tip)(lambda: pl.semaphore_wait(ready, 1))


    sent, roles = {}, {}
    spans, phases = (("slot", 0), ("slot", 1), ("early",), ("norm",), ("shard",)), ({}, {})
    gathers = ("wide", "up", "over", "down", "outward", "across", "inward", "block", "blocks")

    def copy(group, src, dst, **to):
        kind = group[0]
        if group in spans:
            number = spans.index(group)
        else:
            numbers = phases[kind in gathers]
            number = len(spans) + numbers.setdefault(group, len(numbers))
        sent.setdefault(kind, len(sent))
        return pltpu.make_async_remote_copy(
            src_ref=src, dst_ref=dst, send_sem=send_sem.at[sent[kind]], recv_sem=recv_sem.at[number],
            device_id=to, device_id_type=pl.DeviceIdType.MESH,
        )

    def send(group, src, dst, **to):
        roles[group[0]] = None
        copy(group, src, dst, **to).start()

    def send_if(role, group, src, dst, **to):
        roles[group[0]] = role
        pl.when(role)(copy(group, src, dst, **to).start)

    def arrive(group, like):
        copy(group, like, like, rep=q).wait_recv()

    def leave(kind, like):
        made = pltpu.make_async_remote_copy(
            src_ref=like, dst_ref=like, send_sem=send_sem.at[sent[kind]], recv_sem=recv_sem.at[0],
            device_id={"rep": q}, device_id_type=pl.DeviceIdType.MESH,
        )
        if roles[kind] is None:
            made.wait_send()
        else:
            pl.when(roles[kind])(made.wait_send)

    def loop(count, body):
        def step(i, carry):
            body(i)
            return carry

        lax.fori_loop(0, count, step, 0)

    def up(value):
        return value.astype(jnp.float32)

    def down(value):
        return value.astype(jnp.bfloat16)

    def cols(region, k):
        width = widths[region]
        return pl.ds(pl.multiple_of(base[region] + k * width, 128), width)

    def pair_cols(r, b, k):
        return pl.ds(pl.multiple_of(base[r] + k * widths[r], 128), pair(b)[r])

    def local_cols(region):
        return pl.ds(offset[region], widths[region])

    def pair_local(r, b):
        return pl.ds(offset[r], pair(b)[r])

    def deep_cols(b, k):
        return pl.ds(pl.multiple_of(k * deep_width(b), 128), deep_width(b))

    def order(region, b):
        return ("x", "y") if (region + b) % 2 == 0 else ("y", "x")

    def at_rows(g):
        return slice(None) if g is None else (q + g) % rep_count

    def each(g, body):
        if g is None:
            loop(rep_count, body)
        else:
            body((q + g) % rep_count)

    tail = (None,)
    others_of = tuple(range(1, rep_count))

    def late(b):
        return b >= blocks - LATE

    whole = pl.ds(base[2], pod_count * wc)

    def quarter(axis, j, away):
        if axis == "x":
            return j * SIDE + (1 - x if away else x)
        return (1 - y if away else y) * SIDE + j

    def stay(axis):
        return y if axis == "x" else x

    def send_first(b, g):
        i = at_rows(g)
        for r in range(2):
            axis = order(r, b)[0]
            for j in range(SIDE):
                send(
                    ("first", b, g), deltas.at[b, i, :, pair_cols(r, b, quarter(axis, j, True))],
                    first[r].at[j, b, i, :, part(r, b)], outer=neighbour[axis],
                )

    def send_second(b, g):
        arrive(("first", b, g), deltas.at[b, at_rows(g), :, pl.ds(0, SIDE * pair_width(b))])
        for r in range(2):
            axis, other = order(r, b)
            go = 1 - stay(axis)
            at = pair_cols(r, b, quarter(axis, go, False))

            def body(i):
                came = first[r][go, b, i, :, part(r, b)]
                passed[r][b, i, :, part(r, b)] = down(up(deltas[b, i, :, at]) + up(came))

            each(g, body)
            i = at_rows(g)
            send(
                ("second", b, g), passed[r].at[b, i, :, part(r, b)],
                second[r].at[b, i, :, part(r, b)], outer=neighbour[other],
            )

    def pair_total(r, b, i):
        at = part(r, b)
        total = up(deltas[b, i, :, pair_cols(r, b, o)]) + up(first[r][stay(order(r, b)[0]), b, i, :, at])
        return total + up(second[r][b, i, :, at])

    def send_third(b):
        groups = others_of if late(b) else tail
        for g in groups:
            arrive(("second", b, g), deltas.at[b, at_rows(g), :, pl.ds(0, pair_width(b))])
        for d in others_of:
            there = (q + d) % rep_count
            for r in range(2):
                zin[b, d - 1, :, pair_local(r, b)] = down(pair_total(r, b, there))
            at = pl.ds(0, pair_width(b))
            send(("third", b), zin.at[b, d - 1, :, at], zrecv.at[d - 1, b, :, at], rep=there)

    def deep_of(b, i):
        keep = pair(b)[1]
        if keep == wb:
            return deltas[b, i, :, whole]
        parts = []
        for k in range(pod_count):
            parts.append(deltas[b, i, :, pl.ds(base[1] + k * wb + keep, wb - keep)])
            parts.append(deltas[b, i, :, pl.ds(base[2] + k * wc, wc)])
        return jnp.concatenate(parts, axis=-1)

    def start_tips(b):
        @pl.when(is_tip)
        def _():
            for k in (3, 2, 1):
                staged[k - 1, b, :, deep(b)] = deep_of(b, place(k))
                copy(("near", b, k), staged.at[k - 1, b, :, deep(b)], near.at[k - 1, b, :, deep(b)], rep=place(1)).start()

        roles["near"] = is_tip

    def relay_near(b):
        @pl.when(middle)
        def _():
            for k in (3, 2):
                arrive(("near", b, k), near.at[k - 1, b, :, deep(b)])
                onward[k - 1, b, :, deep(b)] = down(up(deep_of(b, place(k))) + up(near[k - 1, b, :, deep(b)]))
                copy(("far", b, 3 - k), onward.at[k - 1, b, :, deep(b)], far.at[3 - k, b, :, deep(b)], rep=place(2)).start()

        roles["far"] = middle

    def relay_far(b):
        @pl.when(middle)
        def _():
            arrive(("far", b, 0), far.at[0, b, :, deep(b)])
            onward[0, b, :, deep(b)] = down(up(deep_of(b, place(0))) + up(far[0, b, :, deep(b)]))
            copy(("last", b), onward.at[0, b, :, deep(b)], last.at[b, :, deep(b)], rep=place(0)).start()

        roles["last"] = middle

    def send_cross(b):
        at = deep(b)

        @pl.when(is_tip)
        def _():
            arrive(("last", b), last.at[b, :, at])
            ztotal[b, :, at] = down(up(deep_of(b, q)) + up(last[b, :, at]))

        @pl.when(middle)
        def _():
            arrive(("near", b, 1), near.at[0, b, :, at])
            arrive(("far", b, 1), far.at[1, b, :, at])
            total = up(deep_of(b, q)) + up(near[0, b, :, at])
            ztotal[b, :, at] = down(total + up(far[1, b, :, at]))

        for d in range(1, pod_count):
            send(
                ("cross", b), ztotal.at[b, :, deep_cols(b, pod(d))],
                cross.at[d - 1, b, :, pl.ds(0, deep_width(b))], outer=pod(d),
            )

    scale = 1.0 / (pod_count * rep_count)

    def put_mean(b, at, total):
        value = total * scale
        mean[b, :, at] = down(value)
        square = value * value
        part = squares[0]
        height, width = square.shape
        for k in range(height // 8):
            for i in range(width // 128):
                part = part + square[k * 8:(k + 1) * 8, i * 128:(i + 1) * 128]
        squares[0] = part

    def finish_pair(b):
        if late(b):
            arrive(("second", b, 0), deltas.at[b, q, :, pl.ds(0, pair_width(b))])
        arrive(("third", b), zrecv.at[:, b, :, pl.ds(0, pair_width(b))])
        for r in range(2):
            total = pair_total(r, b, q)
            for d in range(rep_count - 1):
                total = total + up(zrecv[d, b, :, pair_local(r, b)])
            put_mean(b, pair_local(r, b), total)

    def finish_cross(b):
        at = pl.ds(0, deep_width(b))
        arrive(("cross", b), cross.at[:, b, :, at])
        total = up(ztotal[b, :, deep_cols(b, o)])
        for d in range(pod_count - 1):
            total = total + up(cross[d, b, :, at])
        put_mean(b, pl.ds(pair_width(b), deep_width(b)), total)

    owner, rank = [], []

    def read_owners():
        loads[blocks + 2].wait()
        owner.extend(owners[b] for b in range(blocks))
        for b in range(blocks):
            count = jnp.int32(0)
            for before in range(b):
                count = count + (owner[before] == owner[b]).astype(jnp.int32)
            rank.append(count)

    def block_of(k, j):
        index, found = jnp.int32(0), jnp.int32(0)
        for b in range(blocks):
            match = ((owner[b] == k) & (rank[b] == j)).astype(jnp.int32)
            index, found = index + b * match, found + match
        return index, found

    def load_rows(b):
        loads[b].wait()

    def pack_early():
        loads[blocks].wait()
        loads[blocks + 1].wait()
        for k in range(pod_count):
            for r in range(3):
                at = pl.ds(base[r] + k * widths[r], widths[r])

                def body(i):
                    value = master[i, :, at] - 0.567 * momentum[i, :, at]
                    apack[k, i, :, local_cols(r)] = down(value)

                loop(slots, body)
        arecv[o] = apack[o]

    def send_early():
        for d in range(1, pod_count):
            send(("early",), apack.at[pod(d)], arecv.at[o], outer=pod(d))

    group = pod_count * rep_count

    def norm_send():
        others[0] = jnp.sum(squares[0], axis=0, keepdims=True)
        for d in range(pod_count):
            for e in range(rep_count):
                if d or e:
                    send(
                        ("norm",), others.at[0], others.at[d * rep_count + e],
                        outer=pod(d), rep=(q + e) % rep_count,
                    )

    def mean_send(part):
        at = pl.ds(wa + wb, wc) if part == 0 else pl.ds(0, wa + wb)
        for d in range(pod_count):
            for j in range(slots):
                packed[d, j, :, at] = mean[block_of(pod(d), j)[0], :, at]
            if d == 0:
                slotted[o, :, :, at] = packed[0, :, :, at]
            else:
                send(("slot", part), packed.at[d, :, :, at], slotted.at[o, :, :, at], outer=pod(d))

    def norm_wait():
        arrive(("norm",), others.at[pl.ds(1, group - 1)])
        total = others[0]
        for d in range(1, group):
            total = total + others[d]
        others[group] = total
        for d in range(1, shard_count):
            send(("shard",), others.at[group], others.at[group + d], shard=(s + d) % shard_count)
        arrive(("early",), arecv.at[pl.ds(1, pod_count - 1)])

    def norm_shard():
        arrive(("shard",), others.at[pl.ds(group + 1, shard_count - 1)])
        total = others[group]
        for d in range(1, shard_count):
            total = total + others[group + d]
        total = jnp.sum(total, keepdims=True)
        return jnp.minimum(1.0, clip_limit / jnp.sqrt(total + 1e-06))

    def spread(b, factor):
        for r in range(3):
            at = local_cols(r)
            early = up(arecv[owner[b], jnp.minimum(rank[b], slots - 1), :, at])
            value = early - (1.33 * factor) * up(mean[b, :, at])
            out[b, q, :, cols(r, o)] = down(value)

    def send_wide(b):
        for d in range(1, pod_count):
            at = out.at[b, q, :, cols(2, o)]
            send(("wide", b), at, at, outer=pod(d))

    def pass_line(role, group, b, k, **to):
        for r in range(2):
            at = out.at[b, place(k), :, cols(r, o)]
            send_if(role, group, at, at, **to)

    def line_rows(b, count):
        return out.at[b, pl.ds(0, count), :, pl.ds(0, wa + wb)]

    def send_up(b):
        pass_line(is_tip, ("up", b), b, 0, rep=place(1))

    def send_mid(b):
        pass_line(middle, ("down", b), b, 1, rep=place(0))
        pass_line(middle, ("over", b, 1), b, 1, rep=place(2))

    def line_near(b):
        pl.when(middle)(lambda: arrive(("over", b, 1), line_rows(b, 1)))
        pass_line(middle, ("down", b), b, 2, rep=place(0))
        pl.when(middle)(lambda: arrive(("up", b), line_rows(b, 1)))
        pass_line(middle, ("over", b, 0), b, 0, rep=place(2))

    def line_far(b):
        pl.when(middle)(lambda: arrive(("over", b, 0), line_rows(b, 1)))
        pass_line(middle, ("down", b), b, 3, rep=place(0))

    def wide_done(b):
        arrive(("wide", b), out.at[b, q, :, pl.ds(0, (pod_count - 1) * wc)])

    def line_tip(b):
        mine = out.at[b, q, :, whole]
        pl.when(is_tip)(lambda: wide_done(b))
        send_if(is_tip, ("outward", b, 0), mine, mine, rep=place(1))

    def line_mid(b):
        mine = out.at[b, q, :, whole]
        pl.when(middle)(lambda: wide_done(b))
        send_if(middle, ("across", b, 1), mine, mine, rep=place(2))

    def line_across(b):
        at = out.at[b, place(0), :, whole]
        pl.when(middle)(lambda: arrive(("outward", b, 0), at))
        send_if(middle, ("across", b, 0), at, at, rep=place(2))

    def line_inward(b, k):
        at = out.at[b, place(k), :, whole]
        if k > 1:
            pl.when(middle)(lambda: arrive(("across", b, 3 - k), at))
        send_if(middle, ("inward",), at, at, rep=place(0))

    def line_end():
        pl.when(is_tip)(lambda: arrive(("inward",), out.at[:, pl.ds(0, 3), :, whole]))

    def send_block(b, d):
        i = (q + rep_count - d) % rep_count
        for r in range(2):
            at = out.at[b, i, :, cols(r, o)]
            send(("block", b, d), at, at, outer=neighbour[order(r, b)[1]])

    def send_blocks(b, d):
        i = (q + rep_count - d) % rep_count
        arrive(("block", b, d), out.at[b, i, :, pl.ds(0, wa + wb)])
        for r in range(2):
            axis = order(r, b)[0]
            for j in range(SIDE):
                at = out.at[b, i, :, cols(r, quarter(axis, j, False))]
                send(("blocks",), at, at, outer=neighbour[axis])

    def update(factor):
        for part, width in enumerate((wc, wa + wb)):
            arrive(("slot", part), slotted.at[pl.ds(1, pod_count - 1), :, :, pl.ds(0, width)])
        for j in range(slots):
            found = block_of(o, j)[1].astype(jnp.float32)
            for k in range(pod_count):
                for r in range(3):
                    at = pl.ds(base[r] + k * widths[r], widths[r])
                    step = (factor * found) * up(slotted[k, j, :, local_cols(r)])
                    moved = 0.9 * momentum[j, :, at] + step
                    new_momentum[j, :, at] = moved
                    new_master[j, :, at] = master[j, :, at] - 0.7 * (step + 0.9 * moved)

    def finish():
        arrive(("blocks",), out.at[:, :, :, pl.ds(0, SIDE * (wa + wb))])

    def drain():
        pairs = sum(pair_width(b) for b in range(blocks))
        deeps = sum(deep_width(b) for b in range(blocks))
        some = blocks // 2

        def rows(count, width):
            return deltas.at[0, pl.ds(0, count), :, pl.ds(0, width)]

        def deep_rows(count):
            return deltas.at[pl.ds(0, some), pl.ds(0, count), :, pl.ds(0, pod_count * deeps // some)]

        leave("first", deltas.at[pl.ds(0, SIDE), :, :, pl.ds(0, pairs)])
        leave("second", rows(rep_count, pairs))
        leave("third", rows(rep_count - 1, pairs))
        leave("near", deep_rows(3))
        leave("far", deep_rows(2))
        leave("last", deep_rows(1))
        leave("cross", rows(pod_count - 1, deeps))
        leave("early", arecv.at[pl.ds(1, pod_count - 1)])
        leave("norm", others.at[pl.ds(1, group - 1)])
        leave("slot", slotted.at[pl.ds(1, pod_count - 1)])
        leave("shard", others.at[pl.ds(group + 1, shard_count - 1)])
        leave("wide", out.at[:, 0, :, pl.ds(0, (pod_count - 1) * wc)])
        leave("up", out.at[:, 0, :, pl.ds(0, wa + wb)])
        leave("over", out.at[:, pl.ds(0, 2), :, pl.ds(0, wa + wb)])
        leave("down", out.at[:, pl.ds(0, 3), :, pl.ds(0, wa + wb)])
        leave("outward", out.at[:, 0, :, whole])
        leave("across", out.at[:, pl.ds(0, 2), :, whole])
        leave("inward", out.at[:, pl.ds(0, 3), :, whole])
        leave("block", out.at[:, :, :, pl.ds(0, wa + wb)])
        leave("blocks", out.at[:, :, :, pl.ds(0, SIDE * (wa + wb))])

    def rests(b):
        pl.when(is_tip)(lambda: arrive(("down", b), line_rows(b, 3)))
        for d in others_of:
            send_block(b, d)

    def rests_on(b):
        for d in others_of:
            send_blocks(b, d)

    squares[0] = jnp.zeros(squares.shape[1:], jnp.float32)
    def firsts(b):
        for g in others_of if late(b) else tail:
            send_first(b, g)

    def seconds(b):
        for g in others_of if late(b) else tail:
            send_second(b, g)

    for b in range(blocks):
        load_rows(b)
        if b < 2:
            firsts(b)
        if b > 0:
            start_tips(b - 1)
    start_tips(blocks - 1)
    pack_early()
    read_owners()
    for t in range(blocks + 2):
        if t < blocks:
            relay_near(t)
            if t == 0:
                pass_ready()
            seconds(t)
            if t == 0:
                all_ready()
        if t + 2 < blocks:
            firsts(t + 2)
            if t + 3 == blocks:
                for b in range(blocks - LATE, blocks):
                    send_first(b, 0)
        if 0 <= t - 1 < blocks:
            if t == blocks:
                send_early()
                for b in range(blocks - LATE, blocks):
                    send_second(b, 0)
                send_third(t - 1)
                relay_far(t - 1)
            else:
                relay_far(t - 1)
                send_third(t - 1)
        if 0 <= t - 2 < blocks:
            send_cross(t - 2)
    for b in range(blocks):
        if b < 2:
            finish_pair(b)
        finish_cross(b)
    mean_send(0)
    for b in range(2, blocks):
        finish_pair(b)
    norm_send()
    mean_send(1)
    norm_wait()
    factor = norm_shard()
    for b in range(blocks):
        spread(b, factor)
        send_wide(b)
        send_up(b)
        if b < 2:
            send_mid(b)
        send_block(b, 0)
    line_near(0)
    send_blocks(0, 0)
    line_tip(0)
    line_near(1)
    send_blocks(1, 0)
    line_tip(1)
    send_mid(2)
    line_far(0)
    send_blocks(2, 0)
    send_blocks(3, 0)
    line_tip(2)
    line_tip(3)
    rests(0)
    line_near(2)
    line_far(1)
    send_mid(3)
    line_near(3)
    rests(1)
    line_mid(0)
    line_mid(1)
    line_far(2)
    line_mid(2)
    line_mid(3)
    rests_on(0)
    line_across(0)
    rests(2)
    line_far(3)
    line_across(1)
    rests_on(1)
    rests(3)
    line_across(2)
    line_across(3)
    for b in range(blocks):
        line_inward(b, 1)
        line_inward(b, 2)
    rests_on(2)
    update(factor)
    line_inward(0, 3)
    line_inward(1, 3)
    rests_on(3)
    line_inward(2, 3)
    line_inward(3, 3)
    line_end()
    finish()
    drain()
    assert len(spans) + max(len(p) for p in phases) == recv_sem.shape[0]
    assert len(sent) == send_sem.shape[0]


def store(*refs):
    sem = refs[-1]
    copies = []
    for i in range(3):
        for k in range(refs[i].shape[0]):
            copies.append(pltpu.make_async_copy(refs[i].at[k], refs[i + 3].at[k], sem.at[len(copies)]))
    for copy in copies:
        copy.start()
    for copy in copies:
        copy.wait()


def regions(width, pod_count):
    tiles = width // (128 * pod_count)
    wc = max(1, round(tiles * DEEP))
    wb = (tiles - wc) // 2
    return tuple(128 * n for n in (tiles - wc - wb, wb, wc, EXTRA))


def fused(deltas, owners, master, momentum):
    blocks = owners.shape[1]
    slots, sub_rows, width = master.shape[2:]
    pod_count, rep_count = lax.axis_size("outer"), lax.axis_size("rep")
    shard_count = lax.axis_size("shard")
    entries = shard_count * blocks * rep_count * sub_rows * width
    clip_limit = 0.5 * math.sqrt(entries)
    widths = regions(width, pod_count)
    wa, wb, wc, extra = widths
    part, deep_width = width // pod_count, extra + wc
    deep = pod_count * deep_width
    group = pod_count * rep_count
    reduce_waits = 2 * (blocks + (rep_count - 1) * LATE) + 8 * blocks
    waits = 5 + max(reduce_waits, blocks * (rep_count + 8) + 2)
    vmem, hbm = pl.BlockSpec(memory_space=pltpu.VMEM), pl.BlockSpec(memory_space=pltpu.HBM)
    bf16, f32 = jnp.bfloat16, jnp.float32
    V = pltpu.VMEM
    out, new_momentum, new_master = pl.pallas_call(
        functools.partial(kernel, widths, (pod_count, rep_count, shard_count), clip_limit),
        out_shape=(
            V((blocks, rep_count, sub_rows, width), bf16),
            V(master.shape[2:], f32),
            V(master.shape[2:], f32),
        ),
        in_specs=[hbm] * 4,
        out_specs=(vmem, vmem, vmem),
        scratch_shapes=[
            pltpu.SMEM((blocks,), jnp.int32),
            V((blocks, rep_count, sub_rows, width), bf16),
            V(master.shape[2:], f32),
            V(master.shape[2:], f32),
            pltpu.SemaphoreType.DMA((blocks + 3,)),
            [V((SIDE, blocks, rep_count, sub_rows, w), bf16) for w in (wa, wb)],
            [V((blocks, rep_count, sub_rows, w), bf16) for w in (wa, wb)],
            [V((blocks, rep_count, sub_rows, w), bf16) for w in (wa, wb)],
            V((blocks, rep_count - 1, sub_rows, wa + wb), bf16),
            V((rep_count - 1, blocks, sub_rows, wa + wb), bf16),
            V((3, blocks, sub_rows, deep), bf16),
            V((3, blocks, sub_rows, deep), bf16),
            V((2, blocks, sub_rows, deep), bf16),
            V((blocks, sub_rows, deep), bf16),
            V((3, blocks, sub_rows, deep), bf16),
            V((blocks, sub_rows, deep), bf16),
            V((pod_count - 1, blocks, sub_rows, deep_width), bf16),
            V((pod_count, slots, sub_rows, part), bf16),
            V((pod_count, slots, sub_rows, part), bf16),
            V((blocks, sub_rows, part), bf16),
            V((pod_count, slots, sub_rows, part), bf16),
            V((pod_count, slots, sub_rows, part), bf16),
            V((1, 8, 128), f32),
            V((group + shard_count, 1, 128), f32),
            pltpu.SemaphoreType.DMA((KINDS,)),
            pltpu.SemaphoreType.DMA((waits,)),
            pltpu.SemaphoreType.REGULAR,
        ],
        compiler_params=pltpu.CompilerParams(
            collective_id=0, has_side_effects=True, vmem_limit_bytes=48 * 1024 * 1024
        ),
    )(
        owners[0, :, 0],
        deltas.reshape(blocks, rep_count, sub_rows, width),
        master.reshape(master.shape[2:]),
        momentum.reshape(momentum.shape[2:]),
    )
    arrays = (out, new_momentum, new_master)
    out, new_momentum, new_master = pl.pallas_call(
        store,
        out_shape=tuple(jax.ShapeDtypeStruct(a.shape, a.dtype) for a in arrays),
        in_specs=[pl.BlockSpec(memory_space=pl.ANY)] * 3,
        out_specs=(hbm,) * 3,
        scratch_shapes=[pltpu.SemaphoreType.DMA((blocks + 2 * slots,))],
        compiler_params=pltpu.CompilerParams(vmem_limit_bytes=4 * 1024 * 1024),
    )(*(pltpu.with_memory_space_constraint(a, pltpu.VMEM) for a in arrays))
    return (
        out.reshape(blocks * rep_count * sub_rows, width),
        new_momentum.reshape(momentum.shape),
        new_master.reshape(master.shape),
    )


def local(deltas, owners, master, momentum):
    blocks_here = owners.shape[1]
    slot_count = master.shape[2]
    sub_rows = master.shape[3]
    row_width = deltas.shape[3]
    block_rows = deltas.shape[2] // blocks_here
    pod_count = lax.axis_size("outer")
    rep_count = lax.axis_size("rep")
    owned_blocks = owners[0, :, 0]
    pod_ids = jnp.arange(pod_count, dtype=jnp.int32)
    onehot = (owned_blocks[:, None] == pod_ids[None, :]).astype(jnp.int32)
    rank_all = jnp.cumsum(onehot, axis=0) - onehot
    rank_own = jnp.sum(rank_all * onehot, axis=1)
    slot_ids = jnp.arange(slot_count, dtype=jnp.int32)
    selector = (
        (owned_blocks[None, None, :] == pod_ids[:, None, None])
        & (rank_own[None, None, :] == slot_ids[None, :, None])
    ).astype(jnp.bfloat16)
    local_rows = deltas[0, 0].reshape(blocks_here, block_rows, row_width)
    block_sums = lax.psum_scatter(
        local_rows.astype(jnp.float32).astype(jnp.bfloat16), "rep", scatter_dimension=1, tiled=True
    ).astype(jnp.float32)
    block_sums = block_sums.astype(jnp.bfloat16)
    pod_part = jnp.einsum(
        "ojb,brw->ojrw", selector, block_sums, preferred_element_type=jnp.float32
    ).astype(jnp.bfloat16)
    arrived = lax.all_to_all(pod_part, "outer", split_axis=0, concat_axis=0, tiled=True)
    mean_share = jnp.sum(arrived.astype(jnp.float32), axis=0) / (pod_count * rep_count)
    local_sq = jnp.sum(mean_share * mean_share)
    total_sq = lax.psum(local_sq, ("outer", "rep", "shard"))
    total_entries = lax.axis_size("shard") * blocks_here * block_rows * row_width
    clip_limit = 0.5 * math.sqrt(total_entries)
    factor = jnp.minimum(1.0, clip_limit / jnp.sqrt(total_sq + 1e-06))
    step_part = factor * mean_share[None, None]
    new_momentum = 0.9 * momentum + step_part
    new_master = master - 0.7 * (step_part + 0.9 * new_momentum)
    params_here = new_master.astype(jnp.bfloat16)
    gathered = lax.all_gather(params_here, ("outer", "rep"), axis=0, tiled=True).reshape(
        pod_count, rep_count, slot_count, sub_rows, row_width
    )
    unpacked = jnp.einsum("ojb,oqjrw->bqrw", selector, gathered, preferred_element_type=jnp.float32)
    new_params = unpacked.astype(jnp.bfloat16).reshape(blocks_here * block_rows, row_width)
    return (new_params, new_momentum, new_master)


def solution(mesh):
    fits = mesh.shape["outer"] == SIDE * SIDE and mesh.shape["rep"] == LINE

    def body(deltas, owners, master, momentum):
        blocks = owners.shape[1]
        width, sub_rows = master.shape[4], master.shape[3]
        tiled = width % (SIDE * SIDE * 128) == 0 and width >= 3 * SIDE * SIDE * 128
        tiled = tiled and sub_rows % TILE == 0 and blocks == SIDE * SIDE
        tiled = tiled and deltas.shape[2] == blocks * LINE * sub_rows
        if tiled:
            wa, wb, wc, extra = regions(width, SIDE * SIDE)
            tiled = wb > extra and SIDE * blocks * (wc + extra) <= width
        return (fused if fits and tiled else local)(deltas, owners, master, momentum)

    return jax.shard_map(
        body,
        mesh=mesh,
        in_specs=(
            P("outer", "rep", "shard", None),
            P("shard", None, None),
            P("outer", "shard", None, "rep", None),
            P("outer", "shard", None, "rep", None),
        ),
        out_specs=(
            P("shard", None),
            P("outer", "shard", None, "rep", None),
            P("outer", "shard", None, "rep", None),
        ),
        check_vma=False,
    )
```

```python
import functools
import math

import jax
import jax.numpy as jnp
from jax import lax
from jax.experimental import pallas as pl
from jax.experimental.pallas import tpu as pltpu
from jax.sharding import PartitionSpec as P

DEEP = 0.2
EXTRA = 1
THICK = 2
TILE = 16
SIDE = 2
LATE = 2
KINDS = 21
LINE = 4


def kernel(
    plan, axis_sizes, clip_limit,
    owners_far, deltas_far, master_far, momentum_far,
    out, new_momentum, new_master,
    owners, deltas, master, momentum, load_sem, first, passed, second, zin, zrecv,
    staged, near, far, last, onward, ztotal, cross,
    apack, arecv, mean, packed, slotted, squares, others,
    send_sem, recv_sem, ready,
):
    wa, wb, wc, extra = plan
    pod_count, rep_count, shard_count = axis_sizes
    blocks, sub_rows, slots = deltas.shape[0], master.shape[1], master.shape[0]
    widths = (wa, wb, wc)
    base = (0, pod_count * wa, pod_count * (wa + wb))
    offset = (0, wa, wa + wb)

    def pair(b):
        return (wa, wb - extra if b < THICK else wb)

    def pair_width(b):
        return sum(pair(b))

    def deep_width(b):
        return wa + wb + wc - pair_width(b)

    def part(r, b):
        return pl.ds(0, pair(b)[r])

    def deep(b):
        return pl.ds(0, pod_count * deep_width(b))

    o, q, s = lax.axis_index("outer"), lax.axis_index("rep"), lax.axis_index("shard")
    y, x = o // SIDE, o % SIDE
    neighbour = {"x": y * SIDE + 1 - x, "y": (1 - y) * SIDE + x}
    is_low = q < rep_count // 2
    tip = jnp.where(is_low, 0, rep_count - 1)
    is_tip = q == tip

    def place(k):
        return jnp.where(is_low, k, rep_count - 1 - k)

    def pod(d):
        return ((y + d // SIDE) % SIDE) * SIDE + (x + d % SIDE) % SIDE

    barrier = pltpu.get_barrier_semaphore()

    def greet(sem, **to):
        pl.semaphore_signal(sem, inc=1, device_id=to, device_id_type=pl.DeviceIdType.MESH)

    middle = jnp.logical_not(is_tip)
    greet(barrier, outer=neighbour["x"])
    greet(barrier, outer=neighbour["y"])
    greet(barrier, rep=jnp.where(is_tip, place(1), place(0)))
    pl.when(middle)(lambda: greet(barrier, rep=place(2)))
    for d in range(1, shard_count):
        greet(barrier, shard=(s + d) % shard_count)
    loads = [
        pltpu.make_async_copy(deltas_far.at[b], deltas.at[b], load_sem.at[b]) for b in range(blocks)
    ]
    loads.append(pltpu.make_async_copy(master_far, master, load_sem.at[blocks]))
    loads.append(pltpu.make_async_copy(momentum_far, momentum, load_sem.at[blocks + 1]))
    loads.append(pltpu.make_async_copy(owners_far, owners, load_sem.at[blocks + 2]))
    for load in loads:
        load.start()
    pl.semaphore_wait(barrier, jnp.where(is_tip, 3, 4) + shard_count - 1)
    pl.when(middle)(lambda: greet(ready, rep=place(2)))

    def pass_ready():
        @pl.when(middle)
        def _():
            pl.semaphore_wait(ready, 1)
            greet(ready, rep=place(0))

    def all_ready():
        pl.when(is_tip)(lambda: pl.semaphore_wait(ready, 1))


    sent, roles = {}, {}
    spans, phases = (("slot", 0), ("slot", 1), ("early",), ("norm",), ("shard",)), ({}, {})
    gathers = ("wide", "wider", "up", "over", "down", "outward", "across", "inward", "block", "blocks")

    def copy(group, src, dst, **to):
        kind = group[0]
        if group in spans:
            number = spans.index(group)
        else:
            numbers = phases[kind in gathers]
            number = len(spans) + numbers.setdefault(group, len(numbers))
        sent.setdefault(kind, len(sent))
        return pltpu.make_async_remote_copy(
            src_ref=src, dst_ref=dst, send_sem=send_sem.at[sent[kind]], recv_sem=recv_sem.at[number],
            device_id=to, device_id_type=pl.DeviceIdType.MESH,
        )

    def send(group, src, dst, **to):
        roles[group[0]] = None
        copy(group, src, dst, **to).start()

    def send_if(role, group, src, dst, **to):
        roles[group[0]] = role
        pl.when(role)(copy(group, src, dst, **to).start)

    def arrive(group, like):
        copy(group, like, like, rep=q).wait_recv()

    def leave(kind, like):
        made = pltpu.make_async_remote_copy(
            src_ref=like, dst_ref=like, send_sem=send_sem.at[sent[kind]], recv_sem=recv_sem.at[0],
            device_id={"rep": q}, device_id_type=pl.DeviceIdType.MESH,
        )
        if roles[kind] is None:
            made.wait_send()
        else:
            pl.when(roles[kind])(made.wait_send)

    def loop(count, body):
        def step(i, carry):
            body(i)
            return carry

        lax.fori_loop(0, count, step, 0)

    def up(value):
        return value.astype(jnp.float32)

    def down(value):
        return value.astype(jnp.bfloat16)

    def cols(region, k):
        width = widths[region]
        return pl.ds(pl.multiple_of(base[region] + k * width, 128), width)

    def pair_cols(r, b, k):
        return pl.ds(pl.multiple_of(base[r] + k * widths[r], 128), pair(b)[r])

    def local_cols(region):
        return pl.ds(offset[region], widths[region])

    def pair_local(r, b):
        return pl.ds(offset[r], pair(b)[r])

    def deep_cols(b, k):
        return pl.ds(pl.multiple_of(k * deep_width(b), 128), deep_width(b))

    def order(region, b):
        return ("x", "y") if (region + b) % 2 == 0 else ("y", "x")

    def at_rows(g):
        return slice(None) if g is None else (q + g) % rep_count

    def each(g, body):
        if g is None:
            loop(rep_count, body)
        else:
            body((q + g) % rep_count)

    tail = (None,)
    others_of = tuple(range(1, rep_count))

    def late(b):
        return b >= blocks - LATE

    whole = pl.ds(base[2], pod_count * wc)

    def quarter(axis, j, away):
        if axis == "x":
            return j * SIDE + (1 - x if away else x)
        return (1 - y if away else y) * SIDE + j

    def stay(axis):
        return y if axis == "x" else x

    def send_first(b, g):
        i = at_rows(g)
        for r in range(2):
            axis = order(r, b)[0]
            for j in range(SIDE):
                send(
                    ("first", b, g), deltas.at[b, i, :, pair_cols(r, b, quarter(axis, j, True))],
                    first[r].at[j, b, i, :, part(r, b)], outer=neighbour[axis],
                )

    def send_second(b, g):
        arrive(("first", b, g), deltas.at[b, at_rows(g), :, pl.ds(0, SIDE * pair_width(b))])
        for r in range(2):
            axis, other = order(r, b)
            go = 1 - stay(axis)
            at = pair_cols(r, b, quarter(axis, go, False))

            def body(i):
                came = first[r][go, b, i, :, part(r, b)]
                passed[r][b, i, :, part(r, b)] = down(up(deltas[b, i, :, at]) + up(came))

            each(g, body)
            i = at_rows(g)
            send(
                ("second", b, g), passed[r].at[b, i, :, part(r, b)],
                second[r].at[b, i, :, part(r, b)], outer=neighbour[other],
            )

    def pair_total(r, b, i):
        at = part(r, b)
        total = up(deltas[b, i, :, pair_cols(r, b, o)]) + up(first[r][stay(order(r, b)[0]), b, i, :, at])
        return total + up(second[r][b, i, :, at])

    def send_third(b):
        groups = others_of if late(b) else tail
        for g in groups:
            arrive(("second", b, g), deltas.at[b, at_rows(g), :, pl.ds(0, pair_width(b))])
        for d in others_of:
            there = (q + d) % rep_count
            for r in range(2):
                zin[b, d - 1, :, pair_local(r, b)] = down(pair_total(r, b, there))
            at = pl.ds(0, pair_width(b))
            send(("third", b), zin.at[b, d - 1, :, at], zrecv.at[d - 1, b, :, at], rep=there)

    def deep_of(b, i):
        keep = pair(b)[1]
        if keep == wb:
            return deltas[b, i, :, whole]
        parts = []
        for k in range(pod_count):
            parts.append(deltas[b, i, :, pl.ds(base[1] + k * wb + keep, wb - keep)])
            parts.append(deltas[b, i, :, pl.ds(base[2] + k * wc, wc)])
        return jnp.concatenate(parts, axis=-1)

    def start_tips(b):
        @pl.when(is_tip)
        def _():
            for k in (3, 2, 1):
                staged[k - 1, b, :, deep(b)] = deep_of(b, place(k))
                copy(("near", b, k), staged.at[k - 1, b, :, deep(b)], near.at[k - 1, b, :, deep(b)], rep=place(1)).start()

        roles["near"] = is_tip

    def relay_near(b):
        @pl.when(middle)
        def _():
            for k in (3, 2):
                arrive(("near", b, k), near.at[k - 1, b, :, deep(b)])
                onward[k - 1, b, :, deep(b)] = down(up(deep_of(b, place(k))) + up(near[k - 1, b, :, deep(b)]))
                copy(("far", b, 3 - k), onward.at[k - 1, b, :, deep(b)], far.at[3 - k, b, :, deep(b)], rep=place(2)).start()

        roles["far"] = middle

    def relay_far(b):
        @pl.when(middle)
        def _():
            arrive(("far", b, 0), far.at[0, b, :, deep(b)])
            onward[0, b, :, deep(b)] = down(up(deep_of(b, place(0))) + up(far[0, b, :, deep(b)]))
            copy(("last", b), onward.at[0, b, :, deep(b)], last.at[b, :, deep(b)], rep=place(0)).start()

        roles["last"] = middle

    def send_cross(b):
        at = deep(b)

        @pl.when(is_tip)
        def _():
            arrive(("last", b), last.at[b, :, at])
            ztotal[b, :, at] = down(up(deep_of(b, q)) + up(last[b, :, at]))

        @pl.when(middle)
        def _():
            arrive(("near", b, 1), near.at[0, b, :, at])
            arrive(("far", b, 1), far.at[1, b, :, at])
            total = up(deep_of(b, q)) + up(near[0, b, :, at])
            ztotal[b, :, at] = down(total + up(far[1, b, :, at]))

        for d in range(1, pod_count):
            send(
                ("cross", b), ztotal.at[b, :, deep_cols(b, pod(d))],
                cross.at[d - 1, b, :, pl.ds(0, deep_width(b))], outer=pod(d),
            )

    scale = 1.0 / (pod_count * rep_count)

    def put_mean(b, at, total):
        value = total * scale
        mean[b, :, at] = down(value)
        square = value * value
        part = squares[0]
        height, width = square.shape
        for k in range(height // 8):
            for i in range(width // 128):
                part = part + square[k * 8:(k + 1) * 8, i * 128:(i + 1) * 128]
        squares[0] = part

    def finish_pair(b):
        if late(b):
            arrive(("second", b, 0), deltas.at[b, q, :, pl.ds(0, pair_width(b))])
        arrive(("third", b), zrecv.at[:, b, :, pl.ds(0, pair_width(b))])
        for r in range(2):
            total = pair_total(r, b, q)
            for d in range(rep_count - 1):
                total = total + up(zrecv[d, b, :, pair_local(r, b)])
            put_mean(b, pair_local(r, b), total)

    def finish_cross(b):
        at = pl.ds(0, deep_width(b))
        arrive(("cross", b), cross.at[:, b, :, at])
        total = up(ztotal[b, :, deep_cols(b, o)])
        for d in range(pod_count - 1):
            total = total + up(cross[d, b, :, at])
        put_mean(b, pl.ds(pair_width(b), deep_width(b)), total)

    owner, rank = [], []

    def read_owners():
        loads[blocks + 2].wait()
        owner.extend(owners[b] for b in range(blocks))
        for b in range(blocks):
            count = jnp.int32(0)
            for before in range(b):
                count = count + (owner[before] == owner[b]).astype(jnp.int32)
            rank.append(count)

    def block_of(k, j):
        index, found = jnp.int32(0), jnp.int32(0)
        for b in range(blocks):
            match = ((owner[b] == k) & (rank[b] == j)).astype(jnp.int32)
            index, found = index + b * match, found + match
        return index, found

    def load_rows(b):
        loads[b].wait()

    def pack_early():
        loads[blocks].wait()
        loads[blocks + 1].wait()
        for k in range(pod_count):
            for r in range(3):
                at = pl.ds(base[r] + k * widths[r], widths[r])

                def body(i):
                    value = master[i, :, at] - 0.567 * momentum[i, :, at]
                    apack[k, i, :, local_cols(r)] = down(value)

                loop(slots, body)
        arecv[o] = apack[o]

    def send_early(*steps):
        for d in steps:
            send(("early",), apack.at[pod(d)], arecv.at[o], outer=pod(d))

    group = pod_count * rep_count

    lead = s == 0
    follow = jnp.logical_not(lead)
    partial = group + shard_count

    def norm_send():
        others[partial] = jnp.sum(squares[0], axis=0, keepdims=True)
        send_if(follow, ("shard",), others.at[partial], others.at[group + s], shard=0)

    def norm_lead():
        roles["norm"] = lead

        @pl.when(lead)
        def _():
            arrive(("shard",), others.at[pl.ds(group + 1, shard_count - 1)])
            total = others[partial]
            for d in range(1, shard_count):
                total = total + others[group + d]
            others[group] = total
            others[0] = total
            for e in range(rep_count):
                for d in range(pod_count):
                    for t in range(shard_count):
                        if d or e or t:
                            copy(
                                ("norm",), others.at[group], others.at[d * rep_count + e],
                                outer=pod(d), rep=(q + e) % rep_count, shard=t,
                            ).start()

    def mean_send(part):
        at = pl.ds(wa + wb, wc) if part == 0 else pl.ds(0, wa + wb)
        for d in range(pod_count):
            for j in range(slots):
                packed[d, j, :, at] = mean[block_of(pod(d), j)[0], :, at]
            if d == 0:
                slotted[o, :, :, at] = packed[0, :, :, at]
            else:
                send(("slot", part), packed.at[d, :, :, at], slotted.at[o, :, :, at], outer=pod(d))

    def norm_wait():
        pl.when(lead)(lambda: arrive(("norm",), others.at[pl.ds(1, group - 1)]))
        pl.when(follow)(lambda: arrive(("norm",), others.at[pl.ds(0, group)]))
        arrive(("early",), arecv.at[pl.ds(1, pod_count - 1)])
        total = others[0]
        for d in range(1, group):
            total = total + others[d]
        total = jnp.sum(total, keepdims=True)
        return jnp.minimum(1.0, clip_limit / jnp.sqrt(total + 1e-06))

    def spread(b, factor):
        for r in range(3):
            at = local_cols(r)
            early = up(arecv[owner[b], jnp.minimum(rank[b], slots - 1), :, at])
            value = early - (1.33 * factor) * up(mean[b, :, at])
            out[b, q, :, cols(r, o)] = down(value)

    def send_wide(b):
        at = out.at[b, q, :, cols(2, o)]
        send(("wide", b), at, at, outer=neighbour[order(0, b)[0]])

    def send_wider(b):
        arrive(("wide", b), out.at[b, q, :, pl.ds(0, wc)])
        axis, other = order(0, b)
        for k in (o, neighbour[axis]):
            at = out.at[b, q, :, cols(2, k)]
            send(("wider", b), at, at, outer=neighbour[other])

    def pass_line(role, group, b, k, **to):
        for r in range(2):
            at = out.at[b, place(k), :, cols(r, o)]
            send_if(role, group, at, at, **to)

    def line_rows(b, count):
        return out.at[b, pl.ds(0, count), :, pl.ds(0, wa + wb)]

    def send_up(b):
        pass_line(is_tip, ("up", b), b, 0, rep=place(1))

    def send_mid(b):
        pass_line(middle, ("down", b), b, 1, rep=place(0))
        pass_line(middle, ("over", b, 1), b, 1, rep=place(2))

    def line_near(b):
        pl.when(middle)(lambda: arrive(("over", b, 1), line_rows(b, 1)))
        pass_line(middle, ("down", b), b, 2, rep=place(0))
        pl.when(middle)(lambda: arrive(("up", b), line_rows(b, 1)))
        pass_line(middle, ("over", b, 0), b, 0, rep=place(2))

    def line_far(b):
        pl.when(middle)(lambda: arrive(("over", b, 0), line_rows(b, 1)))
        pass_line(middle, ("down", b), b, 3, rep=place(0))

    def wide_done(b):
        arrive(("wider", b), out.at[b, q, :, pl.ds(0, SIDE * wc)])

    def line_tip(b):
        mine = out.at[b, q, :, whole]
        pl.when(is_tip)(lambda: wide_done(b))
        send_if(is_tip, ("outward", b, 0), mine, mine, rep=place(1))

    def line_mid(b):
        mine = out.at[b, q, :, whole]
        pl.when(middle)(lambda: wide_done(b))
        send_if(middle, ("across", b, 1), mine, mine, rep=place(2))

    def line_across(b):
        at = out.at[b, place(0), :, whole]
        pl.when(middle)(lambda: arrive(("outward", b, 0), at))
        send_if(middle, ("across", b, 0), at, at, rep=place(2))

    def line_inward(b, k):
        at = out.at[b, place(k), :, whole]
        if k > 1:
            pl.when(middle)(lambda: arrive(("across", b, 3 - k), at))
        send_if(middle, ("inward",), at, at, rep=place(0))

    def line_end():
        pl.when(is_tip)(lambda: arrive(("inward",), out.at[:, pl.ds(0, 3), :, whole]))

    def send_block(b, d):
        i = (q + rep_count - d) % rep_count
        for r in range(2):
            at = out.at[b, i, :, cols(r, o)]
            send(("block", b, d), at, at, outer=neighbour[order(r, b)[1]])

    def send_blocks(b, d):
        i = (q + rep_count - d) % rep_count
        arrive(("block", b, d), out.at[b, i, :, pl.ds(0, wa + wb)])
        for r in range(2):
            axis = order(r, b)[0]
            for j in range(SIDE):
                at = out.at[b, i, :, cols(r, quarter(axis, j, False))]
                send(("blocks",), at, at, outer=neighbour[axis])

    def update(factor):
        for part, width in enumerate((wc, wa + wb)):
            arrive(("slot", part), slotted.at[pl.ds(1, pod_count - 1), :, :, pl.ds(0, width)])
        for j in range(slots):
            found = block_of(o, j)[1].astype(jnp.float32)
            for k in range(pod_count):
                for r in range(3):
                    at = pl.ds(base[r] + k * widths[r], widths[r])
                    step = (factor * found) * up(slotted[k, j, :, local_cols(r)])
                    moved = 0.9 * momentum[j, :, at] + step
                    new_momentum[j, :, at] = moved
                    new_master[j, :, at] = master[j, :, at] - 0.7 * (step + 0.9 * moved)

    def finish():
        arrive(("blocks",), out.at[:, :, :, pl.ds(0, SIDE * (wa + wb))])

    def drain():
        pairs = sum(pair_width(b) for b in range(blocks))
        deeps = sum(deep_width(b) for b in range(blocks))
        some = blocks // 2

        def rows(count, width):
            return deltas.at[0, pl.ds(0, count), :, pl.ds(0, width)]

        def deep_rows(count):
            return deltas.at[pl.ds(0, some), pl.ds(0, count), :, pl.ds(0, pod_count * deeps // some)]

        leave("first", deltas.at[pl.ds(0, SIDE), :, :, pl.ds(0, pairs)])
        leave("second", rows(rep_count, pairs))
        leave("third", rows(rep_count - 1, pairs))
        leave("near", deep_rows(3))
        leave("far", deep_rows(2))
        leave("last", deep_rows(1))
        leave("cross", rows(pod_count - 1, deeps))
        leave("early", arecv.at[pl.ds(1, pod_count - 1)])
        leave("norm", others.at[pl.ds(0, group * shard_count - 1)])
        leave("slot", slotted.at[pl.ds(1, pod_count - 1)])
        leave("shard", others.at[pl.ds(0, 1)])
        leave("wide", out.at[:, 0, :, pl.ds(0, wc)])
        leave("wider", out.at[:, 0, :, pl.ds(0, SIDE * wc)])
        leave("up", out.at[:, 0, :, pl.ds(0, wa + wb)])
        leave("over", out.at[:, pl.ds(0, 2), :, pl.ds(0, wa + wb)])
        leave("down", out.at[:, pl.ds(0, 3), :, pl.ds(0, wa + wb)])
        leave("outward", out.at[:, 0, :, whole])
        leave("across", out.at[:, pl.ds(0, 2), :, whole])
        leave("inward", out.at[:, pl.ds(0, 3), :, whole])
        leave("block", out.at[:, :, :, pl.ds(0, wa + wb)])
        leave("blocks", out.at[:, :, :, pl.ds(0, SIDE * (wa + wb))])

    def rests(b):
        pl.when(is_tip)(lambda: arrive(("down", b), line_rows(b, 3)))
        for d in others_of:
            send_block(b, d)

    def rests_on(b):
        for d in others_of:
            send_blocks(b, d)

    squares[0] = jnp.zeros(squares.shape[1:], jnp.float32)
    def firsts(b):
        for g in others_of if late(b) else tail:
            send_first(b, g)

    def seconds(b):
        for g in others_of if late(b) else tail:
            send_second(b, g)

    for b in range(blocks):
        load_rows(b)
        if b < 2:
            firsts(b)
        if b > 0:
            start_tips(b - 1)
    start_tips(blocks - 1)
    pack_early()
    read_owners()
    for t in range(blocks + 2):
        if t < blocks:
            relay_near(t)
            if t == 0:
                pass_ready()
            seconds(t)
            if t == 0:
                all_ready()
        if t + 2 < blocks:
            firsts(t + 2)
            if t + 3 == blocks:
                for b in range(blocks - LATE, blocks):
                    send_first(b, 0)
        if 0 <= t - 1 < blocks:
            if t == blocks:
                send_early(1, 2)
                for b in range(blocks - LATE, blocks):
                    send_second(b, 0)
                send_third(t - 1)
                relay_far(t - 1)
            else:
                relay_far(t - 1)
                send_third(t - 1)
        if 0 <= t - 2 < blocks:
            send_cross(t - 2)
    send_early(3)
    for b in range(blocks):
        if b < 2:
            finish_pair(b)
        finish_cross(b)
    mean_send(0)
    for b in range(2, blocks):
        finish_pair(b)
    norm_send()
    norm_lead()
    mean_send(1)
    factor = norm_wait()
    for b in range(blocks):
        spread(b, factor)
        send_wide(b)
        send_up(b)
        if b < 2:
            send_mid(b)
        send_block(b, 0)
    line_near(0)
    send_wider(0)
    send_blocks(0, 0)
    line_near(1)
    send_wider(1)
    send_blocks(1, 0)
    send_mid(2)
    line_far(0)
    for b in range(2, blocks):
        send_wider(b)
        send_blocks(b, 0)
    for b in range(blocks):
        line_tip(b)
    rests(0)
    line_near(2)
    line_far(1)
    send_mid(3)
    line_near(3)
    rests(1)
    line_mid(0)
    line_mid(1)
    line_far(2)
    line_mid(2)
    line_mid(3)
    rests_on(0)
    line_across(0)
    rests(2)
    line_far(3)
    line_across(1)
    rests_on(1)
    rests(3)
    line_across(2)
    line_across(3)
    for b in range(blocks):
        line_inward(b, 1)
        line_inward(b, 2)
    rests_on(2)
    update(factor)
    line_inward(0, 3)
    line_inward(1, 3)
    rests_on(3)
    line_inward(2, 3)
    line_inward(3, 3)
    line_end()
    finish()
    drain()
    assert len(spans) + max(len(p) for p in phases) == recv_sem.shape[0]
    assert len(sent) == send_sem.shape[0]


def store(*refs):
    sem = refs[-1]
    copies = []
    for i in range(3):
        for k in range(refs[i].shape[0]):
            copies.append(pltpu.make_async_copy(refs[i].at[k], refs[i + 3].at[k], sem.at[len(copies)]))
    for copy in copies:
        copy.start()
    for copy in copies:
        copy.wait()


def regions(width, pod_count):
    tiles = width // (128 * pod_count)
    wc = max(1, round(tiles * DEEP))
    wb = (tiles - wc) // 2
    return tuple(128 * n for n in (tiles - wc - wb, wb, wc, EXTRA))


def fused(deltas, owners, master, momentum):
    blocks = owners.shape[1]
    slots, sub_rows, width = master.shape[2:]
    pod_count, rep_count = lax.axis_size("outer"), lax.axis_size("rep")
    shard_count = lax.axis_size("shard")
    entries = shard_count * blocks * rep_count * sub_rows * width
    clip_limit = 0.5 * math.sqrt(entries)
    widths = regions(width, pod_count)
    wa, wb, wc, extra = widths
    part, deep_width = width // pod_count, extra + wc
    deep = pod_count * deep_width
    group = pod_count * rep_count
    reduce_waits = 2 * (blocks + (rep_count - 1) * LATE) + 8 * blocks
    waits = 5 + max(reduce_waits, blocks * (rep_count + 9) + 2)
    vmem, hbm = pl.BlockSpec(memory_space=pltpu.VMEM), pl.BlockSpec(memory_space=pltpu.HBM)
    bf16, f32 = jnp.bfloat16, jnp.float32
    V = pltpu.VMEM
    out, new_momentum, new_master = pl.pallas_call(
        functools.partial(kernel, widths, (pod_count, rep_count, shard_count), clip_limit),
        out_shape=(
            V((blocks, rep_count, sub_rows, width), bf16),
            V(master.shape[2:], f32),
            V(master.shape[2:], f32),
        ),
        in_specs=[hbm] * 4,
        out_specs=(vmem, vmem, vmem),
        scratch_shapes=[
            pltpu.SMEM((blocks,), jnp.int32),
            V((blocks, rep_count, sub_rows, width), bf16),
            V(master.shape[2:], f32),
            V(master.shape[2:], f32),
            pltpu.SemaphoreType.DMA((blocks + 3,)),
            [V((SIDE, blocks, rep_count, sub_rows, w), bf16) for w in (wa, wb)],
            [V((blocks, rep_count, sub_rows, w), bf16) for w in (wa, wb)],
            [V((blocks, rep_count, sub_rows, w), bf16) for w in (wa, wb)],
            V((blocks, rep_count - 1, sub_rows, wa + wb), bf16),
            V((rep_count - 1, blocks, sub_rows, wa + wb), bf16),
            V((3, blocks, sub_rows, deep), bf16),
            V((3, blocks, sub_rows, deep), bf16),
            V((2, blocks, sub_rows, deep), bf16),
            V((blocks, sub_rows, deep), bf16),
            V((3, blocks, sub_rows, deep), bf16),
            V((blocks, sub_rows, deep), bf16),
            V((pod_count - 1, blocks, sub_rows, deep_width), bf16),
            V((pod_count, slots, sub_rows, part), bf16),
            V((pod_count, slots, sub_rows, part), bf16),
            V((blocks, sub_rows, part), bf16),
            V((pod_count, slots, sub_rows, part), bf16),
            V((pod_count, slots, sub_rows, part), bf16),
            V((1, 8, 128), f32),
            V((group * shard_count + shard_count, 1, 128), f32),
            pltpu.SemaphoreType.DMA((KINDS,)),
            pltpu.SemaphoreType.DMA((waits,)),
            pltpu.SemaphoreType.REGULAR,
        ],
        compiler_params=pltpu.CompilerParams(
            collective_id=0, has_side_effects=True, vmem_limit_bytes=48 * 1024 * 1024
        ),
    )(
        owners[0, :, 0],
        deltas.reshape(blocks, rep_count, sub_rows, width),
        master.reshape(master.shape[2:]),
        momentum.reshape(momentum.shape[2:]),
    )
    arrays = (out, new_momentum, new_master)
    out, new_momentum, new_master = pl.pallas_call(
        store,
        out_shape=tuple(jax.ShapeDtypeStruct(a.shape, a.dtype) for a in arrays),
        in_specs=[pl.BlockSpec(memory_space=pl.ANY)] * 3,
        out_specs=(hbm,) * 3,
        scratch_shapes=[pltpu.SemaphoreType.DMA((blocks + 2 * slots,))],
        compiler_params=pltpu.CompilerParams(vmem_limit_bytes=4 * 1024 * 1024),
    )(*(pltpu.with_memory_space_constraint(a, pltpu.VMEM) for a in arrays))
    return (
        out.reshape(blocks * rep_count * sub_rows, width),
        new_momentum.reshape(momentum.shape),
        new_master.reshape(master.shape),
    )


def local(deltas, owners, master, momentum):
    blocks_here = owners.shape[1]
    slot_count = master.shape[2]
    sub_rows = master.shape[3]
    row_width = deltas.shape[3]
    block_rows = deltas.shape[2] // blocks_here
    pod_count = lax.axis_size("outer")
    rep_count = lax.axis_size("rep")
    owned_blocks = owners[0, :, 0]
    pod_ids = jnp.arange(pod_count, dtype=jnp.int32)
    onehot = (owned_blocks[:, None] == pod_ids[None, :]).astype(jnp.int32)
    rank_all = jnp.cumsum(onehot, axis=0) - onehot
    rank_own = jnp.sum(rank_all * onehot, axis=1)
    slot_ids = jnp.arange(slot_count, dtype=jnp.int32)
    selector = (
        (owned_blocks[None, None, :] == pod_ids[:, None, None])
        & (rank_own[None, None, :] == slot_ids[None, :, None])
    ).astype(jnp.bfloat16)
    local_rows = deltas[0, 0].reshape(blocks_here, block_rows, row_width)
    block_sums = lax.psum_scatter(
        local_rows.astype(jnp.float32).astype(jnp.bfloat16), "rep", scatter_dimension=1, tiled=True
    ).astype(jnp.float32)
    block_sums = block_sums.astype(jnp.bfloat16)
    pod_part = jnp.einsum(
        "ojb,brw->ojrw", selector, block_sums, preferred_element_type=jnp.float32
    ).astype(jnp.bfloat16)
    arrived = lax.all_to_all(pod_part, "outer", split_axis=0, concat_axis=0, tiled=True)
    mean_share = jnp.sum(arrived.astype(jnp.float32), axis=0) / (pod_count * rep_count)
    local_sq = jnp.sum(mean_share * mean_share)
    total_sq = lax.psum(local_sq, ("outer", "rep", "shard"))
    total_entries = lax.axis_size("shard") * blocks_here * block_rows * row_width
    clip_limit = 0.5 * math.sqrt(total_entries)
    factor = jnp.minimum(1.0, clip_limit / jnp.sqrt(total_sq + 1e-06))
    step_part = factor * mean_share[None, None]
    new_momentum = 0.9 * momentum + step_part
    new_master = master - 0.7 * (step_part + 0.9 * new_momentum)
    params_here = new_master.astype(jnp.bfloat16)
    gathered = lax.all_gather(params_here, ("outer", "rep"), axis=0, tiled=True).reshape(
        pod_count, rep_count, slot_count, sub_rows, row_width
    )
    unpacked = jnp.einsum("ojb,oqjrw->bqrw", selector, gathered, preferred_element_type=jnp.float32)
    new_params = unpacked.astype(jnp.bfloat16).reshape(blocks_here * block_rows, row_width)
    return (new_params, new_momentum, new_master)


def solution(mesh):
    fits = mesh.shape["outer"] == SIDE * SIDE and mesh.shape["rep"] == LINE

    def body(deltas, owners, master, momentum):
        blocks = owners.shape[1]
        width, sub_rows = master.shape[4], master.shape[3]
        tiled = width % (SIDE * SIDE * 128) == 0 and width >= 3 * SIDE * SIDE * 128
        tiled = tiled and sub_rows % TILE == 0 and blocks == SIDE * SIDE
        tiled = tiled and deltas.shape[2] == blocks * LINE * sub_rows
        if tiled:
            wa, wb, wc, extra = regions(width, SIDE * SIDE)
            tiled = wb > extra and SIDE * blocks * (wc + extra) <= width
        return (fused if fits and tiled else local)(deltas, owners, master, momentum)

    return jax.shard_map(
        body,
        mesh=mesh,
        in_specs=(
            P("outer", "rep", "shard", None),
            P("shard", None, None),
            P("outer", "shard", None, "rep", None),
            P("outer", "shard", None, "rep", None),
        ),
        out_specs=(
            P("shard", None),
            P("outer", "shard", None, "rep", None),
            P("outer", "shard", None, "rep", None),
        ),
        check_vma=False,
    )
```

```python
import functools
import math

import jax
import jax.numpy as jnp
from jax import lax
from jax.experimental import pallas as pl
from jax.experimental.pallas import tpu as pltpu
from jax.sharding import PartitionSpec as P

DEEP = 0.2
EXTRA = 1
THICK = 2
TILE = 16
SIDE = 2
LATE = 4
KINDS = 21
LINE = 4


def kernel(
    plan, axis_sizes, clip_limit,
    owners_far, deltas_far, master_far, momentum_far,
    out, new_momentum, new_master,
    owners, deltas, master, momentum, load_sem, first, passed, second, zin, zrecv,
    staged, near, far, last, onward, ztotal, cross,
    apack, arecv, mean, packed, slotted, squares, others,
    send_sem, recv_sem, ready,
):
    wa, wb, wc, extra = plan
    pod_count, rep_count, shard_count = axis_sizes
    blocks, sub_rows, slots = deltas.shape[0], master.shape[1], master.shape[0]
    widths = (wa, wb, wc)
    base = (0, pod_count * wa, pod_count * (wa + wb))
    offset = (0, wa, wa + wb)

    def pair(b):
        return (wa, wb - extra if b < THICK else wb)

    def pair_width(b):
        return sum(pair(b))

    def deep_width(b):
        return wa + wb + wc - pair_width(b)

    def part(r, b):
        return pl.ds(0, pair(b)[r])

    def deep(b):
        return pl.ds(0, pod_count * deep_width(b))

    o, q, s = lax.axis_index("outer"), lax.axis_index("rep"), lax.axis_index("shard")
    y, x = o // SIDE, o % SIDE
    neighbour = {"x": y * SIDE + 1 - x, "y": (1 - y) * SIDE + x}
    is_low = q < rep_count // 2
    tip = jnp.where(is_low, 0, rep_count - 1)
    is_tip = q == tip

    def place(k):
        return jnp.where(is_low, k, rep_count - 1 - k)

    def pod(d):
        return ((y + d // SIDE) % SIDE) * SIDE + (x + d % SIDE) % SIDE

    barrier = pltpu.get_barrier_semaphore()

    def greet(sem, **to):
        pl.semaphore_signal(sem, inc=1, device_id=to, device_id_type=pl.DeviceIdType.MESH)

    middle = jnp.logical_not(is_tip)
    greet(barrier, outer=neighbour["x"])
    greet(barrier, outer=neighbour["y"])
    greet(barrier, rep=jnp.where(is_tip, place(1), place(0)))
    pl.when(middle)(lambda: greet(barrier, rep=place(2)))
    for d in range(1, shard_count):
        greet(barrier, shard=(s + d) % shard_count)
    loads = [
        pltpu.make_async_copy(deltas_far.at[b], deltas.at[b], load_sem.at[b]) for b in range(blocks)
    ]
    loads.append(pltpu.make_async_copy(master_far, master, load_sem.at[blocks]))
    loads.append(pltpu.make_async_copy(momentum_far, momentum, load_sem.at[blocks + 1]))
    loads.append(pltpu.make_async_copy(owners_far, owners, load_sem.at[blocks + 2]))
    for load in loads:
        load.start()
    pl.semaphore_wait(barrier, jnp.where(is_tip, 3, 4) + shard_count - 1)
    pl.when(middle)(lambda: greet(ready, rep=place(2)))

    def pass_ready():
        @pl.when(middle)
        def _():
            pl.semaphore_wait(ready, 1)
            greet(ready, rep=place(0))

    def all_ready():
        pl.when(is_tip)(lambda: pl.semaphore_wait(ready, 1))


    sent, roles = {}, {}
    spans, phases = (("slot", 0), ("slot", 1), ("early",), ("norm",), ("shard",)), ({}, {})
    gathers = ("wide", "wider", "up", "over", "down", "outward", "across", "inward", "block", "blocks")

    def copy(group, src, dst, **to):
        kind = group[0]
        if group in spans:
            number = spans.index(group)
        else:
            numbers = phases[kind in gathers]
            number = len(spans) + numbers.setdefault(group, len(numbers))
        sent.setdefault(kind, len(sent))
        return pltpu.make_async_remote_copy(
            src_ref=src, dst_ref=dst, send_sem=send_sem.at[sent[kind]], recv_sem=recv_sem.at[number],
            device_id=to, device_id_type=pl.DeviceIdType.MESH,
        )

    def send(group, src, dst, **to):
        roles[group[0]] = None
        copy(group, src, dst, **to).start()

    def send_if(role, group, src, dst, **to):
        roles[group[0]] = role
        pl.when(role)(copy(group, src, dst, **to).start)

    def arrive(group, like):
        copy(group, like, like, rep=q).wait_recv()

    def leave(kind, like):
        made = pltpu.make_async_remote_copy(
            src_ref=like, dst_ref=like, send_sem=send_sem.at[sent[kind]], recv_sem=recv_sem.at[0],
            device_id={"rep": q}, device_id_type=pl.DeviceIdType.MESH,
        )
        if roles[kind] is None:
            made.wait_send()
        else:
            pl.when(roles[kind])(made.wait_send)

    def loop(count, body):
        def step(i, carry):
            body(i)
            return carry

        lax.fori_loop(0, count, step, 0)

    def up(value):
        return value.astype(jnp.float32)

    def down(value):
        return value.astype(jnp.bfloat16)

    def cols(region, k):
        width = widths[region]
        return pl.ds(pl.multiple_of(base[region] + k * width, 128), width)

    def pair_cols(r, b, k):
        return pl.ds(pl.multiple_of(base[r] + k * widths[r], 128), pair(b)[r])

    def local_cols(region):
        return pl.ds(offset[region], widths[region])

    def pair_local(r, b):
        return pl.ds(offset[r], pair(b)[r])

    def deep_cols(b, k):
        return pl.ds(pl.multiple_of(k * deep_width(b), 128), deep_width(b))

    def order(region, b):
        return ("x", "y") if (region + b) % 2 == 0 else ("y", "x")

    def at_rows(g):
        return slice(None) if g is None else (q + g) % rep_count

    def each(g, body):
        if g is None:
            loop(rep_count, body)
        else:
            body((q + g) % rep_count)

    tail = (None,)
    others_of = tuple(range(1, rep_count))

    def late(b):
        return b >= blocks - LATE

    whole = pl.ds(base[2], pod_count * wc)

    def quarter(axis, j, away):
        if axis == "x":
            return j * SIDE + (1 - x if away else x)
        return (1 - y if away else y) * SIDE + j

    def stay(axis):
        return y if axis == "x" else x

    def send_first(b, g):
        i = at_rows(g)
        for r in range(2):
            axis = order(r, b)[0]
            for j in range(SIDE):
                send(
                    ("first", b, g), deltas.at[b, i, :, pair_cols(r, b, quarter(axis, j, True))],
                    first[r].at[j, b, i, :, part(r, b)], outer=neighbour[axis],
                )

    def send_second(b, g):
        arrive(("first", b, g), deltas.at[b, at_rows(g), :, pl.ds(0, SIDE * pair_width(b))])
        for r in range(2):
            axis, other = order(r, b)
            go = 1 - stay(axis)
            at = pair_cols(r, b, quarter(axis, go, False))

            def body(i):
                came = first[r][go, b, i, :, part(r, b)]
                passed[r][b, i, :, part(r, b)] = down(up(deltas[b, i, :, at]) + up(came))

            each(g, body)
            i = at_rows(g)
            send(
                ("second", b, g), passed[r].at[b, i, :, part(r, b)],
                second[r].at[b, i, :, part(r, b)], outer=neighbour[other],
            )

    def pair_total(r, b, i):
        at = part(r, b)
        total = up(deltas[b, i, :, pair_cols(r, b, o)]) + up(first[r][stay(order(r, b)[0]), b, i, :, at])
        return total + up(second[r][b, i, :, at])

    def send_third(b):
        groups = others_of if late(b) else tail
        for g in groups:
            arrive(("second", b, g), deltas.at[b, at_rows(g), :, pl.ds(0, pair_width(b))])
        for d in others_of:
            there = (q + d) % rep_count
            for r in range(2):
                zin[b, d - 1, :, pair_local(r, b)] = down(pair_total(r, b, there))
            at = pl.ds(0, pair_width(b))
            send(("third", b), zin.at[b, d - 1, :, at], zrecv.at[d - 1, b, :, at], rep=there)

    def deep_of(b, i):
        keep = pair(b)[1]
        if keep == wb:
            return deltas[b, i, :, whole]
        parts = []
        for k in range(pod_count):
            parts.append(deltas[b, i, :, pl.ds(base[1] + k * wb + keep, wb - keep)])
            parts.append(deltas[b, i, :, pl.ds(base[2] + k * wc, wc)])
        return jnp.concatenate(parts, axis=-1)

    def start_tips(b):
        @pl.when(is_tip)
        def _():
            for k in (3, 2, 1):
                staged[k - 1, b, :, deep(b)] = deep_of(b, place(k))
                copy(("near", b, k), staged.at[k - 1, b, :, deep(b)], near.at[k - 1, b, :, deep(b)], rep=place(1)).start()

        roles["near"] = is_tip

    def relay_near(b):
        @pl.when(middle)
        def _():
            for k in (3, 2):
                arrive(("near", b, k), near.at[k - 1, b, :, deep(b)])
                onward[k - 1, b, :, deep(b)] = down(up(deep_of(b, place(k))) + up(near[k - 1, b, :, deep(b)]))
                copy(("far", b, 3 - k), onward.at[k - 1, b, :, deep(b)], far.at[3 - k, b, :, deep(b)], rep=place(2)).start()

        roles["far"] = middle

    def relay_far(b):
        @pl.when(middle)
        def _():
            arrive(("far", b, 0), far.at[0, b, :, deep(b)])
            onward[0, b, :, deep(b)] = down(up(deep_of(b, place(0))) + up(far[0, b, :, deep(b)]))
            copy(("last", b), onward.at[0, b, :, deep(b)], last.at[b, :, deep(b)], rep=place(0)).start()

        roles["last"] = middle

    def send_cross(b):
        at = deep(b)

        @pl.when(is_tip)
        def _():
            arrive(("last", b), last.at[b, :, at])
            ztotal[b, :, at] = down(up(deep_of(b, q)) + up(last[b, :, at]))

        @pl.when(middle)
        def _():
            arrive(("near", b, 1), near.at[0, b, :, at])
            arrive(("far", b, 1), far.at[1, b, :, at])
            total = up(deep_of(b, q)) + up(near[0, b, :, at])
            ztotal[b, :, at] = down(total + up(far[1, b, :, at]))

        for d in range(1, pod_count):
            send(
                ("cross", b), ztotal.at[b, :, deep_cols(b, pod(d))],
                cross.at[d - 1, b, :, pl.ds(0, deep_width(b))], outer=pod(d),
            )

    scale = 1.0 / (pod_count * rep_count)

    def put_mean(b, at, total):
        value = total * scale
        mean[b, :, at] = down(value)
        square = value * value
        part = squares[0]
        height, width = square.shape
        for k in range(height // 8):
            for i in range(width // 128):
                part = part + square[k * 8:(k + 1) * 8, i * 128:(i + 1) * 128]
        squares[0] = part

    def finish_pair(b):
        if late(b):
            arrive(("second", b, 0), deltas.at[b, q, :, pl.ds(0, pair_width(b))])
        arrive(("third", b), zrecv.at[:, b, :, pl.ds(0, pair_width(b))])
        for r in range(2):
            total = pair_total(r, b, q)
            for d in range(rep_count - 1):
                total = total + up(zrecv[d, b, :, pair_local(r, b)])
            put_mean(b, pair_local(r, b), total)

    def finish_cross(b):
        at = pl.ds(0, deep_width(b))
        arrive(("cross", b), cross.at[:, b, :, at])
        total = up(ztotal[b, :, deep_cols(b, o)])
        for d in range(pod_count - 1):
            total = total + up(cross[d, b, :, at])
        put_mean(b, pl.ds(pair_width(b), deep_width(b)), total)

    owner, rank = [], []

    def read_owners():
        loads[blocks + 2].wait()
        owner.extend(owners[b] for b in range(blocks))
        for b in range(blocks):
            count = jnp.int32(0)
            for before in range(b):
                count = count + (owner[before] == owner[b]).astype(jnp.int32)
            rank.append(count)

    def block_of(k, j):
        index, found = jnp.int32(0), jnp.int32(0)
        for b in range(blocks):
            match = ((owner[b] == k) & (rank[b] == j)).astype(jnp.int32)
            index, found = index + b * match, found + match
        return index, found

    def load_rows(b):
        loads[b].wait()

    def pack_early():
        loads[blocks].wait()
        loads[blocks + 1].wait()
        for k in range(pod_count):
            for r in range(3):
                at = pl.ds(base[r] + k * widths[r], widths[r])

                def body(i):
                    value = master[i, :, at] - 0.567 * momentum[i, :, at]
                    apack[k, i, :, local_cols(r)] = down(value)

                loop(slots, body)
        arecv[o] = apack[o]

    def send_early(*steps):
        for d in steps:
            send(("early",), apack.at[pod(d)], arecv.at[o], outer=pod(d))

    group = pod_count * rep_count

    lead = s == 0
    follow = jnp.logical_not(lead)
    partial = group + shard_count

    def norm_send():
        others[partial] = jnp.sum(squares[0], axis=0, keepdims=True)
        send_if(follow, ("shard",), others.at[partial], others.at[group + s], shard=0)

    def norm_lead():
        roles["norm"] = lead

        @pl.when(lead)
        def _():
            arrive(("shard",), others.at[pl.ds(group + 1, shard_count - 1)])
            total = others[partial]
            for d in range(1, shard_count):
                total = total + others[group + d]
            others[group] = total
            others[0] = total
            for e in range(rep_count):
                for d in range(pod_count):
                    for t in range(shard_count):
                        if d or e or t:
                            copy(
                                ("norm",), others.at[group], others.at[d * rep_count + e],
                                outer=pod(d), rep=(q + e) % rep_count, shard=t,
                            ).start()

    def mean_send(part):
        at = pl.ds(wa + wb, wc) if part == 0 else pl.ds(0, wa + wb)
        for d in range(pod_count):
            for j in range(slots):
                packed[d, j, :, at] = mean[block_of(pod(d), j)[0], :, at]
            if d == 0:
                slotted[o, :, :, at] = packed[0, :, :, at]
            else:
                send(("slot", part), packed.at[d, :, :, at], slotted.at[o, :, :, at], outer=pod(d))

    def norm_wait():
        pl.when(lead)(lambda: arrive(("norm",), others.at[pl.ds(1, group - 1)]))
        pl.when(follow)(lambda: arrive(("norm",), others.at[pl.ds(0, group)]))
        arrive(("early",), arecv.at[pl.ds(1, pod_count - 1)])
        total = others[0]
        for d in range(1, group):
            total = total + others[d]
        total = jnp.sum(total, keepdims=True)
        return jnp.minimum(1.0, clip_limit / jnp.sqrt(total + 1e-06))

    def spread(b, factor):
        for r in range(3):
            at = local_cols(r)
            early = up(arecv[owner[b], jnp.minimum(rank[b], slots - 1), :, at])
            value = early - (1.33 * factor) * up(mean[b, :, at])
            out[b, q, :, cols(r, o)] = down(value)

    def send_wide(b):
        at = out.at[b, q, :, cols(2, o)]
        send(("wide", b), at, at, outer=neighbour[order(0, b)[0]])

    def send_wider(b):
        arrive(("wide", b), out.at[b, q, :, pl.ds(0, wc)])
        axis, other = order(0, b)
        for k in (o, neighbour[axis]):
            at = out.at[b, q, :, cols(2, k)]
            send(("wider", b), at, at, outer=neighbour[other])

    def pass_line(role, group, b, k, **to):
        for r in range(2):
            at = out.at[b, place(k), :, cols(r, o)]
            send_if(role, group, at, at, **to)

    def line_rows(b, count):
        return out.at[b, pl.ds(0, count), :, pl.ds(0, wa + wb)]

    def send_up(b):
        pass_line(is_tip, ("up", b), b, 0, rep=place(1))

    def send_mid(b):
        pass_line(middle, ("down", b), b, 1, rep=place(0))
        pass_line(middle, ("over", b, 1), b, 1, rep=place(2))

    def line_near(b):
        pl.when(middle)(lambda: arrive(("over", b, 1), line_rows(b, 1)))
        pass_line(middle, ("down", b), b, 2, rep=place(0))
        pl.when(middle)(lambda: arrive(("up", b), line_rows(b, 1)))
        pass_line(middle, ("over", b, 0), b, 0, rep=place(2))

    def line_far(b):
        pl.when(middle)(lambda: arrive(("over", b, 0), line_rows(b, 1)))
        pass_line(middle, ("down", b), b, 3, rep=place(0))

    def wide_done(b):
        arrive(("wider", b), out.at[b, q, :, pl.ds(0, SIDE * wc)])

    def line_tip(b):
        mine = out.at[b, q, :, whole]
        pl.when(is_tip)(lambda: wide_done(b))
        send_if(is_tip, ("outward", b, 0), mine, mine, rep=place(1))

    def line_mid(b):
        mine = out.at[b, q, :, whole]
        pl.when(middle)(lambda: wide_done(b))
        send_if(middle, ("across", b, 1), mine, mine, rep=place(2))

    def line_across(b):
        at = out.at[b, place(0), :, whole]
        pl.when(middle)(lambda: arrive(("outward", b, 0), at))
        send_if(middle, ("across", b, 0), at, at, rep=place(2))

    def line_inward(b, k):
        at = out.at[b, place(k), :, whole]
        if k > 1:
            pl.when(middle)(lambda: arrive(("across", b, 3 - k), at))
        send_if(middle, ("inward",), at, at, rep=place(0))

    def line_end():
        pl.when(is_tip)(lambda: arrive(("inward",), out.at[:, pl.ds(0, 3), :, whole]))

    def send_block(b, d):
        i = (q + rep_count - d) % rep_count
        for r in range(2):
            at = out.at[b, i, :, cols(r, o)]
            send(("block", b, d), at, at, outer=neighbour[order(r, b)[1]])

    def send_blocks(b, d):
        i = (q + rep_count - d) % rep_count
        arrive(("block", b, d), out.at[b, i, :, pl.ds(0, wa + wb)])
        for r in range(2):
            axis = order(r, b)[0]
            for j in range(SIDE):
                at = out.at[b, i, :, cols(r, quarter(axis, j, False))]
                send(("blocks",), at, at, outer=neighbour[axis])

    def update(factor):
        for part, width in enumerate((wc, wa + wb)):
            arrive(("slot", part), slotted.at[pl.ds(1, pod_count - 1), :, :, pl.ds(0, width)])
        for j in range(slots):
            found = block_of(o, j)[1].astype(jnp.float32)
            for k in range(pod_count):
                for r in range(3):
                    at = pl.ds(base[r] + k * widths[r], widths[r])
                    step = (factor * found) * up(slotted[k, j, :, local_cols(r)])
                    moved = 0.9 * momentum[j, :, at] + step
                    new_momentum[j, :, at] = moved
                    new_master[j, :, at] = master[j, :, at] - 0.7 * (step + 0.9 * moved)

    def finish():
        arrive(("blocks",), out.at[:, :, :, pl.ds(0, SIDE * (wa + wb))])

    def drain():
        pairs = sum(pair_width(b) for b in range(blocks))
        deeps = sum(deep_width(b) for b in range(blocks))
        some = blocks // 2

        def rows(count, width):
            return deltas.at[0, pl.ds(0, count), :, pl.ds(0, width)]

        def deep_rows(count):
            return deltas.at[pl.ds(0, some), pl.ds(0, count), :, pl.ds(0, pod_count * deeps // some)]

        leave("first", deltas.at[pl.ds(0, SIDE), :, :, pl.ds(0, pairs)])
        leave("second", rows(rep_count, pairs))
        leave("third", rows(rep_count - 1, pairs))
        leave("near", deep_rows(3))
        leave("far", deep_rows(2))
        leave("last", deep_rows(1))
        leave("cross", rows(pod_count - 1, deeps))
        leave("early", arecv.at[pl.ds(1, pod_count - 1)])
        leave("norm", others.at[pl.ds(0, group * shard_count - 1)])
        leave("slot", slotted.at[pl.ds(1, pod_count - 1)])
        leave("shard", others.at[pl.ds(0, 1)])
        leave("wide", out.at[:, 0, :, pl.ds(0, wc)])
        leave("wider", out.at[:, 0, :, pl.ds(0, SIDE * wc)])
        leave("up", out.at[:, 0, :, pl.ds(0, wa + wb)])
        leave("over", out.at[:, pl.ds(0, 2), :, pl.ds(0, wa + wb)])
        leave("down", out.at[:, pl.ds(0, 3), :, pl.ds(0, wa + wb)])
        leave("outward", out.at[:, 0, :, whole])
        leave("across", out.at[:, pl.ds(0, 2), :, whole])
        leave("inward", out.at[:, pl.ds(0, 3), :, whole])
        leave("block", out.at[:, :, :, pl.ds(0, wa + wb)])
        leave("blocks", out.at[:, :, :, pl.ds(0, SIDE * (wa + wb))])

    def rests(b):
        pl.when(is_tip)(lambda: arrive(("down", b), line_rows(b, 3)))
        for d in others_of:
            send_block(b, d)

    def rests_on(b):
        for d in others_of:
            send_blocks(b, d)

    squares[0] = jnp.zeros(squares.shape[1:], jnp.float32)
    def firsts(b):
        for g in others_of if late(b) else tail:
            send_first(b, g)

    def seconds(b):
        for g in others_of if late(b) else tail:
            send_second(b, g)

    for b in range(blocks):
        load_rows(b)
        if b < 2:
            firsts(b)
        if b > 0:
            start_tips(b - 1)
    start_tips(blocks - 1)
    pack_early()
    read_owners()
    for t in range(blocks + 2):
        if t < blocks:
            relay_near(t)
            if t == 0:
                pass_ready()
            seconds(t)
            if t == 0:
                all_ready()
        if t + 2 < blocks:
            firsts(t + 2)
            if t + 3 == blocks:
                for b in range(blocks - LATE, blocks - 2):
                    send_first(b, 0)
        if t == blocks - 1:
            for b in range(max(blocks - LATE, blocks - 2), blocks):
                send_first(b, 0)
        if 0 <= t - 1 < blocks:
            if t == blocks:
                send_early(1, 2)
                for b in range(blocks - LATE, blocks):
                    send_second(b, 0)
                send_third(t - 1)
                relay_far(t - 1)
            else:
                relay_far(t - 1)
                send_third(t - 1)
        if 0 <= t - 2 < blocks:
            send_cross(t - 2)
    send_early(3)
    for b in range(blocks):
        if b < 2:
            finish_pair(b)
        finish_cross(b)
    mean_send(0)
    for b in range(2, blocks):
        finish_pair(b)
    norm_send()
    norm_lead()
    mean_send(1)
    factor = norm_wait()
    for b in range(blocks):
        spread(b, factor)
        send_wide(b)
        send_up(b)
        if b < 2:
            send_mid(b)
        send_block(b, 0)
    line_near(0)
    send_wider(0)
    send_blocks(0, 0)
    line_near(1)
    send_wider(1)
    send_blocks(1, 0)
    send_mid(2)
    line_far(0)
    for b in range(2, blocks):
        send_wider(b)
        send_blocks(b, 0)
    for b in range(blocks):
        line_tip(b)
    rests(0)
    line_near(2)
    line_far(1)
    send_mid(3)
    line_near(3)
    rests(1)
    line_mid(0)
    line_mid(1)
    line_far(2)
    line_mid(2)
    line_mid(3)
    rests_on(0)
    line_across(0)
    rests(2)
    line_far(3)
    line_across(1)
    rests_on(1)
    rests(3)
    line_across(2)
    line_across(3)
    for b in range(blocks):
        line_inward(b, 1)
        line_inward(b, 2)
    rests_on(2)
    update(factor)
    line_inward(0, 3)
    line_inward(1, 3)
    rests_on(3)
    line_inward(2, 3)
    line_inward(3, 3)
    line_end()
    finish()
    drain()
    assert len(spans) + max(len(p) for p in phases) == recv_sem.shape[0]
    assert len(sent) == send_sem.shape[0]


def store(*refs):
    sem = refs[-1]
    copies = []
    for i in range(3):
        for k in range(refs[i].shape[0]):
            copies.append(pltpu.make_async_copy(refs[i].at[k], refs[i + 3].at[k], sem.at[len(copies)]))
    for copy in copies:
        copy.start()
    for copy in copies:
        copy.wait()


def regions(width, pod_count):
    tiles = width // (128 * pod_count)
    wc = max(1, round(tiles * DEEP))
    wb = (tiles - wc) // 2
    return tuple(128 * n for n in (tiles - wc - wb, wb, wc, EXTRA))


def fused(deltas, owners, master, momentum):
    blocks = owners.shape[1]
    slots, sub_rows, width = master.shape[2:]
    pod_count, rep_count = lax.axis_size("outer"), lax.axis_size("rep")
    shard_count = lax.axis_size("shard")
    entries = shard_count * blocks * rep_count * sub_rows * width
    clip_limit = 0.5 * math.sqrt(entries)
    widths = regions(width, pod_count)
    wa, wb, wc, extra = widths
    part, deep_width = width // pod_count, extra + wc
    deep = pod_count * deep_width
    group = pod_count * rep_count
    reduce_waits = 2 * (blocks + (rep_count - 1) * LATE) + 8 * blocks
    waits = 5 + max(reduce_waits, blocks * (rep_count + 9) + 2)
    vmem, hbm = pl.BlockSpec(memory_space=pltpu.VMEM), pl.BlockSpec(memory_space=pltpu.HBM)
    bf16, f32 = jnp.bfloat16, jnp.float32
    V = pltpu.VMEM
    out, new_momentum, new_master = pl.pallas_call(
        functools.partial(kernel, widths, (pod_count, rep_count, shard_count), clip_limit),
        out_shape=(
            V((blocks, rep_count, sub_rows, width), bf16),
            V(master.shape[2:], f32),
            V(master.shape[2:], f32),
        ),
        in_specs=[hbm] * 4,
        out_specs=(vmem, vmem, vmem),
        scratch_shapes=[
            pltpu.SMEM((blocks,), jnp.int32),
            V((blocks, rep_count, sub_rows, width), bf16),
            V(master.shape[2:], f32),
            V(master.shape[2:], f32),
            pltpu.SemaphoreType.DMA((blocks + 3,)),
            [V((SIDE, blocks, rep_count, sub_rows, w), bf16) for w in (wa, wb)],
            [V((blocks, rep_count, sub_rows, w), bf16) for w in (wa, wb)],
            [V((blocks, rep_count, sub_rows, w), bf16) for w in (wa, wb)],
            V((blocks, rep_count - 1, sub_rows, wa + wb), bf16),
            V((rep_count - 1, blocks, sub_rows, wa + wb), bf16),
            V((3, blocks, sub_rows, deep), bf16),
            V((3, blocks, sub_rows, deep), bf16),
            V((2, blocks, sub_rows, deep), bf16),
            V((blocks, sub_rows, deep), bf16),
            V((3, blocks, sub_rows, deep), bf16),
            V((blocks, sub_rows, deep), bf16),
            V((pod_count - 1, blocks, sub_rows, deep_width), bf16),
            V((pod_count, slots, sub_rows, part), bf16),
            V((pod_count, slots, sub_rows, part), bf16),
            V((blocks, sub_rows, part), bf16),
            V((pod_count, slots, sub_rows, part), bf16),
            V((pod_count, slots, sub_rows, part), bf16),
            V((1, 8, 128), f32),
            V((group * shard_count + shard_count, 1, 128), f32),
            pltpu.SemaphoreType.DMA((KINDS,)),
            pltpu.SemaphoreType.DMA((waits,)),
            pltpu.SemaphoreType.REGULAR,
        ],
        compiler_params=pltpu.CompilerParams(
            collective_id=0, has_side_effects=True, vmem_limit_bytes=48 * 1024 * 1024
        ),
    )(
        owners[0, :, 0],
        deltas.reshape(blocks, rep_count, sub_rows, width),
        master.reshape(master.shape[2:]),
        momentum.reshape(momentum.shape[2:]),
    )
    arrays = (out, new_momentum, new_master)
    out, new_momentum, new_master = pl.pallas_call(
        store,
        out_shape=tuple(jax.ShapeDtypeStruct(a.shape, a.dtype) for a in arrays),
        in_specs=[pl.BlockSpec(memory_space=pl.ANY)] * 3,
        out_specs=(hbm,) * 3,
        scratch_shapes=[pltpu.SemaphoreType.DMA((blocks + 2 * slots,))],
        compiler_params=pltpu.CompilerParams(vmem_limit_bytes=4 * 1024 * 1024),
    )(*(pltpu.with_memory_space_constraint(a, pltpu.VMEM) for a in arrays))
    return (
        out.reshape(blocks * rep_count * sub_rows, width),
        new_momentum.reshape(momentum.shape),
        new_master.reshape(master.shape),
    )


def local(deltas, owners, master, momentum):
    blocks_here = owners.shape[1]
    slot_count = master.shape[2]
    sub_rows = master.shape[3]
    row_width = deltas.shape[3]
    block_rows = deltas.shape[2] // blocks_here
    pod_count = lax.axis_size("outer")
    rep_count = lax.axis_size("rep")
    owned_blocks = owners[0, :, 0]
    pod_ids = jnp.arange(pod_count, dtype=jnp.int32)
    onehot = (owned_blocks[:, None] == pod_ids[None, :]).astype(jnp.int32)
    rank_all = jnp.cumsum(onehot, axis=0) - onehot
    rank_own = jnp.sum(rank_all * onehot, axis=1)
    slot_ids = jnp.arange(slot_count, dtype=jnp.int32)
    selector = (
        (owned_blocks[None, None, :] == pod_ids[:, None, None])
        & (rank_own[None, None, :] == slot_ids[None, :, None])
    ).astype(jnp.bfloat16)
    local_rows = deltas[0, 0].reshape(blocks_here, block_rows, row_width)
    block_sums = lax.psum_scatter(
        local_rows.astype(jnp.float32).astype(jnp.bfloat16), "rep", scatter_dimension=1, tiled=True
    ).astype(jnp.float32)
    block_sums = block_sums.astype(jnp.bfloat16)
    pod_part = jnp.einsum(
        "ojb,brw->ojrw", selector, block_sums, preferred_element_type=jnp.float32
    ).astype(jnp.bfloat16)
    arrived = lax.all_to_all(pod_part, "outer", split_axis=0, concat_axis=0, tiled=True)
    mean_share = jnp.sum(arrived.astype(jnp.float32), axis=0) / (pod_count * rep_count)
    local_sq = jnp.sum(mean_share * mean_share)
    total_sq = lax.psum(local_sq, ("outer", "rep", "shard"))
    total_entries = lax.axis_size("shard") * blocks_here * block_rows * row_width
    clip_limit = 0.5 * math.sqrt(total_entries)
    factor = jnp.minimum(1.0, clip_limit / jnp.sqrt(total_sq + 1e-06))
    step_part = factor * mean_share[None, None]
    new_momentum = 0.9 * momentum + step_part
    new_master = master - 0.7 * (step_part + 0.9 * new_momentum)
    params_here = new_master.astype(jnp.bfloat16)
    gathered = lax.all_gather(params_here, ("outer", "rep"), axis=0, tiled=True).reshape(
        pod_count, rep_count, slot_count, sub_rows, row_width
    )
    unpacked = jnp.einsum("ojb,oqjrw->bqrw", selector, gathered, preferred_element_type=jnp.float32)
    new_params = unpacked.astype(jnp.bfloat16).reshape(blocks_here * block_rows, row_width)
    return (new_params, new_momentum, new_master)


def solution(mesh):
    fits = mesh.shape["outer"] == SIDE * SIDE and mesh.shape["rep"] == LINE

    def body(deltas, owners, master, momentum):
        blocks = owners.shape[1]
        width, sub_rows = master.shape[4], master.shape[3]
        tiled = width % (SIDE * SIDE * 128) == 0 and width >= 3 * SIDE * SIDE * 128
        tiled = tiled and sub_rows % TILE == 0 and blocks == SIDE * SIDE
        tiled = tiled and deltas.shape[2] == blocks * LINE * sub_rows
        if tiled:
            wa, wb, wc, extra = regions(width, SIDE * SIDE)
            tiled = wb > extra and SIDE * blocks * (wc + extra) <= width
        return (fused if fits and tiled else local)(deltas, owners, master, momentum)

    return jax.shard_map(
        body,
        mesh=mesh,
        in_specs=(
            P("outer", "rep", "shard", None),
            P("shard", None, None),
            P("outer", "shard", None, "rep", None),
            P("outer", "shard", None, "rep", None),
        ),
        out_specs=(
            P("shard", None),
            P("outer", "shard", None, "rep", None),
            P("outer", "shard", None, "rep", None),
        ),
        check_vma=False,
    )
```

```python
import functools
import math

import jax
import jax.numpy as jnp
from jax import lax
from jax.experimental import pallas as pl
from jax.experimental.pallas import tpu as pltpu
from jax.sharding import PartitionSpec as P

DEEP = 0.2
EXTRA = 1
THICK = 2
TILE = 16
SIDE = 2
LATE = 4
KINDS = 14
LINE = 4


def kernel(
    plan, axis_sizes, clip_limit,
    owners_far, deltas_far, master_far, momentum_far,
    out, new_momentum, new_master,
    owners, deltas, master, momentum, load_sem, first, passed, second, zin, zrecv,
    staged, near, far, last, onward, ztotal, cross,
    apack, arecv, mean, packed, slotted, squares, others,
    send_sem, recv_sem, ready,
):
    wa, wb, wc, extra = plan
    pod_count, rep_count, shard_count = axis_sizes
    blocks, sub_rows, slots = deltas.shape[0], master.shape[1], master.shape[0]
    widths = (wa, wb, wc)
    base = (0, pod_count * wa, pod_count * (wa + wb))
    offset = (0, wa, wa + wb)

    def pair(b):
        return (wa, wb - extra if b < THICK else wb)

    def pair_width(b):
        return sum(pair(b))

    def deep_width(b):
        return wa + wb + wc - pair_width(b)

    def part(r, b):
        return pl.ds(0, pair(b)[r])

    def deep(b):
        return pl.ds(0, pod_count * deep_width(b))

    o, q, s = lax.axis_index("outer"), lax.axis_index("rep"), lax.axis_index("shard")
    y, x = o // SIDE, o % SIDE
    neighbour = {"x": y * SIDE + 1 - x, "y": (1 - y) * SIDE + x}
    is_low = q < rep_count // 2
    tip = jnp.where(is_low, 0, rep_count - 1)
    is_tip = q == tip

    def place(k):
        return jnp.where(is_low, k, rep_count - 1 - k)

    def pod(d):
        return ((y + d // SIDE) % SIDE) * SIDE + (x + d % SIDE) % SIDE

    barrier = pltpu.get_barrier_semaphore()

    def greet(sem, **to):
        pl.semaphore_signal(sem, inc=1, device_id=to, device_id_type=pl.DeviceIdType.MESH)

    middle = jnp.logical_not(is_tip)
    greet(barrier, outer=neighbour["x"])
    greet(barrier, outer=neighbour["y"])
    greet(barrier, rep=jnp.where(is_tip, place(1), place(0)))
    pl.when(middle)(lambda: greet(barrier, rep=place(2)))
    for d in range(1, shard_count):
        greet(barrier, shard=(s + d) % shard_count)
    loads = [
        pltpu.make_async_copy(deltas_far.at[b], deltas.at[b], load_sem.at[b]) for b in range(blocks)
    ]
    loads.append(pltpu.make_async_copy(master_far, master, load_sem.at[blocks]))
    loads.append(pltpu.make_async_copy(momentum_far, momentum, load_sem.at[blocks + 1]))
    loads.append(pltpu.make_async_copy(owners_far, owners, load_sem.at[blocks + 2]))
    for load in loads:
        load.start()
    pl.semaphore_wait(barrier, jnp.where(is_tip, 3, 4) + shard_count - 1)
    pl.when(middle)(lambda: greet(ready, rep=place(2)))

    def pass_ready():
        @pl.when(middle)
        def _():
            pl.semaphore_wait(ready, 1)
            greet(ready, rep=place(0))

    def all_ready():
        pl.when(is_tip)(lambda: pl.semaphore_wait(ready, 1))


    sent, roles = {}, {}
    shared = {
        "second": "first", "last": "far", "slot": "early", "outward": "up", "across": "over",
        "inward": "down", "blocks": "block",
    }
    spans, phases = (("slot", 0), ("slot", 1), ("early",), ("norm",), ("shard",)), ({}, {})
    gathers = ("wide", "wider", "up", "over", "down", "outward", "across", "inward", "block", "blocks")

    def copy(group, src, dst, **to):
        kind = shared.get(group[0], group[0])
        if group in spans:
            number = spans.index(group)
        else:
            numbers = phases[group[0] in gathers]
            number = len(spans) + numbers.setdefault(group, len(numbers))
        sent.setdefault(kind, len(sent))
        return pltpu.make_async_remote_copy(
            src_ref=src, dst_ref=dst, send_sem=send_sem.at[sent[kind]], recv_sem=recv_sem.at[number],
            device_id=to, device_id_type=pl.DeviceIdType.MESH,
        )

    def send(group, src, dst, **to):
        roles[group[0]] = None
        copy(group, src, dst, **to).start()

    def send_if(role, group, src, dst, **to):
        roles[group[0]] = role
        pl.when(role)(copy(group, src, dst, **to).start)

    def arrive(group, like):
        copy(group, like, like, rep=q).wait_recv()

    def leave(kind, like):
        made = pltpu.make_async_remote_copy(
            src_ref=like, dst_ref=like, send_sem=send_sem.at[sent[kind]], recv_sem=recv_sem.at[0],
            device_id={"rep": q}, device_id_type=pl.DeviceIdType.MESH,
        )
        if roles[kind] is None:
            made.wait_send()
        else:
            pl.when(roles[kind])(made.wait_send)

    def loop(count, body):
        def step(i, carry):
            body(i)
            return carry

        lax.fori_loop(0, count, step, 0)

    def up(value):
        return value.astype(jnp.float32)

    def down(value):
        return value.astype(jnp.bfloat16)

    def cols(region, k):
        width = widths[region]
        return pl.ds(pl.multiple_of(base[region] + k * width, 128), width)

    def pair_cols(r, b, k):
        return pl.ds(pl.multiple_of(base[r] + k * widths[r], 128), pair(b)[r])

    def local_cols(region):
        return pl.ds(offset[region], widths[region])

    def pair_local(r, b):
        return pl.ds(offset[r], pair(b)[r])

    def deep_cols(b, k):
        return pl.ds(pl.multiple_of(k * deep_width(b), 128), deep_width(b))

    def order(region, b):
        return ("x", "y") if (region + b) % 2 == 0 else ("y", "x")

    def at_rows(g):
        return slice(None) if g is None else (q + g) % rep_count

    def each(g, body):
        if g is None:
            loop(rep_count, body)
        else:
            body((q + g) % rep_count)

    tail = (None,)
    others_of = tuple(range(1, rep_count))

    def late(b):
        return b >= blocks - LATE

    whole = pl.ds(base[2], pod_count * wc)

    def quarter(axis, j, away):
        if axis == "x":
            return j * SIDE + (1 - x if away else x)
        return (1 - y if away else y) * SIDE + j

    def stay(axis):
        return y if axis == "x" else x

    def send_first(b, g):
        i = at_rows(g)
        for r in range(2):
            axis = order(r, b)[0]
            for j in range(SIDE):
                send(
                    ("first", b, g), deltas.at[b, i, :, pair_cols(r, b, quarter(axis, j, True))],
                    first[r].at[j, b, i, :, part(r, b)], outer=neighbour[axis],
                )

    def send_second(b, g):
        arrive(("first", b, g), deltas.at[b, at_rows(g), :, pl.ds(0, SIDE * pair_width(b))])
        for r in range(2):
            axis, other = order(r, b)
            go = 1 - stay(axis)
            at = pair_cols(r, b, quarter(axis, go, False))

            def body(i):
                came = first[r][go, b, i, :, part(r, b)]
                passed[r][b, i, :, part(r, b)] = down(up(deltas[b, i, :, at]) + up(came))

            each(g, body)
            i = at_rows(g)
            send(
                ("second", b, g and 1), passed[r].at[b, i, :, part(r, b)],
                second[r].at[b, i, :, part(r, b)], outer=neighbour[other],
            )

    def pair_total(r, b, i):
        at = part(r, b)
        total = up(deltas[b, i, :, pair_cols(r, b, o)]) + up(first[r][stay(order(r, b)[0]), b, i, :, at])
        return total + up(second[r][b, i, :, at])

    def send_third(b):
        width = pl.ds(0, pair_width(b))
        if late(b):
            arrive(("second", b, 1), deltas.at[b, pl.ds(0, rep_count - 1), :, width])
        else:
            arrive(("second", b, None), deltas.at[b, :, :, width])
        for d in others_of:
            there = (q + d) % rep_count
            for r in range(2):
                zin[b, d - 1, :, pair_local(r, b)] = down(pair_total(r, b, there))
            at = pl.ds(0, pair_width(b))
            send(("third", b), zin.at[b, d - 1, :, at], zrecv.at[d - 1, b, :, at], rep=there)

    def deep_of(b, i):
        keep = pair(b)[1]
        if keep == wb:
            return deltas[b, i, :, whole]
        parts = []
        for k in range(pod_count):
            parts.append(deltas[b, i, :, pl.ds(base[1] + k * wb + keep, wb - keep)])
            parts.append(deltas[b, i, :, pl.ds(base[2] + k * wc, wc)])
        return jnp.concatenate(parts, axis=-1)

    def start_tips(b):
        @pl.when(is_tip)
        def _():
            for k in (3, 2, 1):
                staged[k - 1, b, :, deep(b)] = deep_of(b, place(k))
                copy(("near", b, k), staged.at[k - 1, b, :, deep(b)], near.at[k - 1, b, :, deep(b)], rep=place(1)).start()

        roles["near"] = is_tip

    def relay_near(b):
        @pl.when(middle)
        def _():
            for k in (3, 2):
                arrive(("near", b, k), near.at[k - 1, b, :, deep(b)])
                onward[k - 1, b, :, deep(b)] = down(up(deep_of(b, place(k))) + up(near[k - 1, b, :, deep(b)]))
                copy(("far", b, 3 - k), onward.at[k - 1, b, :, deep(b)], far.at[3 - k, b, :, deep(b)], rep=place(2)).start()

        roles["far"] = middle

    def relay_far(b):
        @pl.when(middle)
        def _():
            arrive(("far", b, 0), far.at[0, b, :, deep(b)])
            onward[0, b, :, deep(b)] = down(up(deep_of(b, place(0))) + up(far[0, b, :, deep(b)]))
            copy(("last", b), onward.at[0, b, :, deep(b)], last.at[b, :, deep(b)], rep=place(0)).start()

        roles["last"] = middle

    def send_cross(b):
        at = deep(b)

        @pl.when(is_tip)
        def _():
            arrive(("last", b), last.at[b, :, at])
            ztotal[b, :, at] = down(up(deep_of(b, q)) + up(last[b, :, at]))

        @pl.when(middle)
        def _():
            arrive(("near", b, 1), near.at[0, b, :, at])
            arrive(("far", b, 1), far.at[1, b, :, at])
            total = up(deep_of(b, q)) + up(near[0, b, :, at])
            ztotal[b, :, at] = down(total + up(far[1, b, :, at]))

        for d in range(1, pod_count):
            send(
                ("cross", b), ztotal.at[b, :, deep_cols(b, pod(d))],
                cross.at[d - 1, b, :, pl.ds(0, deep_width(b))], outer=pod(d),
            )

    scale = 1.0 / (pod_count * rep_count)

    def put_mean(b, at, total):
        value = total * scale
        mean[b, :, at] = down(value)
        square = value * value
        part = squares[0]
        height, width = square.shape
        for k in range(height // 8):
            for i in range(width // 128):
                part = part + square[k * 8:(k + 1) * 8, i * 128:(i + 1) * 128]
        squares[0] = part

    def finish_pair(b):
        if late(b):
            arrive(("second", b, 0), deltas.at[b, q, :, pl.ds(0, pair_width(b))])
        arrive(("third", b), zrecv.at[:, b, :, pl.ds(0, pair_width(b))])
        for r in range(2):
            total = pair_total(r, b, q)
            for d in range(rep_count - 1):
                total = total + up(zrecv[d, b, :, pair_local(r, b)])
            put_mean(b, pair_local(r, b), total)

    def finish_cross(b):
        at = pl.ds(0, deep_width(b))
        arrive(("cross", b), cross.at[:, b, :, at])
        total = up(ztotal[b, :, deep_cols(b, o)])
        for d in range(pod_count - 1):
            total = total + up(cross[d, b, :, at])
        put_mean(b, pl.ds(pair_width(b), deep_width(b)), total)

    owner, rank = [], []

    def read_owners():
        loads[blocks + 2].wait()
        owner.extend(owners[b] for b in range(blocks))
        for b in range(blocks):
            count = jnp.int32(0)
            for before in range(b):
                count = count + (owner[before] == owner[b]).astype(jnp.int32)
            rank.append(count)

    def block_of(k, j):
        index, found = jnp.int32(0), jnp.int32(0)
        for b in range(blocks):
            match = ((owner[b] == k) & (rank[b] == j)).astype(jnp.int32)
            index, found = index + b * match, found + match
        return index, found

    def load_rows(b):
        loads[b].wait()

    def pack_early():
        loads[blocks].wait()
        loads[blocks + 1].wait()
        for k in range(pod_count):
            for r in range(3):
                at = pl.ds(base[r] + k * widths[r], widths[r])

                def body(i):
                    value = master[i, :, at] - 0.567 * momentum[i, :, at]
                    apack[k, i, :, local_cols(r)] = down(value)

                loop(slots, body)
        arecv[o] = apack[o]

    def send_early(*steps):
        for d in steps:
            send(("early",), apack.at[pod(d)], arecv.at[o], outer=pod(d))

    group = pod_count * rep_count

    lead = s == 0
    follow = jnp.logical_not(lead)
    partial = group + shard_count

    def norm_send():
        others[partial] = jnp.sum(squares[0], axis=0, keepdims=True)
        send_if(follow, ("shard",), others.at[partial], others.at[group + s], shard=0)

    def norm_lead():
        roles["norm"] = lead

        @pl.when(lead)
        def _():
            arrive(("shard",), others.at[pl.ds(group + 1, shard_count - 1)])
            total = others[partial]
            for d in range(1, shard_count):
                total = total + others[group + d]
            others[group] = total
            others[0] = total
            for e in range(rep_count):
                for d in range(pod_count):
                    for t in range(shard_count):
                        if d or e or t:
                            copy(
                                ("norm",), others.at[group], others.at[d * rep_count + e],
                                outer=pod(d), rep=(q + e) % rep_count, shard=t,
                            ).start()

    def mean_send(part):
        at = pl.ds(wa + wb, wc) if part == 0 else pl.ds(0, wa + wb)
        for d in range(pod_count):
            for j in range(slots):
                packed[d, j, :, at] = mean[block_of(pod(d), j)[0], :, at]
            if d == 0:
                slotted[o, :, :, at] = packed[0, :, :, at]
            else:
                send(("slot", part), packed.at[d, :, :, at], slotted.at[o, :, :, at], outer=pod(d))

    def norm_wait():
        pl.when(lead)(lambda: arrive(("norm",), others.at[pl.ds(1, group - 1)]))
        pl.when(follow)(lambda: arrive(("norm",), others.at[pl.ds(0, group)]))
        arrive(("early",), arecv.at[pl.ds(1, pod_count - 1)])
        total = others[0]
        for d in range(1, group):
            total = total + others[d]
        total = jnp.sum(total, keepdims=True)
        return jnp.minimum(1.0, clip_limit / jnp.sqrt(total + 1e-06))

    def spread(b, factor):
        for r in range(3):
            at = local_cols(r)
            early = up(arecv[owner[b], jnp.minimum(rank[b], slots - 1), :, at])
            value = early - (1.33 * factor) * up(mean[b, :, at])
            out[b, q, :, cols(r, o)] = down(value)

    def send_wide(b):
        at = out.at[b, q, :, cols(2, o)]
        send(("wide", b), at, at, outer=neighbour[order(0, b)[0]])

    def send_wider(b):
        arrive(("wide", b), out.at[b, q, :, pl.ds(0, wc)])
        axis, other = order(0, b)
        for k in (o, neighbour[axis]):
            at = out.at[b, q, :, cols(2, k)]
            send(("wider", b), at, at, outer=neighbour[other])

    def pass_line(role, group, b, k, **to):
        for r in range(2):
            at = out.at[b, place(k), :, cols(r, o)]
            send_if(role, group, at, at, **to)

    def line_rows(b, count):
        return out.at[b, pl.ds(0, count), :, pl.ds(0, wa + wb)]

    def send_up(b):
        pass_line(is_tip, ("up", b), b, 0, rep=place(1))

    def send_mid(b):
        pass_line(middle, ("down", b), b, 1, rep=place(0))
        pass_line(middle, ("over", b, 1), b, 1, rep=place(2))

    def line_near(b):
        pl.when(middle)(lambda: arrive(("over", b, 1), line_rows(b, 1)))
        pass_line(middle, ("down", b), b, 2, rep=place(0))
        pl.when(middle)(lambda: arrive(("up", b), line_rows(b, 1)))
        pass_line(middle, ("over", b, 0), b, 0, rep=place(2))

    def line_far(b):
        pl.when(middle)(lambda: arrive(("over", b, 0), line_rows(b, 1)))
        pass_line(middle, ("down", b), b, 3, rep=place(0))

    def wide_done(b):
        arrive(("wider", b), out.at[b, q, :, pl.ds(0, SIDE * wc)])

    def line_tip(b):
        mine = out.at[b, q, :, whole]
        pl.when(is_tip)(lambda: wide_done(b))
        send_if(is_tip, ("outward", b, 0), mine, mine, rep=place(1))

    def line_mid(b):
        mine = out.at[b, q, :, whole]
        pl.when(middle)(lambda: wide_done(b))
        send_if(middle, ("across", b, 1), mine, mine, rep=place(2))

    def line_across(b):
        at = out.at[b, place(0), :, whole]
        pl.when(middle)(lambda: arrive(("outward", b, 0), at))
        send_if(middle, ("across", b, 0), at, at, rep=place(2))

    def line_inward(b, k):
        at = out.at[b, place(k), :, whole]
        if k > 1:
            pl.when(middle)(lambda: arrive(("across", b, 3 - k), at))
        send_if(middle, ("inward",), at, at, rep=place(0))

    def line_end():
        pl.when(is_tip)(lambda: arrive(("inward",), out.at[:, pl.ds(0, 3), :, whole]))

    def send_block(b, d):
        i = (q + rep_count - d) % rep_count
        for r in range(2):
            at = out.at[b, i, :, cols(r, o)]
            send(("block", b, d), at, at, outer=neighbour[order(r, b)[1]])

    def send_blocks(b, d):
        i = (q + rep_count - d) % rep_count
        arrive(("block", b, d), out.at[b, i, :, pl.ds(0, wa + wb)])
        for r in range(2):
            axis = order(r, b)[0]
            for j in range(SIDE):
                at = out.at[b, i, :, cols(r, quarter(axis, j, False))]
                send(("blocks",), at, at, outer=neighbour[axis])

    def update(factor):
        for part, width in enumerate((wc, wa + wb)):
            arrive(("slot", part), slotted.at[pl.ds(1, pod_count - 1), :, :, pl.ds(0, width)])
        for j in range(slots):
            found = block_of(o, j)[1].astype(jnp.float32)
            for k in range(pod_count):
                for r in range(3):
                    at = pl.ds(base[r] + k * widths[r], widths[r])
                    step = (factor * found) * up(slotted[k, j, :, local_cols(r)])
                    moved = 0.9 * momentum[j, :, at] + step
                    new_momentum[j, :, at] = moved
                    new_master[j, :, at] = master[j, :, at] - 0.7 * (step + 0.9 * moved)

    def finish():
        arrive(("blocks",), out.at[:, :, :, pl.ds(0, SIDE * (wa + wb))])

    def drain():
        pairs = sum(pair_width(b) for b in range(blocks))
        deeps = sum(deep_width(b) for b in range(blocks))
        some = blocks // 2

        def rows(count, width):
            return deltas.at[0, pl.ds(0, count), :, pl.ds(0, width)]

        def deep_rows(count):
            return deltas.at[pl.ds(0, some), pl.ds(0, count), :, pl.ds(0, pod_count * deeps // some)]

        leave("first", deltas.at[pl.ds(0, SIDE + 1), :, :, pl.ds(0, pairs)])
        leave("third", rows(rep_count - 1, pairs))
        leave("near", deep_rows(3))
        leave("far", deep_rows(3))
        leave("cross", rows(pod_count - 1, deeps))
        leave("early", deltas.at[pl.ds(0, pod_count - 1), pl.ds(0, SIDE * slots), :, pl.ds(0, arecv.shape[3])])
        leave("norm", others.at[pl.ds(0, group * shard_count - 1)])
        leave("shard", others.at[pl.ds(0, 1)])
        leave("wide", out.at[:, 0, :, pl.ds(0, wc)])
        leave("wider", out.at[:, 0, :, pl.ds(0, SIDE * wc)])
        leave("up", out.at[:, 0, :, pl.ds(0, wa + wb + pod_count * wc)])
        leave("over", out.at[:, pl.ds(0, 2), :, pl.ds(0, wa + wb + pod_count * wc)])
        leave("down", out.at[:, pl.ds(0, 3), :, pl.ds(0, wa + wb + pod_count * wc)])
        leave("block", out.at[:, :, :, pl.ds(0, (1 + SIDE) * (wa + wb))])

    def rests(b):
        pl.when(is_tip)(lambda: arrive(("down", b), line_rows(b, 3)))
        for d in others_of:
            send_block(b, d)

    def rests_on(b):
        for d in others_of:
            send_blocks(b, d)

    squares[0] = jnp.zeros(squares.shape[1:], jnp.float32)
    def firsts(b):
        for g in others_of if late(b) else tail:
            send_first(b, g)

    def seconds(b):
        for g in others_of if late(b) else tail:
            send_second(b, g)

    for b in range(blocks):
        load_rows(b)
        if b < 2:
            firsts(b)
        if b > 0:
            start_tips(b - 1)
    start_tips(blocks - 1)
    pack_early()
    read_owners()
    for t in range(blocks + 2):
        if t < blocks:
            relay_near(t)
            if t == 0:
                pass_ready()
            seconds(t)
            if t == 0:
                all_ready()
        if t + 2 < blocks:
            firsts(t + 2)
            if t + 3 == blocks:
                for b in range(blocks - LATE, blocks - 2):
                    send_first(b, 0)
        if t == blocks - 1:
            for b in range(max(blocks - LATE, blocks - 2), blocks):
                send_first(b, 0)
        if 0 <= t - 1 < blocks:
            if t == blocks:
                send_early(1, 2)
                for b in range(blocks - LATE, blocks):
                    send_second(b, 0)
                send_third(t - 1)
                relay_far(t - 1)
            else:
                relay_far(t - 1)
                send_third(t - 1)
        if 0 <= t - 2 < blocks:
            send_cross(t - 2)
    send_early(3)
    for b in range(blocks):
        if b < 2:
            finish_pair(b)
        finish_cross(b)
    mean_send(0)
    for b in range(2, blocks):
        finish_pair(b)
    norm_send()
    norm_lead()
    mean_send(1)
    factor = norm_wait()
    for b in range(blocks):
        spread(b, factor)
        send_wide(b)
        send_up(b)
        if b < 2:
            send_mid(b)
        send_block(b, 0)
    line_near(0)
    send_wider(0)
    send_blocks(0, 0)
    line_near(1)
    send_wider(1)
    send_blocks(1, 0)
    send_mid(2)
    line_far(0)
    for b in range(2, blocks):
        send_wider(b)
        send_blocks(b, 0)
    for b in range(blocks):
        line_tip(b)
    rests(0)
    line_near(2)
    line_far(1)
    send_mid(3)
    line_near(3)
    rests(1)
    line_mid(0)
    line_mid(1)
    line_far(2)
    line_mid(2)
    line_mid(3)
    rests_on(0)
    line_across(0)
    rests(2)
    line_far(3)
    line_across(1)
    rests_on(1)
    rests(3)
    line_across(2)
    line_across(3)
    for b in range(blocks):
        line_inward(b, 1)
        line_inward(b, 2)
    rests_on(2)
    update(factor)
    line_inward(0, 3)
    line_inward(1, 3)
    rests_on(3)
    line_inward(2, 3)
    line_inward(3, 3)
    line_end()
    finish()
    drain()
    assert len(spans) + max(len(p) for p in phases) == recv_sem.shape[0]
    assert len(sent) == send_sem.shape[0]


def store(*refs):
    sem = refs[-1]
    copies = []
    for i in range(3):
        for k in range(refs[i].shape[0]):
            copies.append(pltpu.make_async_copy(refs[i].at[k], refs[i + 3].at[k], sem.at[len(copies)]))
    for copy in copies:
        copy.start()
    for copy in copies:
        copy.wait()


def regions(width, pod_count):
    tiles = width // (128 * pod_count)
    wc = max(1, round(tiles * DEEP))
    wb = (tiles - wc) // 2
    return tuple(128 * n for n in (tiles - wc - wb, wb, wc, EXTRA))


def fused(deltas, owners, master, momentum):
    blocks = owners.shape[1]
    slots, sub_rows, width = master.shape[2:]
    pod_count, rep_count = lax.axis_size("outer"), lax.axis_size("rep")
    shard_count = lax.axis_size("shard")
    entries = shard_count * blocks * rep_count * sub_rows * width
    clip_limit = 0.5 * math.sqrt(entries)
    widths = regions(width, pod_count)
    wa, wb, wc, extra = widths
    part, deep_width = width // pod_count, extra + wc
    deep = pod_count * deep_width
    group = pod_count * rep_count
    reduce_waits = 2 * blocks + rep_count * LATE + 8 * blocks
    waits = 5 + max(reduce_waits, blocks * (rep_count + 9) + 2)
    vmem, hbm = pl.BlockSpec(memory_space=pltpu.VMEM), pl.BlockSpec(memory_space=pltpu.HBM)
    bf16, f32 = jnp.bfloat16, jnp.float32
    V = pltpu.VMEM
    out, new_momentum, new_master = pl.pallas_call(
        functools.partial(kernel, widths, (pod_count, rep_count, shard_count), clip_limit),
        out_shape=(
            V((blocks, rep_count, sub_rows, width), bf16),
            V(master.shape[2:], f32),
            V(master.shape[2:], f32),
        ),
        in_specs=[hbm] * 4,
        out_specs=(vmem, vmem, vmem),
        scratch_shapes=[
            pltpu.SMEM((blocks,), jnp.int32),
            V((blocks, rep_count, sub_rows, width), bf16),
            V(master.shape[2:], f32),
            V(master.shape[2:], f32),
            pltpu.SemaphoreType.DMA((blocks + 3,)),
            [V((SIDE, blocks, rep_count, sub_rows, w), bf16) for w in (wa, wb)],
            [V((blocks, rep_count, sub_rows, w), bf16) for w in (wa, wb)],
            [V((blocks, rep_count, sub_rows, w), bf16) for w in (wa, wb)],
            V((blocks, rep_count - 1, sub_rows, wa + wb), bf16),
            V((rep_count - 1, blocks, sub_rows, wa + wb), bf16),
            V((3, blocks, sub_rows, deep), bf16),
            V((3, blocks, sub_rows, deep), bf16),
            V((2, blocks, sub_rows, deep), bf16),
            V((blocks, sub_rows, deep), bf16),
            V((3, blocks, sub_rows, deep), bf16),
            V((blocks, sub_rows, deep), bf16),
            V((pod_count - 1, blocks, sub_rows, deep_width), bf16),
            V((pod_count, slots, sub_rows, part), bf16),
            V((pod_count, slots, sub_rows, part), bf16),
            V((blocks, sub_rows, part), bf16),
            V((pod_count, slots, sub_rows, part), bf16),
            V((pod_count, slots, sub_rows, part), bf16),
            V((1, 8, 128), f32),
            V((group * shard_count + shard_count, 1, 128), f32),
            pltpu.SemaphoreType.DMA((KINDS,)),
            pltpu.SemaphoreType.DMA((waits,)),
            pltpu.SemaphoreType.REGULAR,
        ],
        compiler_params=pltpu.CompilerParams(
            collective_id=0, has_side_effects=True, vmem_limit_bytes=48 * 1024 * 1024
        ),
    )(
        owners[0, :, 0],
        deltas.reshape(blocks, rep_count, sub_rows, width),
        master.reshape(master.shape[2:]),
        momentum.reshape(momentum.shape[2:]),
    )
    arrays = (out, new_momentum, new_master)
    out, new_momentum, new_master = pl.pallas_call(
        store,
        out_shape=tuple(jax.ShapeDtypeStruct(a.shape, a.dtype) for a in arrays),
        in_specs=[pl.BlockSpec(memory_space=pl.ANY)] * 3,
        out_specs=(hbm,) * 3,
        scratch_shapes=[pltpu.SemaphoreType.DMA((blocks + 2 * slots,))],
        compiler_params=pltpu.CompilerParams(vmem_limit_bytes=4 * 1024 * 1024),
    )(*(pltpu.with_memory_space_constraint(a, pltpu.VMEM) for a in arrays))
    return (
        out.reshape(blocks * rep_count * sub_rows, width),
        new_momentum.reshape(momentum.shape),
        new_master.reshape(master.shape),
    )


def local(deltas, owners, master, momentum):
    blocks_here = owners.shape[1]
    slot_count = master.shape[2]
    sub_rows = master.shape[3]
    row_width = deltas.shape[3]
    block_rows = deltas.shape[2] // blocks_here
    pod_count = lax.axis_size("outer")
    rep_count = lax.axis_size("rep")
    owned_blocks = owners[0, :, 0]
    pod_ids = jnp.arange(pod_count, dtype=jnp.int32)
    onehot = (owned_blocks[:, None] == pod_ids[None, :]).astype(jnp.int32)
    rank_all = jnp.cumsum(onehot, axis=0) - onehot
    rank_own = jnp.sum(rank_all * onehot, axis=1)
    slot_ids = jnp.arange(slot_count, dtype=jnp.int32)
    selector = (
        (owned_blocks[None, None, :] == pod_ids[:, None, None])
        & (rank_own[None, None, :] == slot_ids[None, :, None])
    ).astype(jnp.bfloat16)
    local_rows = deltas[0, 0].reshape(blocks_here, block_rows, row_width)
    block_sums = lax.psum_scatter(
        local_rows.astype(jnp.float32).astype(jnp.bfloat16), "rep", scatter_dimension=1, tiled=True
    ).astype(jnp.float32)
    block_sums = block_sums.astype(jnp.bfloat16)
    pod_part = jnp.einsum(
        "ojb,brw->ojrw", selector, block_sums, preferred_element_type=jnp.float32
    ).astype(jnp.bfloat16)
    arrived = lax.all_to_all(pod_part, "outer", split_axis=0, concat_axis=0, tiled=True)
    mean_share = jnp.sum(arrived.astype(jnp.float32), axis=0) / (pod_count * rep_count)
    local_sq = jnp.sum(mean_share * mean_share)
    total_sq = lax.psum(local_sq, ("outer", "rep", "shard"))
    total_entries = lax.axis_size("shard") * blocks_here * block_rows * row_width
    clip_limit = 0.5 * math.sqrt(total_entries)
    factor = jnp.minimum(1.0, clip_limit / jnp.sqrt(total_sq + 1e-06))
    step_part = factor * mean_share[None, None]
    new_momentum = 0.9 * momentum + step_part
    new_master = master - 0.7 * (step_part + 0.9 * new_momentum)
    params_here = new_master.astype(jnp.bfloat16)
    gathered = lax.all_gather(params_here, ("outer", "rep"), axis=0, tiled=True).reshape(
        pod_count, rep_count, slot_count, sub_rows, row_width
    )
    unpacked = jnp.einsum("ojb,oqjrw->bqrw", selector, gathered, preferred_element_type=jnp.float32)
    new_params = unpacked.astype(jnp.bfloat16).reshape(blocks_here * block_rows, row_width)
    return (new_params, new_momentum, new_master)


def solution(mesh):
    fits = mesh.shape["outer"] == SIDE * SIDE and mesh.shape["rep"] == LINE

    def body(deltas, owners, master, momentum):
        blocks = owners.shape[1]
        width, sub_rows = master.shape[4], master.shape[3]
        tiled = width % (SIDE * SIDE * 128) == 0 and width >= 3 * SIDE * SIDE * 128
        tiled = tiled and sub_rows % TILE == 0 and blocks == SIDE * SIDE
        tiled = tiled and deltas.shape[2] == blocks * LINE * sub_rows
        if tiled:
            wa, wb, wc, extra = regions(width, SIDE * SIDE)
            tiled = wb > extra and SIDE * blocks * (wc + extra) <= width
        return (fused if fits and tiled else local)(deltas, owners, master, momentum)

    return jax.shard_map(
        body,
        mesh=mesh,
        in_specs=(
            P("outer", "rep", "shard", None),
            P("shard", None, None),
            P("outer", "shard", None, "rep", None),
            P("outer", "shard", None, "rep", None),
        ),
        out_specs=(
            P("shard", None),
            P("outer", "shard", None, "rep", None),
            P("outer", "shard", None, "rep", None),
        ),
        check_vma=False,
    )
```
